256 devices in a mesh: gx: 4 (over x), gy: 4 (over y), gz: 16 (over z, core).
Axes of the slice: x: 4, y: 4, z: 8, core: 2. Of those that a mesh axis runs over, the one named last changes fastest.
Arguments:
- residual: float32 [3, 256, 256, 512], P(None, 'gz', 'gx', 'gy'), may hold values from -32 to 32
- edge_diag: float32 [3, 256, 256, 512], P(None, 'gz', 'gx', 'gy'), may hold values from 6.5 to 9
- node_shift: float32 [256, 256, 512], P('gz', 'gx', 'gy'), may hold values from 0.05 to 3
- coarse_shift: float32 [128, 128, 256], P('gz', 'gx', 'gy'), may hold values from 0.05 to 3
Outputs:
- correction: float32 [3, 256, 256, 512], P(None, 'gz', 'gx', 'gy')
The draws below stay inside these ranges and needn't reach their ends.
All inputs are finite; a program needn't handle non-finite values.
Results may differ from the reference program's by a relative error of at most 0.000021.
Values sent between devices are 32-bit elements; how exact they have to be, the bound alone decides.
A program may use at most 128 MiB of HBM per device.

```python
import math
import jax
import jax.numpy as jnp

NX = 256
NY = 512
NZ = 256


def draw_residual(key, part):
    second_key = jax.random.fold_in(jax.random.fold_in(key, 11), 1)
    zpos = jnp.arange(NZ, dtype=jnp.float32) / NZ
    xpos = jnp.arange(NX, dtype=jnp.float32) / NX
    ramp = 2.0 * (1.0 + zpos)[:, None, None] * (1.0 + xpos)[None, :, None] * jnp.ones((1, 1, NY), jnp.float32)
    rough = jnp.clip(jax.random.normal(second_key, (3, NZ, NX, NY), jnp.float32), -4.0, 4.0)
    values = ramp[None] * rough
    return values.astype(jnp.float32)


def level_of(own_key, shape, shards, least, top_value):
    loudness = 1.0
    for position, shards_of in shards:
        draws = jax.random.uniform(jax.random.fold_in(jax.random.fold_in(own_key, 6), position), (shards_of,), jnp.float32, least / len(shards), top_value / len(shards))
        loudness = loudness * jnp.repeat(jnp.exp(draws), shape[position] // shards_of).reshape((-1,) + (1,) * (len(shape) - 1 - position))
    return loudness


def setup_inputs(seed: int = 0) -> dict:
    keys = jax.random.split(jax.random.key(seed), 5)
    return {
        "residual": draw_residual(jax.random.fold_in(keys[4], 71), 0),
        "edge_diag": jnp.clip(6.5 + 2.5 * jax.random.uniform(keys[1], (3, NZ, NX, NY), jnp.float32) ** level_of(keys[1], (3, NZ, NX, NY), ((1, 16), (2, 4), (3, 4)), -0.2, 0.2), 6.5, 9.0),
        "node_shift": jnp.clip(jnp.exp(math.log(3.0) - 4.0943445 * jax.random.uniform(keys[2], (NZ, NX, NY), jnp.float32) ** level_of(keys[2], (NZ, NX, NY), ((0, 16), (1, 4), (2, 4)), -0.2, 0.2)), 0.05, 3.0),
        "coarse_shift": jnp.clip(jnp.exp(math.log(3.0) - 4.0943445 * jax.random.uniform(keys[3], (NZ // 2, NX // 2, NY // 2), jnp.float32) ** level_of(keys[3], (NZ // 2, NX // 2, NY // 2), ((0, 16), (1, 4), (2, 4)), -0.2, 0.2)), 0.05, 3.0),
    }


def neighbours(padded):
    total = padded[2:, 1:-1, 1:-1] + padded[:-2, 1:-1, 1:-1]
    total = total + padded[1:-1, 2:, 1:-1] + padded[1:-1, :-2, 1:-1]
    return total + padded[1:-1, 1:-1, 2:] + padded[1:-1, 1:-1, :-2]


def apply_op(field, diagonal):
    return diagonal * field - neighbours(jnp.pad(field, 1))


def reference(residual, edge_diag, node_shift, coarse_shift):
    scaled = residual / edge_diag
    padded = jnp.pad(scaled, ((0, 0), (1, 1), (1, 1), (1, 1)))
    edge_near = jnp.stack([neighbours(padded[component]) for component in range(3)])
    smooth_part = 2.0 * scaled - (edge_diag * scaled - edge_near) / edge_diag
    nodal_rhs = (padded[0, :-2, 1:-1, 1:-1] - scaled[0]) + (padded[1, 1:-1, :-2, 1:-1] - scaled[1]) + (padded[2, 1:-1, 1:-1, :-2] - scaled[2])
    node_diag = 6.0 + node_shift
    first_guess = nodal_rhs / node_diag
    node_res = nodal_rhs - apply_op(first_guess, node_diag)
    sx, sy, sz = node_res.shape
    coarse_rhs = node_res.reshape(sx // 2, 2, sy // 2, 2, sz // 2, 2).sum(axis=(1, 3, 5))
    coarse_diag = 6.0 + coarse_shift
    first_dir = coarse_rhs / coarse_diag
    first_image = apply_op(first_dir, coarse_diag)
    second_dir = first_image / coarse_diag
    second_image = apply_op(second_dir, coarse_diag)
    gone = jnp.sum(first_dir * coarse_rhs)
    gtwo = jnp.sum(second_dir * coarse_rhs)
    hone = jnp.sum(first_dir * first_image)
    hmix = jnp.sum(second_dir * first_image)
    htwo = jnp.sum(second_dir * second_image)
    coef_two = (gtwo - hmix * gone / hone) / (htwo - hmix * hmix / hone)
    coef_one = (gone - hmix * coef_two) / hone
    coarse_sol = coef_one * first_dir + coef_two * second_dir
    spread = jnp.broadcast_to(coarse_sol[:, None, :, None, :, None], (sx // 2, 2, sy // 2, 2, sz // 2, 2)).reshape(sx, sy, sz)
    nodal = first_guess + spread
    final_nodal = nodal + (nodal_rhs - apply_op(nodal, node_diag)) / node_diag
    fpad = jnp.pad(final_nodal, 1)
    grads = jnp.stack([fpad[2:, 1:-1, 1:-1] - final_nodal, fpad[1:-1, 2:, 1:-1] - final_nodal, fpad[1:-1, 1:-1, 2:] - final_nodal])
    return smooth_part + grads
```

```python
import functools

import jax
import jax.numpy as jnp
from jax import lax
from jax.experimental import pallas as pl
from jax.experimental.pallas import tpu as pltpu
from jax.sharding import PartitionSpec as P

MESH = pl.DeviceIdType.MESH
AXES = ("gx", "gy", "gz")
L = 128
F32 = jnp.float32


def iota(shape, dim):
    return lax.broadcasted_iota(jnp.int32, shape, dim)


class Message:
    def __init__(self, copy, sends, receives):
        self.copy, self.sends, self.receives = copy, sends, receives

    def start(self):
        pl.when(self.sends)(lambda: self.copy.start())

    def wait_recv(self):
        pl.when(self.receives)(lambda: self.copy.wait_recv())

    def wait_send(self):
        pl.when(self.sends)(lambda: self.copy.wait_send())


def kernel(
    sizes, res_h, ed_h, ns_h, cs_h, out_h,
    res, ed, ns, cs, sc, fg, tmp, cr, cd, v1, v2, wy1, wy2, a1s, ab, ff,
    rt_sc, rt_fg, rt_v1, rt_v2, rt_ab,
    xs_sc, xr_sc, xs_fg, xr_fg, xs_v1, xr_v1, xs_v2, xr_v2, xs_ab, xr_ab,
    ys_sc, yr_sc, ys_fg, yr_fg, ys_v1, yr_v1, ys_v2, yr_v2, ys_ab, yr_ab,
    ar1, ar2, in_sem, out_sem, send_sem, recv_sem, ar_send, ar_recv,
):
    _, Z, X, _ = res.shape
    ZC, XC = Z // 2, X // 2
    NB = Z // 2
    PC = L // XC
    NBC = ZC // PC
    me = {a: lax.axis_index(a) for a in AXES}
    used = []

    def message(src, dst, axis, step):
        i = len(used)
        last = sizes[axis] - 1
        copy = pltpu.make_async_remote_copy(
            src_ref=src, dst_ref=dst, send_sem=send_sem.at[i], recv_sem=recv_sem.at[i],
            device_id={axis: me[axis] + step}, device_id_type=MESH,
        )
        low, high = me[axis] > 0, me[axis] < last
        made = Message(copy, *((high, low) if step > 0 else (low, high)))
        used.append(made)
        return made

    def load(k):
        return (
            pltpu.make_async_copy(ed_h.at[k], ed.at[k], in_sem.at[2 * k]),
            pltpu.make_async_copy(res_h.at[k], res.at[k], in_sem.at[2 * k + 1]),
        )

    loads = [load(k) for k in range(3)]
    load_ns = pltpu.make_async_copy(ns_h, ns, in_sem.at[6])
    load_cs = pltpu.make_async_copy(cs_h, cs, in_sem.at[7])
    for k in (2, 1, 0):
        for copy in loads[k]:
            copy.start()
    load_ns.start()
    load_cs.start()

    zero_plane = jnp.zeros((X, L), F32)
    zero_coarse = jnp.zeros((XC, L), F32)
    for k in range(3):
        for z in (0, Z + 1):
            sc[k, z, 8 : 8 + X, :] = zero_plane
        ab[k, Z, 0:X, :] = zero_plane
    for z in (0, Z + 1):
        fg[z, 8 : 8 + X, :] = zero_plane
    for z in (0, ZC + 1):
        v1[z, 8 : 8 + XC, :] = zero_coarse
        v2[z, 8 : 8 + XC, :] = zero_coarse
    for ref in (xr_sc, xr_fg, xr_v1, xr_v2, xr_ab, yr_sc, yr_fg, yr_v1, yr_v2, yr_ab):
        ref[...] = jnp.zeros(ref.shape, F32)

    partners = [{"gz": lax.rem(me["gz"] + d, sizes["gz"])} for d in range(1, sizes["gz"])]
    plane = [
        {"gx": lax.rem(me["gx"] + dx, sizes["gx"]), "gy": lax.rem(me["gy"] + dy, sizes["gy"])}
        for dx in range(sizes["gx"]) for dy in range(sizes["gy"]) if dx or dy
    ]
    barrier = pltpu.get_barrier_semaphore()
    for other in partners + plane:
        pl.semaphore_signal(barrier, inc=1, device_id=other, device_id_type=MESH)

    lane = iota((X, L), 1)
    lane2 = iota((L, L), 1)
    lanec = iota((XC, L), 1)
    evenc = lanec % 2 == 0

    def put(packed, block, q):
        return jnp.where(lax.shift_right_logical(lane2, 1) == q, pltpu.roll(block, 2 * q + 1, 1), packed)

    def halo(rt, row, rows, q):
        return pltpu.roll(rt[row : row + rows, :], L - 1 - 2 * q, 1)

    def before(x, h, at):
        return jnp.where(at == 0, h, pltpu.roll(x, 1, 1))

    def after(x, h, at):
        return jnp.where(at == L - 1, h, pltpu.roll(x, L - 1, 1))

    def unpack(rt, got):
        n = got.shape[1]
        mixed = jnp.where(
            iota((n, L), 0) % 2 == 1, pltpu.roll(got[0], 1, 0), pltpu.roll(got[1], n - 1, 0)
        )
        rt[...] = jnp.concatenate([mixed, jnp.zeros((L - n, L), F32)], axis=0).T

    def scale(k, packed):
        for copy in loads[k]:
            copy.wait()

        def body(b, packed):
            block = []
            for p in range(2):
                z = 2 * b + p
                r = 1.0 / ed[k, z]
                ed[k, z] = r
                s = res[k, z] * r
                sc[k, z + 1, 8 : 8 + X, :] = s
                xs_sc[0, k, pl.ds(z, 1), :] = s[0:1]
                xs_sc[1, k, pl.ds(z, 1), :] = s[X - 1 : X]
                block.append(s)
            return put(packed, jnp.concatenate(block, axis=0), k * NB + b)

        return lax.fori_loop(0, NB, body, packed)

    packed = jnp.zeros((L, L), F32)
    for k in (2, 1, 0):
        packed = scale(k, packed)
    ys_sc[...] = packed.T[: 6 * NB]
    pl.semaphore_wait(barrier, len(partners) + len(plane))

    inner = pl.ds(8, X)
    sc_zu0 = message(sc.at[0, Z, inner, :], sc.at[0, 0, inner, :], "gz", 1)
    sc_zu = message(sc.at[1:3, Z, inner, :], sc.at[1:3, 0, inner, :], "gz", 1)
    sc_zd = message(sc.at[:, 1, inner, :], sc.at[:, Z + 1, inner, :], "gz", -1)
    sc_xu = message(xs_sc.at[1], xr_sc.at[0], "gx", 1)
    sc_xd = message(xs_sc.at[0], xr_sc.at[1], "gx", -1)
    sc_yu = message(ys_sc, yr_sc.at[0], "gy", 1)
    sc_yd = message(ys_sc, yr_sc.at[1], "gy", -1)
    for m in (sc_zu0, sc_xu, sc_yu, sc_yd, sc_xd, sc_zd, sc_zu):
        m.start()

    load_ns.wait()
    load_cs.wait()

    def invert(z, _):
        ns[z] = 1.0 / (6.0 + ns[z])
        return 0

    lax.fori_loop(0, Z, invert, 0)
    twice = (iota((L // 2, L), 0) == iota((L // 2, L), 1) // 2).astype(F32)
    wide = jnp.dot(
        cs[...].reshape(ZC * XC, L // 2), twice,
        precision=lax.Precision.HIGHEST, preferred_element_type=F32,
    )
    cd[...] = (1.0 / (6.0 + wide)).reshape(ZC, XC, L)

    for m in (sc_zu0, sc_xu, sc_yu, sc_yd, sc_xd):
        m.wait_recv()
    for k in range(3):
        sc[k, 1 : Z + 1, 7, :] = xr_sc[0, k]
        sc[k, 1 : Z + 1, 8 + X, :] = xr_sc[1, k]
    unpack(rt_sc, yr_sc)

    def guess(b, packed):
        block = []
        for p in range(2):
            z = 2 * b + p
            s0, s0m = sc[0, z + 1, 8 : 8 + X, :], sc[0, z, 8 : 8 + X, :]
            s1, s1m = sc[1, z + 1, 8 : 8 + X, :], sc[1, z + 1, 7 : 7 + X, :]
            s2 = sc[2, z + 1, 8 : 8 + X, :]
            s2m = before(s2, halo(rt_sc, p * X, X, 2 * NB + b), lane)
            g = ((s0m - s0) + (s1m - s1) + (s2m - s2)) * ns[z]
            fg[z + 1, 8 : 8 + X, :] = g
            xs_fg[0, pl.ds(z, 1), :] = g[0:1]
            xs_fg[1, pl.ds(z, 1), :] = g[X - 1 : X]
            block.append(g)
        return put(packed, jnp.concatenate(block, axis=0), b)

    packed = lax.fori_loop(0, NB, guess, jnp.zeros((L, L), F32))
    ys_fg[...] = packed.T[: 2 * NB]
    fg_m = [
        message(ys_fg, yr_fg.at[0], "gy", 1),
        message(ys_fg, yr_fg.at[1], "gy", -1),
        message(xs_fg.at[1], xr_fg.at[0], "gx", 1),
        message(xs_fg.at[0], xr_fg.at[1], "gx", -1),
        message(fg.at[Z, inner, :], fg.at[0, inner, :], "gz", 1),
        message(fg.at[1, inner, :], fg.at[Z + 1, inner, :], "gz", -1),
    ]
    for m in fg_m:
        m.start()

    def smooth(k):
        def body(b, _):
            for p in range(2):
                z = 2 * b + p
                s = sc[k, z + 1, 8 : 8 + X, :]
                h = halo(rt_sc, p * X, X, k * NB + b)
                n = sc[k, z, 8 : 8 + X, :] + sc[k, z + 2, 8 : 8 + X, :]
                n += sc[k, z + 1, 7 : 7 + X, :] + sc[k, z + 1, 9 : 9 + X, :]
                n += before(s, h, lane) + after(s, h, lane)
                res[k, z] = s + n * ed[k, z]
            return 0

        lax.fori_loop(0, NB, body, 0)

    sc_zu.wait_recv()
    sc_zd.wait_recv()
    smooth(0)

    for m in fg_m:
        m.wait_recv()
    fg[1 : Z + 1, 7, :] = xr_fg[0]
    fg[1 : Z + 1, 8 + X, :] = xr_fg[1]
    unpack(rt_fg, yr_fg)

    def swap(x):
        return jnp.where(evenc, pltpu.roll(x, L - 1, 1), pltpu.roll(x, 1, 1))

    def restrict(b, _):
        total = None
        for p in range(2):
            z = 2 * b + p
            g = fg[z + 1, 8 : 8 + X, :]
            h = halo(rt_fg, p * X, X, b)
            n = fg[z, 8 : 8 + X, :] + fg[z + 2, 8 : 8 + X, :]
            n += fg[z + 1, 7 : 7 + X, :] + fg[z + 1, 9 : 9 + X, :]
            n += before(g, h, lane) + after(g, h, lane)
            ab[0, z, 0:X, :] = g + n * ns[z]
            total = n if p == 0 else total + n
        tmp[b] = total
        u = tmp[b, pl.ds(0, XC, 2), :] + tmp[b, pl.ds(1, XC, 2), :]
        u = u + swap(u)
        cr[b] = u
        v = u * cd[b]
        v1[b + 1, 8 : 8 + XC, :] = v
        xs_v1[0, pl.ds(b, 1), :] = v[0:1]
        xs_v1[1, pl.ds(b, 1), :] = v[XC - 1 : XC]
        return 0

    lax.fori_loop(0, ZC, restrict, 0)

    def coarse_exchange(v, xs, xr, ys, yr):
        packed = jnp.zeros((L, L), F32)
        for q in range(NBC):
            packed = put(packed, v[1 + PC * q : 1 + PC * (q + 1), 8 : 8 + XC, :].reshape(L, L), q)
        ys[...] = packed.T[:8]
        mid = pl.ds(8, XC)
        sent = [
            message(ys, yr.at[0], "gy", 1),
            message(ys, yr.at[1], "gy", -1),
            message(xs.at[1], xr.at[0], "gx", 1),
            message(xs.at[0], xr.at[1], "gx", -1),
            message(v.at[ZC, mid, :], v.at[0, mid, :], "gz", 1),
            message(v.at[1, mid, :], v.at[ZC + 1, mid, :], "gz", -1),
        ]
        for m in sent:
            m.start()
        return sent

    def coarse_arrive(sent, v, xr, yr, rt):
        for m in sent:
            m.wait_recv()
        v[1 : ZC + 1, 7, :] = xr[0]
        v[1 : ZC + 1, 8 + XC, :] = xr[1]
        unpack(rt, yr)

    def around(v, wy, rt, b):
        c = v[b + 1, 8 : 8 + XC, :]
        h = pltpu.roll(rt[pl.ds(pl.multiple_of((b % PC) * XC, XC), XC), :], L - 1 - 2 * (b // PC), 1)
        w = jnp.where(evenc, before(c, h, lanec), after(c, h, lanec))
        wy[b] = w
        n = v[b, 8 : 8 + XC, :] + v[b + 2, 8 : 8 + XC, :]
        n += v[b + 1, 7 : 7 + XC, :] + v[b + 1, 9 : 9 + XC, :]
        return c, n + (w + swap(w))

    v1_m = coarse_exchange(v1, xs_v1, xr_v1, ys_v1, yr_v1)
    smooth(1)
    coarse_arrive(v1_m, v1, xr_v1, yr_v1, rt_v1)

    def first(b, sums):
        g1, g2, h11, h12 = sums
        c, n = around(v1, wy1, rt_v1, b)
        r = cr[b]
        a = r - n
        a1s[b] = a
        w = a * cd[b]
        v2[b + 1, 8 : 8 + XC, :] = w
        xs_v2[0, pl.ds(b, 1), :] = w[0:1]
        xs_v2[1, pl.ds(b, 1), :] = w[XC - 1 : XC]
        return g1 + c * r, g2 + w * r, h11 + c * a, h12 + w * a

    sums = lax.fori_loop(0, ZC, first, (zero_coarse,) * 4)
    v2_m = coarse_exchange(v2, xs_v2, xr_v2, ys_v2, yr_v2)
    smooth(2)
    coarse_arrive(v2_m, v2, xr_v2, yr_v2, rt_v2)

    def second(b, h22):
        c, n = around(v2, wy2, rt_v2, b)
        return h22 + c * (a1s[b] - n)

    sums += (lax.fori_loop(0, ZC, second, zero_coarse),)

    row = jnp.zeros((1, L), F32)
    for i, s in enumerate(sums):
        one = jnp.sum(jnp.sum(s, axis=0, keepdims=True), axis=1, keepdims=True)
        row = jnp.where(iota((1, L), 1) == i, one, row)
    ar1[0] = row

    def spread_round(buf, others, base):
        copies = [
            pltpu.make_async_remote_copy(
                src_ref=buf.at[0], dst_ref=buf.at[d + 1], send_sem=ar_send.at[base + d],
                recv_sem=ar_recv.at[base + d], device_id=other, device_id_type=MESH,
            )
            for d, other in enumerate(others)
        ]
        for copy in copies:
            copy.start()
        return copies

    round1 = spread_round(ar1, partners, 0)

    def prolong(v, wy, j):
        def body(b, _):
            w = 3.0 * v[b + 1, 8 : 8 + XC, :] + wy[b]
            for px in range(2):
                wx = w + v[b + 1, 7 + 2 * px : 7 + 2 * px + XC, :]
                for pz in range(2):
                    z = 2 * b + pz
                    n = wx + v[b + 2 * pz, 8 : 8 + XC, :]
                    ab[j, z, pl.ds(px, XC, 2), :] = n * ns[z, pl.ds(px, XC, 2), :]
            return 0

        lax.fori_loop(0, ZC, body, 0)

    prolong(v1, wy1, 1)
    prolong(v2, wy2, 2)

    def fill(j):
        def body(b, packed):
            block = []
            for p in range(2):
                z = 2 * b + p
                x = ab[j, z, 0:X, :]
                xs_ab[j, pl.ds(z, 1), :] = x[0:1]
                block.append(x)
            return put(packed, jnp.concatenate(block, axis=0), j * NB + b)

        return body

    packed = jnp.zeros((L, L), F32)
    for j in range(3):
        packed = lax.fori_loop(0, NB, fill(j), packed)
    ys_ab[...] = packed.T[: 6 * NB]
    ab_m = [
        message(ab.at[:, 0, pl.ds(0, X), :], ab.at[:, Z, pl.ds(0, X), :], "gz", -1),
        message(xs_ab, xr_ab, "gx", -1),
        message(ys_ab, yr_ab, "gy", -1),
    ]
    for m in ab_m:
        m.start()

    for copy in round1:
        copy.wait_recv()
    ar2[0] = jnp.sum(ar1[...], axis=0)
    round2 = spread_round(ar2, plane, len(partners))

    for m in ab_m:
        m.wait_recv()
    ab[:, 0:Z, X, :] = xr_ab[...]
    rt_ab[...] = jnp.concatenate(
        [pltpu.roll(yr_ab[...], 6 * NB - 1, 0), jnp.zeros((L - 6 * NB, L), F32)], axis=0
    ).T

    for copy in round2:
        copy.wait_recv()
    total = jnp.sum(ar2[...], axis=0)
    g1, g2, h11, h12, h22 = (
        jnp.sum(jnp.where(iota((1, L), 1) == i, total, 0.0), axis=1, keepdims=True) for i in range(5)
    )
    c2 = (g2 - h12 * g1 / h11) / (h22 - h12 * h12 / h11)
    c1 = (g1 - h12 * c2) / h11

    def combine(z, _):
        ff[z, 0:X, :] = ab[0, z, 0:X, :] + c1 * ab[1, z, 0:X, :] + c2 * ab[2, z, 0:X, :]
        return 0

    lax.fori_loop(0, Z + 1, combine, 0)
    ff[0:Z, X, :] = ab[0, 0:Z, X, :] + c1 * ab[1, 0:Z, X, :] + c2 * ab[2, 0:Z, X, :]
    rt = rt_ab[...]
    rt_ab[...] = rt + c1 * pltpu.roll(rt, L - 2 * NB, 1) + c2 * pltpu.roll(rt, L - 4 * NB, 1)

    def store(b):
        part = pl.ds(2 * b, 2)
        return pltpu.make_async_copy(res.at[:, part], out_h.at[:, part], out_sem.at[b])

    def finish(b, _):
        for p in range(2):
            z = 2 * b + p
            f = ff[z, 0:X, :]
            h = halo(rt_ab, p * X, X, b)
            res[0, z] = res[0, z] + (ff[z + 1, 0:X, :] - f)
            res[1, z] = res[1, z] + (ff[z, 1 : X + 1, :] - f)
            res[2, z] = res[2, z] + (after(f, h, lane) - f)
        store(b).start()
        return 0

    lax.fori_loop(0, NB, finish, 0)

    for m in used:
        m.wait_send()
    for copy in round1 + round2:
        copy.wait_send()
    for b in range(NB):
        store(b).wait()


def solution(mesh):
    sizes = dict(mesh.shape)
    n_ar = sizes["gz"] - 1 + sizes["gx"] * sizes["gy"] - 1

    def local(residual, edge_diag, node_shift, coarse_shift):
        _, Z, X, Y = residual.shape
        ZC, XC, NB = Z // 2, X // 2, Z // 2
        assert X == 64 and Y == L and Z % 8 == 0

        def v(*shape):
            return pltpu.VMEM(shape, F32)

        scratch = [
            v(3, Z, X, L), v(3, Z, X, L), v(Z, X, L), v(ZC, XC, L // 2),
            v(3, Z + 2, X + 16, L), v(Z + 2, X + 16, L), v(ZC, X, L),
            v(ZC, XC, L), v(ZC, XC, L),
            v(ZC + 2, XC + 16, L), v(ZC + 2, XC + 16, L),
            v(ZC, XC, L), v(ZC, XC, L), v(ZC, XC, L),
            v(3, Z + 1, X + 8, L), v(Z + 1, X + 8, L),
            v(L, L), v(L, L), v(L, L), v(L, L), v(L, L),
            v(2, 3, Z, L), v(2, 3, Z, L), v(2, Z, L), v(2, Z, L),
            v(2, ZC, L), v(2, ZC, L), v(2, ZC, L), v(2, ZC, L), v(3, Z, L), v(3, Z, L),
            v(6 * NB, L), v(2, 6 * NB, L), v(2 * NB, L), v(2, 2 * NB, L),
            v(8, L), v(2, 8, L), v(8, L), v(2, 8, L), v(6 * NB, L), v(6 * NB, L),
            v(sizes["gz"], 1, L), v(sizes["gx"] * sizes["gy"], 1, L),
            pltpu.SemaphoreType.DMA((8,)), pltpu.SemaphoreType.DMA((NB,)),
            pltpu.SemaphoreType.DMA((32,)), pltpu.SemaphoreType.DMA((32,)),
            pltpu.SemaphoreType.DMA((n_ar,)), pltpu.SemaphoreType.DMA((n_ar,)),
        ]
        return pl.pallas_call(
            functools.partial(kernel, sizes),
            out_shape=jax.ShapeDtypeStruct(residual.shape, F32),
            in_specs=[pl.BlockSpec(memory_space=pl.ANY)] * 4,
            out_specs=pl.BlockSpec(memory_space=pl.ANY),
            scratch_shapes=scratch,
            compiler_params=pltpu.CompilerParams(
                collective_id=0, has_side_effects=True, vmem_limit_bytes=48 * 1024 * 1024
            ),
        )(residual, edge_diag, node_shift, coarse_shift)

    fine, coarse = P(None, "gz", "gx", "gy"), P("gz", "gx", "gy")
    return jax.shard_map(
        local, mesh=mesh, in_specs=(fine, fine, coarse, coarse), out_specs=fine, check_vma=False
    )
```

```python
import functools

import jax
import jax.numpy as jnp
from jax import lax
from jax.experimental import pallas as pl
from jax.experimental.pallas import tpu as pltpu
from jax.sharding import PartitionSpec as P

MESH = pl.DeviceIdType.MESH
AXES = ("gx", "gy", "gz")
L = 128
F32 = jnp.float32


def iota(shape, dim):
    return lax.broadcasted_iota(jnp.int32, shape, dim)


class Message:
    def __init__(self, copy, sends, receives):
        self.copy, self.sends, self.receives = copy, sends, receives

    def start(self):
        pl.when(self.sends)(lambda: self.copy.start())

    def wait_recv(self):
        pl.when(self.receives)(lambda: self.copy.wait_recv())

    def wait_send(self):
        pl.when(self.sends)(lambda: self.copy.wait_send())


def kernel(
    sizes, res_h, ed_h, ns_h, cs_h, out,
    res, ed, ns, cs, sc, fg, tmp, cr, cd, v1, v2, wy1, wy2, a1s, ab, face_e, face_r,
    rt_g, rt_sc, rt_fg, rt_v1, rt_v2, rt_ab,
    xs_sc, xr_sc, xs_fg, xr_fg, xs_v1, xr_v1, xs_v2, xr_v2, xs_ab, xr_ab,
    ys_sc, yr_sc, ys_fg, yr_fg, ys_v1, yr_v1, ys_v2, yr_v2, ys_ab, yr_ab,
    ar1, ar2, in_sem, send_sem, recv_sem, ar_send, ar_recv,
):
    _, Z, X, _ = res.shape
    ZC, XC = Z // 2, X // 2
    NB = Z // 2
    PC = L // XC
    NBC = ZC // PC
    me = {a: lax.axis_index(a) for a in AXES}
    used = []

    def message(src, dst, axis, step):
        i = len(used)
        last = sizes[axis] - 1
        copy = pltpu.make_async_remote_copy(
            src_ref=src, dst_ref=dst, send_sem=send_sem.at[i], recv_sem=recv_sem.at[i],
            device_id={axis: me[axis] + step}, device_id_type=MESH,
        )
        low, high = me[axis] > 0, me[axis] < last
        made = Message(copy, *((high, low) if step > 0 else (low, high)))
        used.append(made)
        return made

    def load(i, pick, into):
        return (
            pltpu.make_async_copy(pick(ed_h), into(ed, face_e), in_sem.at[2 * i]),
            pltpu.make_async_copy(pick(res_h), into(res, face_r), in_sem.at[2 * i + 1]),
        )

    loads = [
        load(0, lambda h: h.at[0, Z - 1], lambda v, f: v.at[0, Z - 1]),
        load(1, lambda h: h.at[1, :, pl.ds(X - 8, 8), :], lambda v, f: f),
        load(2, lambda h: h.at[2], lambda v, f: v.at[2]),
        load(3, lambda h: h.at[1], lambda v, f: v.at[1]),
        load(4, lambda h: h.at[0, pl.ds(0, Z - 1)], lambda v, f: v.at[0, pl.ds(0, Z - 1)]),
    ]
    load_ns = pltpu.make_async_copy(ns_h, ns, in_sem.at[10])
    load_cs = pltpu.make_async_copy(cs_h, cs, in_sem.at[11])
    for pair in loads:
        for copy in pair:
            copy.start()
    load_ns.start()
    load_cs.start()

    partners = [{"gz": lax.rem(me["gz"] + d, sizes["gz"])} for d in range(1, sizes["gz"])]
    plane = [
        {"gx": lax.rem(me["gx"] + dx, sizes["gx"]), "gy": lax.rem(me["gy"] + dy, sizes["gy"])}
        for dx in range(sizes["gx"]) for dy in range(sizes["gy"]) if dx or dy
    ]
    near = [partners[0], partners[-1], *(
        {"gx": lax.rem(me["gx"] + d, sizes["gx"])} for d in (1, sizes["gx"] - 1)
    ), *({"gy": lax.rem(me["gy"] + d, sizes["gy"])} for d in (1, sizes["gy"] - 1))]
    barrier = pltpu.get_barrier_semaphore()
    for other in partners + plane:
        pl.semaphore_signal(barrier, inc=1, device_id=other, device_id_type=MESH)

    zero_plane = jnp.zeros((X, L), F32)
    zero_coarse = jnp.zeros((XC, L), F32)
    for k in range(3):
        for z in (0, Z + 1):
            sc[k, z, 8 : 8 + X, :] = zero_plane
        ab[k, Z, 0:X, :] = zero_plane
    for z in (0, Z + 1):
        fg[z, 8 : 8 + X, :] = zero_plane
    for z in (0, ZC + 1):
        v1[z, 8 : 8 + XC, :] = zero_coarse
        v2[z, 8 : 8 + XC, :] = zero_coarse
    for ref in (xr_sc, xr_fg, xr_v1, xr_v2, xr_ab, yr_sc, yr_fg, yr_v1, yr_v2, yr_ab):
        ref[...] = jnp.zeros(ref.shape, F32)

    for other in near:
        pl.semaphore_signal(barrier, inc=1, device_id=other, device_id_type=MESH)

    lane = iota((X, L), 1)
    lane2 = iota((L, L), 1)
    lanec = iota((XC, L), 1)
    evenc = lanec % 2 == 0

    def put(packed, block, q):
        return jnp.where(lax.shift_right_logical(lane2, 1) == q, pltpu.roll(block, 2 * q + 1, 1), packed)

    def halo(rt, row, rows, q):
        return pltpu.roll(rt[pl.ds(row, rows), :], L - 1 - 2 * q, 1)

    def before(x, h, at):
        return jnp.where(at == 0, h, pltpu.roll(x, 1, 1))

    def after(x, h, at):
        return jnp.where(at == L - 1, h, pltpu.roll(x, L - 1, 1))

    def unpack(rt, low, high):
        n = low.shape[0]
        mixed = jnp.where(iota((n, L), 0) % 2 == 1, pltpu.roll(low, 1, 0), pltpu.roll(high, n - 1, 0))
        rt[...] = jnp.concatenate([mixed, jnp.zeros((L - n, L), F32)], axis=0).T

    def each(n, body, init):
        return lax.fori_loop(0, n, body, init, unroll=True)

    inner = pl.ds(8, X)
    third = 2 * NB
    sc_zu0 = message(sc.at[0, Z, inner, :], sc.at[0, 0, inner, :], "gz", 1)
    sc_xu1 = message(xs_sc.at[1, 1], xr_sc.at[0, 1], "gx", 1)
    sc_yu2 = message(ys_sc.at[pl.ds(2 * third, third)], yr_sc.at[0, pl.ds(2 * third, third)], "gy", 1)
    rest = [
        message(xs_sc.at[1, 0], xr_sc.at[0, 0], "gx", 1),
        message(xs_sc.at[1, 2], xr_sc.at[0, 2], "gx", 1),
        message(xs_sc.at[0], xr_sc.at[1], "gx", -1),
        message(ys_sc.at[pl.ds(0, 2 * third)], yr_sc.at[0, pl.ds(0, 2 * third)], "gy", 1),
        message(ys_sc, yr_sc.at[1], "gy", -1),
        message(sc.at[1:3, Z, inner, :], sc.at[1:3, 0, inner, :], "gz", 1),
        message(sc.at[:, 1, inner, :], sc.at[:, Z + 1, inner, :], "gz", -1),
    ]

    def arrived(i):
        for copy in loads[i]:
            copy.wait()

    def scale(k, z):
        r = 1.0 / ed[k, z]
        ed[k, z] = r
        s = res[k, z] * r
        sc[k, z + 1, 8 : 8 + X, :] = s
        xs_sc[0, k, pl.ds(z, 1), :] = s[0:1]
        if k != 1:
            xs_sc[1, k, pl.ds(z, 1), :] = s[X - 1 : X]
        return s

    def scale_all(k, packed, first):
        def body(b, packed):
            block = []
            for p in range(2):
                z = 2 * b + p
                block.append(scale(k, z))
            return put(packed, jnp.concatenate(block, axis=0), first + b)

        return each(NB, body, packed)

    arrived(0)
    scale(0, Z - 1)
    arrived(1)
    xs_sc[1, 1] = face_r[:, 7, :] * (1.0 / face_e[:, 7, :])
    arrived(2)
    ys_sc[2 * third :] = scale_all(2, jnp.zeros((L, L), F32), 0).T[:third]
    pl.semaphore_wait(barrier, len(partners) + len(plane) + len(near))
    for m in (sc_yu2, sc_xu1, sc_zu0):
        m.start()
    arrived(3)
    packed = scale_all(1, jnp.zeros((L, L), F32), NB)
    arrived(4)

    def bulk(b, packed):
        block = [scale(0, 2 * b), scale(0, 2 * b + 1)]
        return put(packed, jnp.concatenate(block, axis=0), b)

    packed = each(NB - 1, bulk, packed)
    block = [scale(0, Z - 2), sc[0, Z, 8 : 8 + X, :]]
    packed = put(packed, jnp.concatenate(block, axis=0), NB - 1)
    ys_sc[0 : 2 * third] = packed.T[: 2 * third]
    for m in rest:
        m.start()

    load_ns.wait()
    load_cs.wait()

    def invert(z, _):
        ns[z] = 1.0 / (6.0 + ns[z])
        return 0

    lax.fori_loop(0, Z, invert, 0, unroll=2)
    twice = (iota((L // 2, L), 0) == iota((L // 2, L), 1) // 2).astype(F32)
    wide = jnp.dot(
        cs[...].reshape(ZC * XC, L // 2), twice,
        precision=lax.Precision.HIGHEST, preferred_element_type=F32,
    )
    cd[...] = (1.0 / (6.0 + wide)).reshape(ZC, XC, L)

    for m in (sc_yu2, sc_xu1, sc_zu0):
        m.wait_recv()
    sc[1, 1 : Z + 1, 7, :] = xr_sc[0, 1]
    low = yr_sc[0, 2 * third :]
    unpack(rt_g, low, jnp.zeros_like(low))

    def guess(b, packed):
        block = []
        for p in range(2):
            z = 2 * b + p
            s0, s0m = sc[0, z + 1, 8 : 8 + X, :], sc[0, z, 8 : 8 + X, :]
            s1, s1m = sc[1, z + 1, 8 : 8 + X, :], sc[1, z + 1, 7 : 7 + X, :]
            s2 = sc[2, z + 1, 8 : 8 + X, :]
            s2m = before(s2, halo(rt_g, p * X, X, b), lane)
            g = ((s0m - s0) + (s1m - s1) + (s2m - s2)) * ns[z]
            fg[z + 1, 8 : 8 + X, :] = g
            xs_fg[0, pl.ds(z, 1), :] = g[0:1]
            xs_fg[1, pl.ds(z, 1), :] = g[X - 1 : X]
            block.append(g)
        return put(packed, jnp.concatenate(block, axis=0), b)

    packed = each(NB, guess, jnp.zeros((L, L), F32))
    ys_fg[...] = packed.T[: 2 * NB]
    fg_m = [
        message(ys_fg, yr_fg.at[0], "gy", 1),
        message(ys_fg, yr_fg.at[1], "gy", -1),
        message(xs_fg.at[1], xr_fg.at[0], "gx", 1),
        message(xs_fg.at[0], xr_fg.at[1], "gx", -1),
        message(fg.at[Z, inner, :], fg.at[0, inner, :], "gz", 1),
        message(fg.at[1, inner, :], fg.at[Z + 1, inner, :], "gz", -1),
    ]
    for m in fg_m:
        m.start()

    for m in fg_m:
        m.wait_recv()
    fg[1 : Z + 1, 7, :] = xr_fg[0]
    fg[1 : Z + 1, 8 + X, :] = xr_fg[1]
    unpack(rt_fg, yr_fg[0], yr_fg[1])

    def swap(x):
        return jnp.where(evenc, pltpu.roll(x, L - 1, 1), pltpu.roll(x, 1, 1))

    def restrict(b, _):
        total = None
        for p in range(2):
            z = 2 * b + p
            g = fg[z + 1, 8 : 8 + X, :]
            h = halo(rt_fg, p * X, X, b)
            n = fg[z, 8 : 8 + X, :] + fg[z + 2, 8 : 8 + X, :]
            n += fg[z + 1, 7 : 7 + X, :] + fg[z + 1, 9 : 9 + X, :]
            n += before(g, h, lane) + after(g, h, lane)
            ab[0, z, 0:X, :] = g + n * ns[z]
            total = n if p == 0 else total + n
        tmp[b] = total
        return 0

    each(ZC, restrict, 0)

    def direction(b, _):
        u = tmp[b, pl.ds(0, XC, 2), :] + tmp[b, pl.ds(1, XC, 2), :]
        u = u + swap(u)
        cr[b] = u
        v = u * cd[b]
        v1[b + 1, 8 : 8 + XC, :] = v
        xs_v1[0, pl.ds(b, 1), :] = v[0:1]
        xs_v1[1, pl.ds(b, 1), :] = v[XC - 1 : XC]
        return 0

    each(ZC, direction, 0)

    def coarse_exchange(v, xs, xr, ys, yr):
        packed = jnp.zeros((L, L), F32)
        for q in range(NBC):
            packed = put(packed, v[1 + PC * q : 1 + PC * (q + 1), 8 : 8 + XC, :].reshape(L, L), q)
        ys[...] = packed.T[:8]
        mid = pl.ds(8, XC)
        sent = [
            message(ys, yr.at[0], "gy", 1),
            message(ys, yr.at[1], "gy", -1),
            message(xs.at[1], xr.at[0], "gx", 1),
            message(xs.at[0], xr.at[1], "gx", -1),
            message(v.at[ZC, mid, :], v.at[0, mid, :], "gz", 1),
            message(v.at[1, mid, :], v.at[ZC + 1, mid, :], "gz", -1),
        ]
        for m in sent:
            m.start()
        return sent

    def coarse_arrive(sent, v, xr, yr, rt):
        for m in sent:
            m.wait_recv()
        v[1 : ZC + 1, 7, :] = xr[0]
        v[1 : ZC + 1, 8 + XC, :] = xr[1]
        unpack(rt, yr[0], yr[1])

    def around(v, wy, rt, b):
        c = v[b + 1, 8 : 8 + XC, :]
        h = halo(rt, (b % PC) * XC, XC, b // PC)
        w = jnp.where(evenc, before(c, h, lanec), after(c, h, lanec))
        wy[b] = w
        n = v[b, 8 : 8 + XC, :] + v[b + 2, 8 : 8 + XC, :]
        n += v[b + 1, 7 : 7 + XC, :] + v[b + 1, 9 : 9 + XC, :]
        return c, n + (w + swap(w))

    v1_m = coarse_exchange(v1, xs_v1, xr_v1, ys_v1, yr_v1)
    coarse_arrive(v1_m, v1, xr_v1, yr_v1, rt_v1)

    def first(b, sums):
        g1, g2, h11, h12 = sums
        c, n = around(v1, wy1, rt_v1, b)
        r = cr[b]
        a = r - n
        a1s[b] = a
        w = a * cd[b]
        v2[b + 1, 8 : 8 + XC, :] = w
        xs_v2[0, pl.ds(b, 1), :] = w[0:1]
        xs_v2[1, pl.ds(b, 1), :] = w[XC - 1 : XC]
        return g1 + c * r, g2 + w * r, h11 + c * a, h12 + w * a

    sums = each(ZC, first, (zero_coarse,) * 4)
    v2_m = coarse_exchange(v2, xs_v2, xr_v2, ys_v2, yr_v2)
    coarse_arrive(v2_m, v2, xr_v2, yr_v2, rt_v2)

    def second(b, h22):
        c, n = around(v2, wy2, rt_v2, b)
        return h22 + c * (a1s[b] - n)

    sums += (each(ZC, second, zero_coarse),)

    row = jnp.zeros((1, L), F32)
    for i, s in enumerate(sums):
        one = jnp.sum(jnp.sum(s, axis=0, keepdims=True), axis=1, keepdims=True)
        row = jnp.where(iota((1, L), 1) == i, one, row)
    ar1[0] = row

    def spread_round(buf, others, base):
        copies = [
            pltpu.make_async_remote_copy(
                src_ref=buf.at[0], dst_ref=buf.at[d + 1], send_sem=ar_send.at[base + d],
                recv_sem=ar_recv.at[base + d], device_id=other, device_id_type=MESH,
            )
            for d, other in enumerate(others)
        ]
        for copy in copies:
            copy.start()
        return copies

    round1 = spread_round(ar1, partners, 0)

    def prolong(v, wy, j):
        def body(b, _):
            w = 3.0 * v[b + 1, 8 : 8 + XC, :] + wy[b]
            for px in range(2):
                wx = w + v[b + 1, 7 + 2 * px : 7 + 2 * px + XC, :]
                for pz in range(2):
                    z = 2 * b + pz
                    n = wx + v[b + 2 * pz, 8 : 8 + XC, :]
                    ab[j, z, pl.ds(px, XC, 2), :] = n * ns[z, pl.ds(px, XC, 2), :]
            return 0

        each(ZC, body, 0)

    prolong(v1, wy1, 1)
    prolong(v2, wy2, 2)

    def fill(j):
        def body(b, packed):
            block = []
            for p in range(2):
                z = 2 * b + p
                x = ab[j, z, 0:X, :]
                xs_ab[j, pl.ds(z, 1), :] = x[0:1]
                block.append(x)
            return put(packed, jnp.concatenate(block, axis=0), j * NB + b)

        return body

    packed = jnp.zeros((L, L), F32)
    for j in range(3):
        packed = each(NB, fill(j), packed)
    ys_ab[...] = packed.T[: 6 * NB]
    ab_m = [
        message(ab.at[:, 0, pl.ds(0, X), :], ab.at[:, Z, pl.ds(0, X), :], "gz", -1),
        message(xs_ab, xr_ab, "gx", -1),
        message(ys_ab, yr_ab, "gy", -1),
    ]
    for m in ab_m:
        m.start()

    def smooth(k):
        def body(b, _):
            for p in range(2):
                z = 2 * b + p
                s = sc[k, z + 1, 8 : 8 + X, :]
                h = halo(rt_sc, p * X, X, k * NB + b)
                n = sc[k, z, 8 : 8 + X, :] + sc[k, z + 2, 8 : 8 + X, :]
                n += sc[k, z + 1, 7 : 7 + X, :] + sc[k, z + 1, 9 : 9 + X, :]
                n += before(s, h, lane) + after(s, h, lane)
                out[k, z] = s + n * ed[k, z]
            return 0

        each(NB, body, 0)

    def fill_rows():
        for m in rest:
            m.wait_recv()
        for k in range(3):
            if k != 1:
                sc[k, 1 : Z + 1, 7, :] = xr_sc[0, k]
            sc[k, 1 : Z + 1, 8 + X, :] = xr_sc[1, k]
        unpack(rt_sc, yr_sc[0], yr_sc[1])

    fill_rows()
    smooth(0)

    for copy in round1:
        copy.wait_recv()
    ar2[0] = jnp.sum(ar1[...], axis=0)
    round2 = spread_round(ar2, plane, len(partners))

    smooth(1)
    smooth(2)
    for m in ab_m:
        m.wait_recv()
    ab[:, 0:Z, X, :] = xr_ab[...]
    rt_ab[...] = jnp.concatenate(
        [pltpu.roll(yr_ab[...], 6 * NB - 1, 0), jnp.zeros((L - 6 * NB, L), F32)], axis=0
    ).T

    def gradient(j, into, add):
        def body(b, _):
            for p in range(2):
                z = 2 * b + p
                f = ab[j, z, 0:X, :]
                h = halo(rt_ab, p * X, X, j * NB + b)
                d = (ab[j, z + 1, 0:X, :] - f, ab[j, z, 1 : X + 1, :] - f, after(f, h, lane) - f)
                for k in range(3):
                    into[k, z] = into[k, z] + d[k] if add else d[k]
            return 0

        each(NB, body, 0)

    gradient(0, out, True)
    gradient(1, res, False)
    gradient(2, ed, False)

    for copy in round2:
        copy.wait_recv()
    total = jnp.sum(ar2[...], axis=0)
    g1, g2, h11, h12, h22 = (
        jnp.sum(jnp.where(iota((1, L), 1) == i, total, 0.0), axis=1, keepdims=True) for i in range(5)
    )
    c2 = (g2 - h12 * g1 / h11) / (h22 - h12 * h12 / h11)
    c1 = (g1 - h12 * c2) / h11

    def finish(z, _):
        for k in range(3):
            out[k, z] = out[k, z] + c1 * res[k, z] + c2 * ed[k, z]
        return 0

    lax.fori_loop(0, Z, finish, 0, unroll=2)

    for m in used:
        m.wait_send()
    for copy in round1 + round2:
        copy.wait_send()


def solution(mesh):
    sizes = dict(mesh.shape)
    n_ar = sizes["gz"] - 1 + sizes["gx"] * sizes["gy"] - 1

    def local(residual, edge_diag, node_shift, coarse_shift):
        _, Z, X, Y = residual.shape
        ZC, XC, NB = Z // 2, X // 2, Z // 2
        assert X == 64 and Y == L and Z % 8 == 0

        def v(*shape):
            return pltpu.VMEM(shape, F32)

        scratch = [
            v(3, Z, X, L), v(3, Z, X, L), v(Z, X, L), v(ZC, XC, L // 2),
            v(3, Z + 2, X + 16, L), v(Z + 2, X + 16, L), v(ZC, X, L),
            v(ZC, XC, L), v(ZC, XC, L),
            v(ZC + 2, XC + 16, L), v(ZC + 2, XC + 16, L),
            v(ZC, XC, L), v(ZC, XC, L), v(ZC, XC, L),
            v(3, Z + 1, X + 8, L), v(Z, 8, L), v(Z, 8, L),
            v(L, L), v(L, L), v(L, L), v(L, L), v(L, L), v(L, L),
            v(2, 3, Z, L), v(2, 3, Z, L), v(2, Z, L), v(2, Z, L),
            v(2, ZC, L), v(2, ZC, L), v(2, ZC, L), v(2, ZC, L), v(3, Z, L), v(3, Z, L),
            v(6 * NB, L), v(2, 6 * NB, L), v(2 * NB, L), v(2, 2 * NB, L),
            v(8, L), v(2, 8, L), v(8, L), v(2, 8, L), v(6 * NB, L), v(6 * NB, L),
            v(sizes["gz"], 1, L), v(sizes["gx"] * sizes["gy"], 1, L),
            pltpu.SemaphoreType.DMA((12,)),
            pltpu.SemaphoreType.DMA((32,)), pltpu.SemaphoreType.DMA((32,)),
            pltpu.SemaphoreType.DMA((n_ar,)), pltpu.SemaphoreType.DMA((n_ar,)),
        ]
        return pl.pallas_call(
            functools.partial(kernel, sizes),
            out_shape=jax.ShapeDtypeStruct(residual.shape, F32),
            in_specs=[pl.BlockSpec(memory_space=pl.ANY)] * 4,
            out_specs=pl.BlockSpec(memory_space=pltpu.VMEM),
            scratch_shapes=scratch,
            compiler_params=pltpu.CompilerParams(
                collective_id=0, has_side_effects=True, vmem_limit_bytes=48 * 1024 * 1024
            ),
        )(*(
            pltpu.with_memory_space_constraint(x, pltpu.HBM)
            for x in (residual, edge_diag, node_shift, coarse_shift)
        ))

    fine, coarse = P(None, "gz", "gx", "gy"), P("gz", "gx", "gy")
    return jax.shard_map(
        local, mesh=mesh, in_specs=(fine, fine, coarse, coarse), out_specs=fine, check_vma=False
    )
```

```python
import functools

import jax
import jax.numpy as jnp
from jax import lax
from jax.experimental import pallas as pl
from jax.experimental.pallas import tpu as pltpu
from jax.sharding import PartitionSpec as P

MESH = pl.DeviceIdType.MESH
AXES = ("gx", "gy", "gz")
L = 128
F32 = jnp.float32


def iota(shape, dim):
    return lax.broadcasted_iota(jnp.int32, shape, dim)


class Message:
    def __init__(self, copy, sends, receives):
        self.copy, self.sends, self.receives = copy, sends, receives

    def start(self):
        pl.when(self.sends)(lambda: self.copy.start())

    def wait_recv(self):
        pl.when(self.receives)(lambda: self.copy.wait_recv())

    def wait_send(self):
        pl.when(self.sends)(lambda: self.copy.wait_send())


def kernel(
    sizes, res_h, ed_h, ns_h, cs_h, out,
    res, ed, ns, cs, sc, fg, tmp, cr, cd, v1, v2, wy1, wy2, a1s, ab, face_e, face_r,
    rt_g, rt_sc, rt_fg, rt_v1, rt_v2, rt_ab,
    xs_sc, xr_sc, xs_fg, xr_fg, xs_v1, xr_v1, xs_v2, xr_v2, xs_ab, xr_ab,
    ys_sc, yr_sc, ys_fg, yr_fg, ys_v1, yr_v1, ys_v2, yr_v2, ys_ab, yr_ab,
    ar1, ar2, present, in_sem, send_sem, recv_sem, ar_send, ar_recv,
):
    _, Z, X, _ = res.shape
    ZC, XC = Z // 2, X // 2
    NB = Z // 2
    PC = L // XC
    NBC = ZC // PC
    me = {a: lax.axis_index(a) for a in AXES}
    used = []

    def message(src, dst, axis, step):
        i = len(used)
        last = sizes[axis] - 1
        copy = pltpu.make_async_remote_copy(
            src_ref=src, dst_ref=dst, send_sem=send_sem.at[i], recv_sem=recv_sem.at[i],
            device_id={axis: me[axis] + step}, device_id_type=MESH,
        )
        low, high = me[axis] > 0, me[axis] < last
        made = Message(copy, *((high, low) if step > 0 else (low, high)))
        used.append(made)
        return made

    def load(i, pick, into):
        return (
            pltpu.make_async_copy(pick(ed_h), into(ed, face_e), in_sem.at[2 * i]),
            pltpu.make_async_copy(pick(res_h), into(res, face_r), in_sem.at[2 * i + 1]),
        )

    loads = [
        load(0, lambda h: h.at[0, Z - 1], lambda v, f: v.at[0, Z - 1]),
        load(1, lambda h: h.at[1, :, pl.ds(X - 8, 8), :], lambda v, f: f),
        load(2, lambda h: h.at[2], lambda v, f: v.at[2]),
        load(3, lambda h: h.at[1], lambda v, f: v.at[1]),
        load(4, lambda h: h.at[0, pl.ds(0, Z - 1)], lambda v, f: v.at[0, pl.ds(0, Z - 1)]),
    ]
    load_ns = pltpu.make_async_copy(ns_h, ns, in_sem.at[10])
    load_cs = pltpu.make_async_copy(cs_h, cs, in_sem.at[11])
    for pair in loads:
        for copy in pair:
            copy.start()
    load_ns.start()
    load_cs.start()

    partners = [{"gz": lax.rem(me["gz"] + d, sizes["gz"])} for d in range(1, sizes["gz"])]
    plane = [
        {"gx": lax.rem(me["gx"] + dx, sizes["gx"]), "gy": lax.rem(me["gy"] + dy, sizes["gy"])}
        for dx in range(sizes["gx"]) for dy in range(sizes["gy"]) if dx or dy
    ]
    far = [
        {"gx": lax.rem(me["gx"] + dx, sizes["gx"]), "gy": lax.rem(me["gy"] + dy, sizes["gy"])}
        for dx in range(sizes["gx"]) for dy in range(sizes["gy"]) if (dx and dy) or dx == 2 or dy == 2
    ]
    near = [partners[0], partners[-1], *(
        {"gx": lax.rem(me["gx"] + d, sizes["gx"])} for d in (1, sizes["gx"] - 1)
    ), *({"gy": lax.rem(me["gy"] + d, sizes["gy"])} for d in (1, sizes["gy"] - 1))]
    barrier = pltpu.get_barrier_semaphore()
    for other in far:
        pl.semaphore_signal(barrier, inc=1, device_id=other, device_id_type=MESH)

    zero_plane = jnp.zeros((X, L), F32)
    zero_coarse = jnp.zeros((XC, L), F32)
    for k in range(3):
        for z in (0, Z + 1):
            sc[k, z, 8 : 8 + X, :] = zero_plane
        ab[k, Z, 0:X, :] = zero_plane
    for z in (0, Z + 1):
        fg[z, 8 : 8 + X, :] = zero_plane
    for z in (0, ZC + 1):
        v1[z, 8 : 8 + XC, :] = zero_coarse
        v2[z, 8 : 8 + XC, :] = zero_coarse
    for ref in (xr_sc, xr_fg, xr_v1, xr_v2, xr_ab, yr_sc, yr_fg, yr_v1, yr_v2, yr_ab):
        ref[...] = jnp.zeros(ref.shape, F32)

    for other in near:
        pl.semaphore_signal(barrier, inc=1, device_id=other, device_id_type=MESH)

    lane = iota((X, L), 1)
    lane2 = iota((L, L), 1)
    lanec = iota((XC, L), 1)
    evenc = lanec % 2 == 0

    def put(packed, block, q):
        return jnp.where(lax.shift_right_logical(lane2, 1) == q, pltpu.roll(block, 2 * q + 1, 1), packed)

    def halo(rt, row, rows, q):
        return pltpu.roll(rt[pl.ds(row, rows), :], L - 1 - 2 * q, 1)

    def before(x, h, at):
        return jnp.where(at == 0, h, pltpu.roll(x, 1, 1))

    def after(x, h, at):
        return jnp.where(at == L - 1, h, pltpu.roll(x, L - 1, 1))

    def unpack(rt, low, high):
        n = low.shape[0]
        mixed = jnp.where(iota((n, L), 0) % 2 == 1, pltpu.roll(low, 1, 0), pltpu.roll(high, n - 1, 0))
        rt[...] = jnp.concatenate([mixed, jnp.zeros((L - n, L), F32)], axis=0).T

    def each(n, body, init):
        return lax.fori_loop(0, n, body, init, unroll=True)

    inner = pl.ds(8, X)
    third = 2 * NB
    sc_zu0 = message(sc.at[0, Z, inner, :], sc.at[0, 0, inner, :], "gz", 1)
    sc_xu1 = message(xs_sc.at[1, 1], xr_sc.at[0, 1], "gx", 1)
    sc_yu2 = message(ys_sc.at[pl.ds(2 * third, third)], yr_sc.at[0, pl.ds(2 * third, third)], "gy", 1)
    rest = [
        message(xs_sc.at[1, 0], xr_sc.at[0, 0], "gx", 1),
        message(xs_sc.at[1, 2], xr_sc.at[0, 2], "gx", 1),
        message(xs_sc.at[0], xr_sc.at[1], "gx", -1),
        message(ys_sc.at[pl.ds(0, 2 * third)], yr_sc.at[0, pl.ds(0, 2 * third)], "gy", 1),
        message(ys_sc, yr_sc.at[1], "gy", -1),
        message(sc.at[1:3, Z, inner, :], sc.at[1:3, 0, inner, :], "gz", 1),
        message(sc.at[:, 1, inner, :], sc.at[:, Z + 1, inner, :], "gz", -1),
    ]

    def arrived(i):
        for copy in loads[i]:
            copy.wait()

    def scale(k, z):
        r = 1.0 / ed[k, z]
        ed[k, z] = r
        s = res[k, z] * r
        sc[k, z + 1, 8 : 8 + X, :] = s
        xs_sc[0, k, pl.ds(z, 1), :] = s[0:1]
        if k != 1:
            xs_sc[1, k, pl.ds(z, 1), :] = s[X - 1 : X]
        return s

    def scale_all(k, packed, first):
        def body(b, packed):
            block = []
            for p in range(2):
                z = 2 * b + p
                block.append(scale(k, z))
            return put(packed, jnp.concatenate(block, axis=0), first + b)

        return each(NB, body, packed)

    arrived(0)
    scale(0, Z - 1)
    arrived(1)
    xs_sc[1, 1] = face_r[:, 7, :] * (1.0 / face_e[:, 7, :])
    arrived(2)
    ys_sc[2 * third :] = scale_all(2, jnp.zeros((L, L), F32), 0).T[:third]
    pl.semaphore_wait(barrier, len(far) + len(near))

    def tell(i):
        for d in (1 << i, sizes["gz"] - (1 << i)):
            other = {"gz": lax.rem(me["gz"] + d, sizes["gz"])}
            pl.semaphore_signal(present.at[i], inc=1, device_id=other, device_id_type=MESH)

    def told(i):
        pl.semaphore_wait(present.at[i], 2)

    steps = [i for i in range(3) if (1 << i) < sizes["gz"] // 2]
    tell_0, tell_1, tell_2 = (i in steps for i in range(3))
    if tell_0:
        tell(0)
    for m in (sc_yu2, sc_xu1, sc_zu0):
        m.start()
    arrived(3)
    packed = scale_all(1, jnp.zeros((L, L), F32), NB)
    arrived(4)

    def bulk(b, packed):
        block = [scale(0, 2 * b), scale(0, 2 * b + 1)]
        return put(packed, jnp.concatenate(block, axis=0), b)

    packed = each(NB - 1, bulk, packed)
    block = [scale(0, Z - 2), sc[0, Z, 8 : 8 + X, :]]
    packed = put(packed, jnp.concatenate(block, axis=0), NB - 1)
    ys_sc[0 : 2 * third] = packed.T[: 2 * third]
    for m in rest:
        m.start()

    load_ns.wait()
    load_cs.wait()

    def invert(z, _):
        ns[z] = 1.0 / (6.0 + ns[z])
        return 0

    lax.fori_loop(0, Z, invert, 0, unroll=2)
    twice = (iota((L // 2, L), 0) == iota((L // 2, L), 1) // 2).astype(F32)
    wide = jnp.dot(
        cs[...].reshape(ZC * XC, L // 2), twice,
        precision=lax.Precision.HIGHEST, preferred_element_type=F32,
    )
    cd[...] = (1.0 / (6.0 + wide)).reshape(ZC, XC, L)

    for m in (sc_yu2, sc_xu1, sc_zu0):
        m.wait_recv()
    if tell_0:
        told(0)
    if tell_1:
        tell(1)
    sc[1, 1 : Z + 1, 7, :] = xr_sc[0, 1]
    low = yr_sc[0, 2 * third :]
    unpack(rt_g, low, jnp.zeros_like(low))

    def guess(b, packed):
        block = []
        for p in range(2):
            z = 2 * b + p
            s0, s0m = sc[0, z + 1, 8 : 8 + X, :], sc[0, z, 8 : 8 + X, :]
            s1, s1m = sc[1, z + 1, 8 : 8 + X, :], sc[1, z + 1, 7 : 7 + X, :]
            s2 = sc[2, z + 1, 8 : 8 + X, :]
            s2m = before(s2, halo(rt_g, p * X, X, b), lane)
            g = ((s0m - s0) + (s1m - s1) + (s2m - s2)) * ns[z]
            fg[z + 1, 8 : 8 + X, :] = g
            xs_fg[0, pl.ds(z, 1), :] = g[0:1]
            xs_fg[1, pl.ds(z, 1), :] = g[X - 1 : X]
            block.append(g)
        return put(packed, jnp.concatenate(block, axis=0), b)

    packed = each(NB, guess, jnp.zeros((L, L), F32))
    ys_fg[...] = packed.T[: 2 * NB]
    fg_m = [
        message(ys_fg, yr_fg.at[0], "gy", 1),
        message(ys_fg, yr_fg.at[1], "gy", -1),
        message(xs_fg.at[1], xr_fg.at[0], "gx", 1),
        message(xs_fg.at[0], xr_fg.at[1], "gx", -1),
        message(fg.at[Z, inner, :], fg.at[0, inner, :], "gz", 1),
        message(fg.at[1, inner, :], fg.at[Z + 1, inner, :], "gz", -1),
    ]
    for m in fg_m:
        m.start()

    for m in fg_m:
        m.wait_recv()
    if tell_1:
        told(1)
    if tell_2:
        tell(2)
    fg[1 : Z + 1, 7, :] = xr_fg[0]
    fg[1 : Z + 1, 8 + X, :] = xr_fg[1]
    unpack(rt_fg, yr_fg[0], yr_fg[1])

    def swap(x):
        return jnp.where(evenc, pltpu.roll(x, L - 1, 1), pltpu.roll(x, 1, 1))

    def restrict(b, _):
        total = None
        for p in range(2):
            z = 2 * b + p
            g = fg[z + 1, 8 : 8 + X, :]
            h = halo(rt_fg, p * X, X, b)
            n = fg[z, 8 : 8 + X, :] + fg[z + 2, 8 : 8 + X, :]
            n += fg[z + 1, 7 : 7 + X, :] + fg[z + 1, 9 : 9 + X, :]
            n += before(g, h, lane) + after(g, h, lane)
            ab[0, z, 0:X, :] = g + n * ns[z]
            total = n if p == 0 else total + n
        tmp[b] = total
        return 0

    each(ZC, restrict, 0)

    def direction(b, _):
        u = tmp[b, pl.ds(0, XC, 2), :] + tmp[b, pl.ds(1, XC, 2), :]
        u = u + swap(u)
        cr[b] = u
        v = u * cd[b]
        v1[b + 1, 8 : 8 + XC, :] = v
        xs_v1[0, pl.ds(b, 1), :] = v[0:1]
        xs_v1[1, pl.ds(b, 1), :] = v[XC - 1 : XC]
        return 0

    each(ZC, direction, 0)

    def coarse_exchange(v, xs, xr, ys, yr):
        packed = jnp.zeros((L, L), F32)
        for q in range(NBC):
            packed = put(packed, v[1 + PC * q : 1 + PC * (q + 1), 8 : 8 + XC, :].reshape(L, L), q)
        ys[...] = packed.T[:8]
        mid = pl.ds(8, XC)
        sent = [
            message(ys, yr.at[0], "gy", 1),
            message(ys, yr.at[1], "gy", -1),
            message(xs.at[1], xr.at[0], "gx", 1),
            message(xs.at[0], xr.at[1], "gx", -1),
            message(v.at[ZC, mid, :], v.at[0, mid, :], "gz", 1),
            message(v.at[1, mid, :], v.at[ZC + 1, mid, :], "gz", -1),
        ]
        for m in sent:
            m.start()
        return sent

    def coarse_arrive(sent, v, xr, yr, rt):
        for m in sent:
            m.wait_recv()
        v[1 : ZC + 1, 7, :] = xr[0]
        v[1 : ZC + 1, 8 + XC, :] = xr[1]
        unpack(rt, yr[0], yr[1])

    def around(v, wy, rt, b):
        c = v[b + 1, 8 : 8 + XC, :]
        h = halo(rt, (b % PC) * XC, XC, b // PC)
        w = jnp.where(evenc, before(c, h, lanec), after(c, h, lanec))
        wy[b] = w
        n = v[b, 8 : 8 + XC, :] + v[b + 2, 8 : 8 + XC, :]
        n += v[b + 1, 7 : 7 + XC, :] + v[b + 1, 9 : 9 + XC, :]
        return c, n + (w + swap(w))

    v1_m = coarse_exchange(v1, xs_v1, xr_v1, ys_v1, yr_v1)
    coarse_arrive(v1_m, v1, xr_v1, yr_v1, rt_v1)

    def first(b, sums):
        g1, g2, h11, h12 = sums
        c, n = around(v1, wy1, rt_v1, b)
        r = cr[b]
        a = r - n
        a1s[b] = a
        w = a * cd[b]
        v2[b + 1, 8 : 8 + XC, :] = w
        xs_v2[0, pl.ds(b, 1), :] = w[0:1]
        xs_v2[1, pl.ds(b, 1), :] = w[XC - 1 : XC]
        return g1 + c * r, g2 + w * r, h11 + c * a, h12 + w * a

    sums = each(ZC, first, (zero_coarse,) * 4)
    v2_m = coarse_exchange(v2, xs_v2, xr_v2, ys_v2, yr_v2)
    coarse_arrive(v2_m, v2, xr_v2, yr_v2, rt_v2)

    def second(b, h22):
        c, n = around(v2, wy2, rt_v2, b)
        return h22 + c * (a1s[b] - n)

    sums += (each(ZC, second, zero_coarse),)

    row = jnp.zeros((1, L), F32)
    for i, s in enumerate(sums):
        one = jnp.sum(jnp.sum(s, axis=0, keepdims=True), axis=1, keepdims=True)
        row = jnp.where(iota((1, L), 1) == i, one, row)
    ar1[0] = row

    def spread_round(buf, others, base):
        copies = [
            pltpu.make_async_remote_copy(
                src_ref=buf.at[0], dst_ref=buf.at[d + 1], send_sem=ar_send.at[base + d],
                recv_sem=ar_recv.at[base + d], device_id=other, device_id_type=MESH,
            )
            for d, other in enumerate(others)
        ]
        for copy in copies:
            copy.start()
        return copies

    round1 = spread_round(ar1, plane, 0)

    def prolong(v, wy, j):
        def body(b, _):
            w = 3.0 * v[b + 1, 8 : 8 + XC, :] + wy[b]
            for px in range(2):
                wx = w + v[b + 1, 7 + 2 * px : 7 + 2 * px + XC, :]
                for pz in range(2):
                    z = 2 * b + pz
                    n = wx + v[b + 2 * pz, 8 : 8 + XC, :]
                    ab[j, z, pl.ds(px, XC, 2), :] = n * ns[z, pl.ds(px, XC, 2), :]
            return 0

        each(ZC, body, 0)

    prolong(v1, wy1, 1)
    prolong(v2, wy2, 2)

    def fill(j):
        def body(b, packed):
            block = []
            for p in range(2):
                z = 2 * b + p
                x = ab[j, z, 0:X, :]
                xs_ab[j, pl.ds(z, 1), :] = x[0:1]
                block.append(x)
            return put(packed, jnp.concatenate(block, axis=0), j * NB + b)

        return body

    packed = jnp.zeros((L, L), F32)
    for j in range(3):
        packed = each(NB, fill(j), packed)
    ys_ab[...] = packed.T[: 6 * NB]
    ab_m = [
        message(ab.at[:, 0, pl.ds(0, X), :], ab.at[:, Z, pl.ds(0, X), :], "gz", -1),
        message(xs_ab, xr_ab, "gx", -1),
        message(ys_ab, yr_ab, "gy", -1),
    ]
    for m in ab_m:
        m.start()

    def smooth(k):
        def body(b, _):
            for p in range(2):
                z = 2 * b + p
                s = sc[k, z + 1, 8 : 8 + X, :]
                h = halo(rt_sc, p * X, X, k * NB + b)
                n = sc[k, z, 8 : 8 + X, :] + sc[k, z + 2, 8 : 8 + X, :]
                n += sc[k, z + 1, 7 : 7 + X, :] + sc[k, z + 1, 9 : 9 + X, :]
                n += before(s, h, lane) + after(s, h, lane)
                out[k, z] = s + n * ed[k, z]
            return 0

        each(NB, body, 0)

    def fill_rows():
        for m in rest:
            m.wait_recv()
        for k in range(3):
            if k != 1:
                sc[k, 1 : Z + 1, 7, :] = xr_sc[0, k]
            sc[k, 1 : Z + 1, 8 + X, :] = xr_sc[1, k]
        unpack(rt_sc, yr_sc[0], yr_sc[1])

    fill_rows()
    smooth(0)

    for copy in round1:
        copy.wait_recv()
    ar2[0] = jnp.sum(ar1[...], axis=0)
    if tell_2:
        told(2)
    round2 = spread_round(ar2, partners, len(plane))

    smooth(1)
    smooth(2)
    for m in ab_m:
        m.wait_recv()
    ab[:, 0:Z, X, :] = xr_ab[...]
    rt_ab[...] = jnp.concatenate(
        [pltpu.roll(yr_ab[...], 6 * NB - 1, 0), jnp.zeros((L - 6 * NB, L), F32)], axis=0
    ).T

    def gradient(j, into, add):
        def body(b, _):
            for p in range(2):
                z = 2 * b + p
                f = ab[j, z, 0:X, :]
                h = halo(rt_ab, p * X, X, j * NB + b)
                d = (ab[j, z + 1, 0:X, :] - f, ab[j, z, 1 : X + 1, :] - f, after(f, h, lane) - f)
                for k in range(3):
                    into[k, z] = into[k, z] + d[k] if add else d[k]
            return 0

        each(NB, body, 0)

    gradient(0, out, True)
    gradient(1, res, False)
    gradient(2, ed, False)

    for copy in round2:
        copy.wait_recv()
    total = jnp.sum(ar2[...], axis=0)
    g1, g2, h11, h12, h22 = (
        jnp.sum(jnp.where(iota((1, L), 1) == i, total, 0.0), axis=1, keepdims=True) for i in range(5)
    )
    c2 = (g2 - h12 * g1 / h11) / (h22 - h12 * h12 / h11)
    c1 = (g1 - h12 * c2) / h11

    def finish(z, _):
        for k in range(3):
            out[k, z] = out[k, z] + c1 * res[k, z] + c2 * ed[k, z]
        return 0

    lax.fori_loop(0, Z, finish, 0, unroll=2)

    for m in used:
        m.wait_send()
    for copy in round1 + round2:
        copy.wait_send()


def solution(mesh):
    sizes = dict(mesh.shape)
    n_ar = sizes["gz"] - 1 + sizes["gx"] * sizes["gy"] - 1

    def local(residual, edge_diag, node_shift, coarse_shift):
        _, Z, X, Y = residual.shape
        ZC, XC, NB = Z // 2, X // 2, Z // 2
        assert X == 64 and Y == L and Z % 8 == 0

        def v(*shape):
            return pltpu.VMEM(shape, F32)

        scratch = [
            v(3, Z, X, L), v(3, Z, X, L), v(Z, X, L), v(ZC, XC, L // 2),
            v(3, Z + 2, X + 16, L), v(Z + 2, X + 16, L), v(ZC, X, L),
            v(ZC, XC, L), v(ZC, XC, L),
            v(ZC + 2, XC + 16, L), v(ZC + 2, XC + 16, L),
            v(ZC, XC, L), v(ZC, XC, L), v(ZC, XC, L),
            v(3, Z + 1, X + 8, L), v(Z, 8, L), v(Z, 8, L),
            v(L, L), v(L, L), v(L, L), v(L, L), v(L, L), v(L, L),
            v(2, 3, Z, L), v(2, 3, Z, L), v(2, Z, L), v(2, Z, L),
            v(2, ZC, L), v(2, ZC, L), v(2, ZC, L), v(2, ZC, L), v(3, Z, L), v(3, Z, L),
            v(6 * NB, L), v(2, 6 * NB, L), v(2 * NB, L), v(2, 2 * NB, L),
            v(8, L), v(2, 8, L), v(8, L), v(2, 8, L), v(6 * NB, L), v(6 * NB, L),
            v(sizes["gx"] * sizes["gy"], 1, L), v(sizes["gz"], 1, L), pltpu.SemaphoreType.REGULAR((3,)),
            pltpu.SemaphoreType.DMA((12,)),
            pltpu.SemaphoreType.DMA((32,)), pltpu.SemaphoreType.DMA((32,)),
            pltpu.SemaphoreType.DMA((n_ar,)), pltpu.SemaphoreType.DMA((n_ar,)),
        ]
        return pl.pallas_call(
            functools.partial(kernel, sizes),
            out_shape=jax.ShapeDtypeStruct(residual.shape, F32),
            in_specs=[pl.BlockSpec(memory_space=pl.ANY)] * 4,
            out_specs=pl.BlockSpec(memory_space=pltpu.VMEM),
            scratch_shapes=scratch,
            compiler_params=pltpu.CompilerParams(
                collective_id=0, has_side_effects=True, vmem_limit_bytes=48 * 1024 * 1024
            ),
        )(*(
            pltpu.with_memory_space_constraint(x, pltpu.HBM)
            for x in (residual, edge_diag, node_shift, coarse_shift)
        ))

    fine, coarse = P(None, "gz", "gx", "gy"), P("gz", "gx", "gy")
    return jax.shard_map(
        local, mesh=mesh, in_specs=(fine, fine, coarse, coarse), out_specs=fine, check_vma=False
    )
```

```python
import functools

import jax
import jax.numpy as jnp
from jax import lax
from jax.experimental import pallas as pl
from jax.experimental.pallas import tpu as pltpu
from jax.sharding import PartitionSpec as P

MESH = pl.DeviceIdType.MESH
AXES = ("gx", "gy", "gz")
L = 128
F32 = jnp.float32


def iota(shape, dim):
    return lax.broadcasted_iota(jnp.int32, shape, dim)


class Message:
    def __init__(self, copy, sends, receives):
        self.copy, self.sends, self.receives = copy, sends, receives

    def start(self):
        pl.when(self.sends)(lambda: self.copy.start())

    def wait_recv(self):
        pl.when(self.receives)(lambda: self.copy.wait_recv())

    def wait_send(self):
        pl.when(self.sends)(lambda: self.copy.wait_send())


def kernel(
    sizes, res_h, ed_h, ns_h, cs_h, out,
    res, ed, ns, cs, sc, fg, tmp, cr, cd, v1, v2, wy1, wy2, ab, face_e, face_r,
    rt_g, rt_sc, rt_fg, rt_v1, rt_v2, rt_ab, rt_d,
    dv, v1b, x2s, x2r, y2s, y2r, cdz, cdxs, cdx, cdys, cdy,
    xs_sc, xr_sc, xs_fg, xr_fg, xs_v1, xr_v1, xs_v2, xr_v2, xs_ab, xr_ab,
    ys_sc, yr_sc, ys_fg, yr_fg, ys_v1, yr_v1, ys_v2, yr_v2, ys_ab, yr_ab,
    ar1, ar2, present, in_sem, send_sem, recv_sem, ar_send, ar_recv,
):
    _, Z, X, _ = res.shape
    ZC, XC = Z // 2, X // 2
    NB = Z // 2
    PC = L // XC
    NBC = ZC // PC
    me = {a: lax.axis_index(a) for a in AXES}
    used = []

    def both(flags):
        return functools.reduce(jnp.logical_and, flags)

    def message(src, dst, *steps):
        i = len(used)
        steps = dict(zip(steps[::2], steps[1::2]))
        copy = pltpu.make_async_remote_copy(
            src_ref=src, dst_ref=dst, send_sem=send_sem.at[i], recv_sem=recv_sem.at[i],
            device_id={a: me[a] + d for a, d in steps.items()}, device_id_type=MESH,
        )
        low = {a: me[a] > 0 for a in steps}
        high = {a: me[a] < sizes[a] - 1 for a in steps}
        made = Message(
            copy,
            both([high[a] if d > 0 else low[a] for a, d in steps.items()]),
            both([low[a] if d > 0 else high[a] for a, d in steps.items()]),
        )
        used.append(made)
        return made

    def load(i, pick, into):
        return (
            pltpu.make_async_copy(pick(ed_h), into(ed, face_e), in_sem.at[2 * i]),
            pltpu.make_async_copy(pick(res_h), into(res, face_r), in_sem.at[2 * i + 1]),
        )

    loads = [
        load(0, lambda h: h.at[0, Z - 1], lambda v, f: v.at[0, Z - 1]),
        load(1, lambda h: h.at[1, :, pl.ds(X - 8, 8), :], lambda v, f: f),
        load(2, lambda h: h.at[2], lambda v, f: v.at[2]),
        load(3, lambda h: h.at[1], lambda v, f: v.at[1]),
        load(4, lambda h: h.at[0, pl.ds(0, Z - 1)], lambda v, f: v.at[0, pl.ds(0, Z - 1)]),
    ]
    load_ns = pltpu.make_async_copy(ns_h, ns, in_sem.at[10])
    load_cs = pltpu.make_async_copy(cs_h, cs, in_sem.at[11])
    for pair in loads:
        for copy in pair:
            copy.start()
    load_ns.start()
    load_cs.start()

    partners = [{"gz": lax.rem(me["gz"] + d, sizes["gz"])} for d in range(1, sizes["gz"])]
    plane = [
        {"gx": lax.rem(me["gx"] + dx, sizes["gx"]), "gy": lax.rem(me["gy"] + dy, sizes["gy"])}
        for dx in range(sizes["gx"]) for dy in range(sizes["gy"]) if dx or dy
    ]
    far = [
        {"gx": lax.rem(me["gx"] + dx, sizes["gx"]), "gy": lax.rem(me["gy"] + dy, sizes["gy"])}
        for dx in range(sizes["gx"]) for dy in range(sizes["gy"]) if dx == 2 or dy == 2
    ]
    def at(**steps):
        return {a: lax.rem(me[a] + d + sizes[a], sizes[a]) for a, d in steps.items()}

    near = [at(**{a: d}) for a in AXES for d in (1, -1)] + [
        at(**{a: d, b: e})
        for a, b in (("gx", "gy"), ("gx", "gz"), ("gy", "gz")) for d in (1, -1) for e in (1, -1)
    ]
    barrier = pltpu.get_barrier_semaphore()
    for other in far:
        pl.semaphore_signal(barrier, inc=1, device_id=other, device_id_type=MESH)

    zero_plane = jnp.zeros((X, L), F32)
    zero_coarse = jnp.zeros((XC, L), F32)
    for k in range(3):
        for z in (0, Z + 1):
            sc[k, z, 8 : 8 + X, :] = zero_plane
        ab[k, Z, 0:X, :] = zero_plane
    for z in (0, Z + 1):
        fg[z, 8 : 8 + X, :] = zero_plane
    for z in (0, ZC + 1):
        v1[z, 8 : 8 + XC, :] = zero_coarse
    v2[ZC + 1, 8 : 8 + XC, :] = zero_coarse
    for ref in (
        xr_sc, xr_fg, xr_v1, xr_v2, xr_ab, yr_sc, yr_fg, yr_v1, yr_v2, yr_ab,
        dv, v1b, x2r, y2r, cdz, cdx, cdy,
    ):
        ref[...] = jnp.zeros(ref.shape, F32)

    for other in near:
        pl.semaphore_signal(barrier, inc=1, device_id=other, device_id_type=MESH)

    lane = iota((X, L), 1)
    lane2 = iota((L, L), 1)
    lanec = iota((XC, L), 1)
    evenc = lanec % 2 == 0

    def put(packed, block, q):
        return jnp.where(lax.shift_right_logical(lane2, 1) == q, pltpu.roll(block, 2 * q + 1, 1), packed)

    def halo(rt, row, rows, q):
        return pltpu.roll(rt[pl.ds(row, rows), :], L - 1 - 2 * q, 1)

    def before(x, h, at):
        return jnp.where(at == 0, h, pltpu.roll(x, 1, 1))

    def after(x, h, at):
        return jnp.where(at == L - 1, h, pltpu.roll(x, L - 1, 1))

    def unpack(rt, low, high):
        n = low.shape[0]
        mixed = jnp.where(iota((n, L), 0) % 2 == 1, pltpu.roll(low, 1, 0), pltpu.roll(high, n - 1, 0))
        rt[...] = jnp.concatenate([mixed, jnp.zeros((L - n, L), F32)], axis=0).T

    def each(n, body, init):
        return lax.fori_loop(0, n, body, init, unroll=True)

    inner = pl.ds(8, X)
    third = 2 * NB
    sc_zu0 = message(sc.at[0, Z, inner, :], sc.at[0, 0, inner, :], "gz", 1)
    sc_xu1 = message(xs_sc.at[1, 1], xr_sc.at[0, 1], "gx", 1)
    sc_yu2 = message(ys_sc.at[pl.ds(2 * third, third)], yr_sc.at[0, pl.ds(2 * third, third)], "gy", 1)
    rest = [
        message(xs_sc.at[1, 0], xr_sc.at[0, 0], "gx", 1),
        message(xs_sc.at[1, 2], xr_sc.at[0, 2], "gx", 1),
        message(xs_sc.at[0], xr_sc.at[1], "gx", -1),
        message(ys_sc.at[pl.ds(0, 2 * third)], yr_sc.at[0, pl.ds(0, 2 * third)], "gy", 1),
        message(ys_sc, yr_sc.at[1], "gy", -1),
        message(sc.at[1:3, Z, inner, :], sc.at[1:3, 0, inner, :], "gz", 1),
        message(sc.at[:, 1, inner, :], sc.at[:, Z + 1, inner, :], "gz", -1),
    ]

    def arrived(i):
        for copy in loads[i]:
            copy.wait()

    def scale(k, z):
        r = 1.0 / ed[k, z]
        ed[k, z] = r
        s = res[k, z] * r
        sc[k, z + 1, 8 : 8 + X, :] = s
        xs_sc[0, k, pl.ds(z, 1), :] = s[0:1]
        if k != 1:
            xs_sc[1, k, pl.ds(z, 1), :] = s[X - 1 : X]
        return s

    def scale_all(k, packed, first):
        def body(b, packed):
            block = []
            for p in range(2):
                z = 2 * b + p
                block.append(scale(k, z))
            return put(packed, jnp.concatenate(block, axis=0), first + b)

        return each(NB, body, packed)

    arrived(0)
    scale(0, Z - 1)
    arrived(1)
    xs_sc[1, 1] = face_r[:, 7, :] * (1.0 / face_e[:, 7, :])
    arrived(2)
    ys_sc[2 * third :] = scale_all(2, jnp.zeros((L, L), F32), 0).T[:third]
    pl.semaphore_wait(barrier, len(far) + len(near))

    def tell(i):
        for d in (1 << i, sizes["gz"] - (1 << i)):
            other = {"gz": lax.rem(me["gz"] + d, sizes["gz"])}
            pl.semaphore_signal(present.at[i], inc=1, device_id=other, device_id_type=MESH)

    def told(i):
        pl.semaphore_wait(present.at[i], 2)

    steps = [i for i in range(3) if (1 << i) < sizes["gz"] // 2]
    tell_0, tell_1, tell_2 = (i in steps for i in range(3))
    if tell_0:
        tell(0)
    for m in (sc_yu2, sc_xu1, sc_zu0):
        m.start()
    arrived(3)
    packed = scale_all(1, jnp.zeros((L, L), F32), NB)
    arrived(4)

    def bulk(b, packed):
        block = [scale(0, 2 * b), scale(0, 2 * b + 1)]
        return put(packed, jnp.concatenate(block, axis=0), b)

    packed = each(NB - 1, bulk, packed)
    block = [scale(0, Z - 2), sc[0, Z, 8 : 8 + X, :]]
    packed = put(packed, jnp.concatenate(block, axis=0), NB - 1)
    ys_sc[0 : 2 * third] = packed.T[: 2 * third]
    for m in rest:
        m.start()

    load_ns.wait()
    load_cs.wait()

    def invert(z, _):
        ns[z] = 1.0 / (6.0 + ns[z])
        return 0

    lax.fori_loop(0, Z, invert, 0, unroll=2)
    twice = (iota((L // 2, L), 0) == iota((L // 2, L), 1) // 2).astype(F32)
    wide = jnp.dot(
        cs[...].reshape(ZC * XC, L // 2), twice,
        precision=lax.Precision.HIGHEST, preferred_element_type=F32,
    )
    cd[...] = (1.0 / (6.0 + wide)).reshape(ZC, XC, L)

    def pack_coarse(planes):
        packed = jnp.zeros((L, L), F32)
        for q in range(NBC):
            packed = put(packed, planes(PC * q, PC * (q + 1)).reshape(L, L), q)
        return packed

    cdxs[...] = cd[:, XC - 1, :]
    cdys[...] = pack_coarse(lambda a, b: cd[a:b]).T[:8]
    fixed = [
        message(cd.at[ZC - 1], cdz, "gz", 1),
        message(cdxs, cdx, "gx", 1),
        message(cdys, cdy, "gy", 1),
    ]
    for m in fixed:
        m.start()

    for m in (sc_yu2, sc_xu1, sc_zu0):
        m.wait_recv()
    if tell_0:
        told(0)
    if tell_1:
        tell(1)
    sc[1, 1 : Z + 1, 7, :] = xr_sc[0, 1]
    low = yr_sc[0, 2 * third :]
    unpack(rt_g, low, jnp.zeros_like(low))

    def guess(b, packed):
        block = []
        for p in range(2):
            z = 2 * b + p
            s0, s0m = sc[0, z + 1, 8 : 8 + X, :], sc[0, z, 8 : 8 + X, :]
            s1, s1m = sc[1, z + 1, 8 : 8 + X, :], sc[1, z + 1, 7 : 7 + X, :]
            s2 = sc[2, z + 1, 8 : 8 + X, :]
            s2m = before(s2, halo(rt_g, p * X, X, b), lane)
            g = ((s0m - s0) + (s1m - s1) + (s2m - s2)) * ns[z]
            fg[z + 1, 8 : 8 + X, :] = g
            xs_fg[0, pl.ds(z, 1), :] = g[0:1]
            xs_fg[1, pl.ds(z, 1), :] = g[X - 1 : X]
            block.append(g)
        return put(packed, jnp.concatenate(block, axis=0), b)

    packed = each(NB, guess, jnp.zeros((L, L), F32))
    ys_fg[...] = packed.T[: 2 * NB]
    fg_m = [
        message(ys_fg, yr_fg.at[0], "gy", 1),
        message(ys_fg, yr_fg.at[1], "gy", -1),
        message(xs_fg.at[1], xr_fg.at[0], "gx", 1),
        message(xs_fg.at[0], xr_fg.at[1], "gx", -1),
        message(fg.at[Z, inner, :], fg.at[0, inner, :], "gz", 1),
        message(fg.at[1, inner, :], fg.at[Z + 1, inner, :], "gz", -1),
    ]
    for m in fg_m:
        m.start()

    for m in fg_m:
        m.wait_recv()
    if tell_1:
        told(1)
    if tell_2:
        tell(2)
    fg[1 : Z + 1, 7, :] = xr_fg[0]
    fg[1 : Z + 1, 8 + X, :] = xr_fg[1]
    unpack(rt_fg, yr_fg[0], yr_fg[1])

    def swap(x):
        return jnp.where(evenc, pltpu.roll(x, L - 1, 1), pltpu.roll(x, 1, 1))

    def restrict(b, _):
        total = None
        for p in range(2):
            z = 2 * b + p
            g = fg[z + 1, 8 : 8 + X, :]
            h = halo(rt_fg, p * X, X, b)
            n = fg[z, 8 : 8 + X, :] + fg[z + 2, 8 : 8 + X, :]
            n += fg[z + 1, 7 : 7 + X, :] + fg[z + 1, 9 : 9 + X, :]
            n += before(g, h, lane) + after(g, h, lane)
            ab[0, z, 0:X, :] = g + n * ns[z]
            total = n if p == 0 else total + n
        tmp[b] = total
        return 0

    each(ZC, restrict, 0)

    def direction(b, _):
        u = tmp[b, pl.ds(0, XC, 2), :] + tmp[b, pl.ds(1, XC, 2), :]
        u = u + swap(u)
        cr[b] = u
        v = u * cd[b]
        v1[b + 1, 8 : 8 + XC, :] = v
        xs_v1[0, pl.ds(b, 1), :] = v[0:1]
        xs_v1[1, pl.ds(b, 1), :] = v[XC - 1 : XC]
        x2s[pl.ds(b, 1), :] = v[XC - 2 : XC - 1]
        return 0

    each(ZC, direction, 0)

    def coarse_faces(v, xs, xr, ys, yr):
        mid = pl.ds(8, XC)
        return [
            message(ys, yr.at[0], "gy", 1),
            message(ys, yr.at[1], "gy", -1),
            message(xs.at[1], xr.at[0], "gx", 1),
            message(xs.at[0], xr.at[1], "gx", -1),
            message(v.at[ZC, mid, :], v.at[0, mid, :], "gz", 1),
            message(v.at[1, mid, :], v.at[ZC + 1, mid, :], "gz", -1),
        ]

    def coarse_arrive(sent, v, xr, yr, rt):
        for m in sent:
            m.wait_recv()
        v[1 : ZC + 1, 7, :] = xr[0]
        v[1 : ZC + 1, 8 + XC, :] = xr[1]
        unpack(rt, yr[0], yr[1])

    def around(v, wy, rt, b):
        c = v[b + 1, 8 : 8 + XC, :]
        h = halo(rt, (b % PC) * XC, XC, b // PC)
        w = jnp.where(evenc, before(c, h, lanec), after(c, h, lanec))
        wy[b] = w
        n = v[b, 8 : 8 + XC, :] + v[b + 2, 8 : 8 + XC, :]
        n += v[b + 1, 7 : 7 + XC, :] + v[b + 1, 9 : 9 + XC, :]
        return c, n + (w + swap(w))

    v1_x = [
        message(xs_v1.at[1], dv.at[0], "gz", 1, "gx", 1),
        message(xs_v1.at[0], dv.at[1], "gz", 1, "gx", -1),
        message(xs_v1.at[1], dv.at[2], "gz", -1, "gx", 1),
        message(xs_v1.at[1], dv.at[3], "gx", 1, "gy", 1),
        message(xs_v1.at[1], dv.at[4], "gx", 1, "gy", -1),
        message(x2s, x2r, "gx", 1),
        message(v1.at[ZC - 1, pl.ds(8, XC), :], v1b, "gz", 1),
    ]
    v1_y = [
        message(ys_v1, dv.at[5], "gz", 1, "gy", 1),
        message(ys_v1, dv.at[6], "gz", 1, "gy", -1),
        message(ys_v1, dv.at[7], "gz", -1, "gy", 1),
        message(ys_v1, dv.at[8], "gx", 1, "gy", 1),
        message(ys_v1, dv.at[9], "gx", -1, "gy", 1),
        message(y2s, y2r, "gy", 1),
    ]
    v1_f = coarse_faces(v1, xs_v1, xr_v1, ys_v1, yr_v1)
    for m in v1_x + v1_f[2:]:
        m.start()
    packed = pack_coarse(lambda a, b: v1[1 + a : 1 + b, 8 : 8 + XC, :])
    for q in range(NBC):
        block = v1[1 + PC * q : 1 + PC * (q + 1), 8 : 8 + XC, :].reshape(L, L)
        to = L // 4 + q
        packed = jnp.where(
            lax.shift_right_logical(lane2, 1) == to, pltpu.roll(block, 2 * to + 3, 1), packed
        )
    turned = packed.T
    ys_v1[...] = turned[:8]
    y2s[...] = turned[L // 2 : L // 2 + 8]
    for m in v1_y + v1_f[:2]:
        m.start()
    coarse_arrive(v1_f, v1, xr_v1, yr_v1, rt_v1)

    def first(b, sums):
        g1, g2, h11, h12 = sums
        c, n = around(v1, wy1, rt_v1, b)
        r = cr[b]
        a = r - n
        w = a * cd[b]
        v2[b + 1, 8 : 8 + XC, :] = w
        xs_v2[pl.ds(b, 1), :] = w[0:1]
        return g1 + c * r, g2 + w * r, h11 + c * a, h12 + w * a

    sums = each(ZC, first, (zero_coarse,) * 4)
    for m in v1_x + v1_y + fixed:
        m.wait_recv()
    v1[0, 7:8, :] = dv[0, 7:8, :]
    v1[0, 8 + XC : 9 + XC, :] = dv[1, 7:8, :]
    unpack(rt_d, dv[5], dv[6])
    c = v1[0, 8 : 8 + XC, :]
    h = halo(rt_d, ((ZC - 1) % PC) * XC, XC, (ZC - 1) // PC)
    w = jnp.where(evenc, before(c, h, lanec), after(c, h, lanec))
    n = v1b[...] + v1[1, 8 : 8 + XC, :] + v1[0, 7 : 7 + XC, :] + v1[0, 9 : 9 + XC, :]
    below_z = c - cdz[...] * (n + (w + swap(w)))

    row, line = iota((8, L), 0), iota((8, L), 1)
    even = line % 2 == 0
    c = xr_v1[0]
    n = x2r[...] + xs_v1[0]
    n += jnp.where(row == 0, pltpu.roll(dv[0], 1, 0), pltpu.roll(c, 1, 0))
    n += jnp.where(row == 7, pltpu.roll(dv[2], 7, 0), pltpu.roll(c, 7, 0))
    low = jnp.where(line == 0, pltpu.roll(dv[3], 1, 1), pltpu.roll(c, 1, 1))
    high = jnp.where(line == L - 1, pltpu.roll(dv[4], L - 1, 1), pltpu.roll(c, L - 1, 1))
    w = jnp.where(even, low, high)
    n += w + jnp.where(even, pltpu.roll(w, L - 1, 1), pltpu.roll(w, 1, 1))
    below_x = c - cdx[...] * n

    c = yr_v1[0]
    n = y2r[...] + pltpu.roll(ys_v1[...], 7, 0)
    down = jnp.where(row >= 2, pltpu.roll(c, 2, 0), pltpu.roll(dv[5], 6, 0))
    up = jnp.where(row < 2, pltpu.roll(c, 6, 0), pltpu.roll(dv[7], 2, 0))
    n += pltpu.roll(jnp.where(line < L - XC, c, down), XC, 1)
    n += pltpu.roll(jnp.where(line >= XC, c, up), L - XC, 1)
    n += jnp.where(line % XC == 0, pltpu.roll(dv[8], L - XC + 1, 1), pltpu.roll(c, 1, 1))
    n += jnp.where(line % XC == XC - 1, pltpu.roll(dv[9], XC - 1, 1), pltpu.roll(c, L - 1, 1))
    below_y = c - cdy[...] * n

    packed = pack_coarse(lambda a, b: v2[1 + a : 1 + b, 8 : 8 + XC, :])
    ys_v2[...] = packed.T[:8]
    v2_m = [
        message(ys_v2, yr_v2, "gy", -1),
        message(xs_v2, xr_v2, "gx", -1),
        message(v2.at[1, pl.ds(8, XC), :], v2.at[ZC + 1, pl.ds(8, XC), :], "gz", -1),
    ]
    for m in v2_m:
        m.start()
    nothing = jnp.zeros((XC, L), F32)
    v2[0, 8 : 8 + XC, :] = below_z
    v2[1 : ZC + 1, 7, :] = below_x

    def pairs(b, sums):
        c = v2[b + 1, 8 : 8 + XC, :]
        w = jnp.where(evenc, before(c, nothing, lanec), after(c, nothing, lanec))
        n = v2[b, 8 : 8 + XC, :] + v2[b + 1, 7 : 7 + XC, :]
        return sums + c * (2.0 * n + 2.0 * w)

    inside = each(ZC, pairs, zero_coarse)
    side = jnp.where((row == 0) | (row == 2), pltpu.roll(ys_v2[...], 7, 0) * below_y, 0.0)
    total = sums[3] - inside
    total = total - jnp.concatenate([4.0 * side, jnp.zeros((XC - 8, L), F32)], axis=0)
    sums += (total,)

    row = jnp.zeros((1, L), F32)
    for i, s in enumerate(sums):
        one = jnp.sum(jnp.sum(s, axis=0, keepdims=True), axis=1, keepdims=True)
        row = jnp.where(iota((1, L), 1) == i, one, row)
    ar1[0] = row

    def spread_round(buf, others, base):
        copies = [
            pltpu.make_async_remote_copy(
                src_ref=buf.at[0], dst_ref=buf.at[d + 1], send_sem=ar_send.at[base + d],
                recv_sem=ar_recv.at[base + d], device_id=other, device_id_type=MESH,
            )
            for d, other in enumerate(others)
        ]
        for copy in copies:
            copy.start()
        return copies

    round1 = spread_round(ar1, plane, 0)

    def prolong(v, wy, j):
        def body(b, _):
            w = 3.0 * v[b + 1, 8 : 8 + XC, :] + wy[b]
            for px in range(2):
                wx = w + v[b + 1, 7 + 2 * px : 7 + 2 * px + XC, :]
                for pz in range(2):
                    z = 2 * b + pz
                    n = wx + v[b + 2 * pz, 8 : 8 + XC, :]
                    ab[j, z, pl.ds(px, XC, 2), :] = n * ns[z, pl.ds(px, XC, 2), :]
            return 0

        each(ZC, body, 0)

    prolong(v1, wy1, 1)
    for m in v2_m:
        m.wait_recv()
    v2[1 : ZC + 1, 8 + XC, :] = xr_v2[...]
    unpack(rt_v2, below_y, yr_v2[...])

    def sides(b, _):
        c = v2[b + 1, 8 : 8 + XC, :]
        h = halo(rt_v2, (b % PC) * XC, XC, b // PC)
        wy2[b] = jnp.where(evenc, before(c, h, lanec), after(c, h, lanec))
        return 0

    each(ZC, sides, 0)
    prolong(v2, wy2, 2)

    def fill(j):
        def body(b, packed):
            block = []
            for p in range(2):
                z = 2 * b + p
                x = ab[j, z, 0:X, :]
                xs_ab[j, pl.ds(z, 1), :] = x[0:1]
                block.append(x)
            return put(packed, jnp.concatenate(block, axis=0), j * NB + b)

        return body

    packed = jnp.zeros((L, L), F32)
    for j in range(3):
        packed = each(NB, fill(j), packed)
    ys_ab[...] = packed.T[: 6 * NB]
    ab_m = [
        message(ab.at[:, 0, pl.ds(0, X), :], ab.at[:, Z, pl.ds(0, X), :], "gz", -1),
        message(xs_ab, xr_ab, "gx", -1),
        message(ys_ab, yr_ab, "gy", -1),
    ]
    for m in ab_m:
        m.start()

    def smooth(k):
        def body(b, _):
            for p in range(2):
                z = 2 * b + p
                s = sc[k, z + 1, 8 : 8 + X, :]
                h = halo(rt_sc, p * X, X, k * NB + b)
                n = sc[k, z, 8 : 8 + X, :] + sc[k, z + 2, 8 : 8 + X, :]
                n += sc[k, z + 1, 7 : 7 + X, :] + sc[k, z + 1, 9 : 9 + X, :]
                n += before(s, h, lane) + after(s, h, lane)
                out[k, z] = s + n * ed[k, z]
            return 0

        each(NB, body, 0)

    def fill_rows():
        for m in rest:
            m.wait_recv()
        for k in range(3):
            if k != 1:
                sc[k, 1 : Z + 1, 7, :] = xr_sc[0, k]
            sc[k, 1 : Z + 1, 8 + X, :] = xr_sc[1, k]
        unpack(rt_sc, yr_sc[0], yr_sc[1])

    fill_rows()
    smooth(0)

    for copy in round1:
        copy.wait_recv()
    ar2[0] = jnp.sum(ar1[...], axis=0)
    if tell_2:
        told(2)
    round2 = spread_round(ar2, partners, len(plane))

    smooth(1)
    smooth(2)
    for m in ab_m:
        m.wait_recv()
    ab[:, 0:Z, X, :] = xr_ab[...]
    rt_ab[...] = jnp.concatenate(
        [pltpu.roll(yr_ab[...], 6 * NB - 1, 0), jnp.zeros((L - 6 * NB, L), F32)], axis=0
    ).T

    def gradient(j, into, add):
        def body(b, _):
            for p in range(2):
                z = 2 * b + p
                f = ab[j, z, 0:X, :]
                h = halo(rt_ab, p * X, X, j * NB + b)
                d = (ab[j, z + 1, 0:X, :] - f, ab[j, z, 1 : X + 1, :] - f, after(f, h, lane) - f)
                for k in range(3):
                    into[k, z] = into[k, z] + d[k] if add else d[k]
            return 0

        each(NB, body, 0)

    gradient(0, out, True)
    gradient(1, res, False)
    gradient(2, ed, False)

    for copy in round2:
        copy.wait_recv()
    total = jnp.sum(ar2[...], axis=0)
    g1, g2, h11, h12, h22 = (
        jnp.sum(jnp.where(iota((1, L), 1) == i, total, 0.0), axis=1, keepdims=True) for i in range(5)
    )
    c2 = (g2 - h12 * g1 / h11) / (h22 - h12 * h12 / h11)
    c1 = (g1 - h12 * c2) / h11

    def finish(z, _):
        for k in range(3):
            out[k, z] = out[k, z] + c1 * res[k, z] + c2 * ed[k, z]
        return 0

    lax.fori_loop(0, Z, finish, 0, unroll=2)

    for m in used:
        m.wait_send()
    for copy in round1 + round2:
        copy.wait_send()


def solution(mesh):
    sizes = dict(mesh.shape)
    n_ar = sizes["gz"] - 1 + sizes["gx"] * sizes["gy"] - 1

    def local(residual, edge_diag, node_shift, coarse_shift):
        _, Z, X, Y = residual.shape
        ZC, XC, NB = Z // 2, X // 2, Z // 2
        assert X == 64 and Y == L and Z % 8 == 0

        def v(*shape):
            return pltpu.VMEM(shape, F32)

        scratch = [
            v(3, Z, X, L), v(3, Z, X, L), v(Z, X, L), v(ZC, XC, L // 2),
            v(3, Z + 2, X + 16, L), v(Z + 2, X + 16, L), v(ZC, X, L),
            v(ZC, XC, L), v(ZC, XC, L),
            v(ZC + 2, XC + 16, L), v(ZC + 2, XC + 16, L),
            v(ZC, XC, L), v(ZC, XC, L),
            v(3, Z + 1, X + 8, L), v(Z, 8, L), v(Z, 8, L),
            v(L, L), v(L, L), v(L, L), v(L, L), v(L, L), v(L, L), v(L, L),
            v(10, 8, L), v(XC, L), v(ZC, L), v(ZC, L), v(8, L), v(8, L),
            v(XC, L), v(ZC, L), v(ZC, L), v(8, L), v(8, L),
            v(2, 3, Z, L), v(2, 3, Z, L), v(2, Z, L), v(2, Z, L),
            v(2, ZC, L), v(2, ZC, L), v(ZC, L), v(ZC, L), v(3, Z, L), v(3, Z, L),
            v(6 * NB, L), v(2, 6 * NB, L), v(2 * NB, L), v(2, 2 * NB, L),
            v(8, L), v(2, 8, L), v(8, L), v(8, L), v(6 * NB, L), v(6 * NB, L),
            v(sizes["gx"] * sizes["gy"], 1, L), v(sizes["gz"], 1, L), pltpu.SemaphoreType.REGULAR((3,)),
            pltpu.SemaphoreType.DMA((12,)),
            pltpu.SemaphoreType.DMA((56,)), pltpu.SemaphoreType.DMA((56,)),
            pltpu.SemaphoreType.DMA((n_ar,)), pltpu.SemaphoreType.DMA((n_ar,)),
        ]
        return pl.pallas_call(
            functools.partial(kernel, sizes),
            out_shape=jax.ShapeDtypeStruct(residual.shape, F32),
            in_specs=[pl.BlockSpec(memory_space=pl.ANY)] * 4,
            out_specs=pl.BlockSpec(memory_space=pltpu.VMEM),
            scratch_shapes=scratch,
            compiler_params=pltpu.CompilerParams(
                collective_id=0, has_side_effects=True, vmem_limit_bytes=48 * 1024 * 1024
            ),
        )(*(
            pltpu.with_memory_space_constraint(x, pltpu.HBM)
            for x in (residual, edge_diag, node_shift, coarse_shift)
        ))

    fine, coarse = P(None, "gz", "gx", "gy"), P("gz", "gx", "gy")
    return jax.shard_map(
        local, mesh=mesh, in_specs=(fine, fine, coarse, coarse), out_specs=fine, check_vma=False
    )
```

```python
import functools

import jax
import jax.numpy as jnp
from jax import lax
from jax.experimental import pallas as pl
from jax.experimental.pallas import tpu as pltpu
from jax.sharding import PartitionSpec as P

MESH = pl.DeviceIdType.MESH
AXES = ("gx", "gy", "gz")
L = 128
F32 = jnp.float32


def iota(shape, dim):
    return lax.broadcasted_iota(jnp.int32, shape, dim)


class Message:
    def __init__(self, copy, sends, receives):
        self.copy, self.sends, self.receives = copy, sends, receives

    def start(self):
        pl.when(self.sends)(lambda: self.copy.start())

    def wait_recv(self):
        pl.when(self.receives)(lambda: self.copy.wait_recv())

    def wait_send(self):
        pl.when(self.sends)(lambda: self.copy.wait_send())


def kernel(
    sizes, res_h, ed_h, ns_h, cs_h, out,
    res, ed, ns, cs, sc, fg, tmp, cr, cd, v1, v2, wy1, wy2, ab, face_e, face_r,
    rt_g, rt_sc, rt_fg, rt_v1, rt_v2, rt_ab, rt_d,
    dv, v1b, x2s, x2r, y2s, y2r, cdz, cdxs, cdx, cdys, cdy,
    xs_sc, xr_sc, xs_fg, xr_fg, xs_v1, xr_v1, xs_v2, xr_v2, xs_ab, xr_ab,
    ys_sc, yr_sc, ys_fg, yr_fg, ys_v1, yr_v1, ys_v2, yr_v2, ys_ab, yr_ab,
    ar1, ar2, present, in_sem, send_sem, recv_sem, ar_send, ar_recv,
):
    _, Z, X, _ = res.shape
    ZC, XC = Z // 2, X // 2
    NB = Z // 2
    PC = L // XC
    NBC = ZC // PC
    me = {a: lax.axis_index(a) for a in AXES}
    used = []

    def both(flags):
        return functools.reduce(jnp.logical_and, flags)

    def message(src, dst, *steps):
        i = len(used)
        steps = dict(zip(steps[::2], steps[1::2]))
        copy = pltpu.make_async_remote_copy(
            src_ref=src, dst_ref=dst, send_sem=send_sem.at[i], recv_sem=recv_sem.at[i],
            device_id={a: me[a] + d for a, d in steps.items()}, device_id_type=MESH,
        )
        low = {a: me[a] > 0 for a in steps}
        high = {a: me[a] < sizes[a] - 1 for a in steps}
        made = Message(
            copy,
            both([high[a] if d > 0 else low[a] for a, d in steps.items()]),
            both([low[a] if d > 0 else high[a] for a, d in steps.items()]),
        )
        used.append(made)
        return made

    def load(i, pick, into):
        return (
            pltpu.make_async_copy(pick(ed_h), into(ed, face_e), in_sem.at[2 * i]),
            pltpu.make_async_copy(pick(res_h), into(res, face_r), in_sem.at[2 * i + 1]),
        )

    loads = [
        load(0, lambda h: h.at[0, Z - 1], lambda v, f: v.at[0, Z - 1]),
        load(1, lambda h: h.at[1, :, pl.ds(X - 8, 8), :], lambda v, f: f),
        load(2, lambda h: h.at[2], lambda v, f: v.at[2]),
        load(3, lambda h: h.at[1], lambda v, f: v.at[1]),
        load(4, lambda h: h.at[0, pl.ds(0, Z - 1)], lambda v, f: v.at[0, pl.ds(0, Z - 1)]),
    ]
    load_ns = pltpu.make_async_copy(ns_h, ns, in_sem.at[10])
    load_cs = pltpu.make_async_copy(cs_h, cs, in_sem.at[11])
    for pair in loads:
        for copy in pair:
            copy.start()
    load_ns.start()
    load_cs.start()

    partners = [{"gz": lax.rem(me["gz"] + d, sizes["gz"])} for d in range(1, sizes["gz"])]
    plane = [
        {"gx": lax.rem(me["gx"] + dx, sizes["gx"]), "gy": lax.rem(me["gy"] + dy, sizes["gy"])}
        for dx in range(sizes["gx"]) for dy in range(sizes["gy"]) if dx or dy
    ]
    def at(**steps):
        return {a: lax.rem(me[a] + d + sizes[a], sizes[a]) for a, d in steps.items()}

    near = [at(**{a: d}) for a in AXES for d in (1, -1)]
    barrier = pltpu.get_barrier_semaphore()

    zero_plane = jnp.zeros((X, L), F32)
    zero_coarse = jnp.zeros((XC, L), F32)
    for k in range(3):
        for z in (0, Z + 1):
            sc[k, z, 8 : 8 + X, :] = zero_plane
        ab[k, Z, 0:X, :] = zero_plane
    for z in (0, Z + 1):
        fg[z, 8 : 8 + X, :] = zero_plane
    for z in (0, ZC + 1):
        v1[z, 8 : 8 + XC, :] = zero_coarse
    v2[ZC + 1, 8 : 8 + XC, :] = zero_coarse
    for ref in (
        xr_sc, xr_fg, xr_v1, xr_v2, xr_ab, yr_sc, yr_fg, yr_v1, yr_v2, yr_ab,
        dv, v1b, x2r, y2r, cdz, cdx, cdy,
    ):
        ref[...] = jnp.zeros(ref.shape, F32)

    for other in near:
        pl.semaphore_signal(barrier, inc=1, device_id=other, device_id_type=MESH)

    lane = iota((X, L), 1)
    lane2 = iota((L, L), 1)
    lanec = iota((XC, L), 1)
    evenc = lanec % 2 == 0

    def put(packed, block, q):
        return jnp.where(lax.shift_right_logical(lane2, 1) == q, pltpu.roll(block, 2 * q + 1, 1), packed)

    def halo(rt, row, rows, q):
        return pltpu.roll(rt[pl.ds(row, rows), :], L - 1 - 2 * q, 1)

    def before(x, h, at):
        return jnp.where(at == 0, h, pltpu.roll(x, 1, 1))

    def after(x, h, at):
        return jnp.where(at == L - 1, h, pltpu.roll(x, L - 1, 1))

    def unpack(rt, low, high):
        n = low.shape[0]
        mixed = jnp.where(iota((n, L), 0) % 2 == 1, pltpu.roll(low, 1, 0), pltpu.roll(high, n - 1, 0))
        rt[...] = jnp.concatenate([mixed, jnp.zeros((L - n, L), F32)], axis=0).T

    def each(n, body, init):
        return lax.fori_loop(0, n, body, init, unroll=True)

    inner = pl.ds(8, X)
    third = 2 * NB
    sc_zu0 = message(sc.at[0, Z, inner, :], sc.at[0, 0, inner, :], "gz", 1)
    sc_xu1 = message(xs_sc.at[1, 1], xr_sc.at[0, 1], "gx", 1)
    sc_yu2 = message(ys_sc.at[pl.ds(2 * third, third)], yr_sc.at[0, pl.ds(2 * third, third)], "gy", 1)
    rest = [
        message(xs_sc.at[1, 0], xr_sc.at[0, 0], "gx", 1),
        message(xs_sc.at[1, 2], xr_sc.at[0, 2], "gx", 1),
        message(xs_sc.at[0], xr_sc.at[1], "gx", -1),
        message(ys_sc.at[pl.ds(0, 2 * third)], yr_sc.at[0, pl.ds(0, 2 * third)], "gy", 1),
        message(ys_sc, yr_sc.at[1], "gy", -1),
        message(sc.at[1:3, Z, inner, :], sc.at[1:3, 0, inner, :], "gz", 1),
        message(sc.at[:, 1, inner, :], sc.at[:, Z + 1, inner, :], "gz", -1),
    ]

    def arrived(i):
        for copy in loads[i]:
            copy.wait()

    def scale(k, z):
        r = 1.0 / ed[k, z]
        ed[k, z] = r
        s = res[k, z] * r
        sc[k, z + 1, 8 : 8 + X, :] = s
        xs_sc[0, k, pl.ds(z, 1), :] = s[0:1]
        if k != 1:
            xs_sc[1, k, pl.ds(z, 1), :] = s[X - 1 : X]
        return s

    def scale_all(k, packed, first):
        def body(b, packed):
            block = []
            for p in range(2):
                z = 2 * b + p
                block.append(scale(k, z))
            return put(packed, jnp.concatenate(block, axis=0), first + b)

        return each(NB, body, packed)

    arrived(0)
    scale(0, Z - 1)
    arrived(1)
    xs_sc[1, 1] = face_r[:, 7, :] * (1.0 / face_e[:, 7, :])
    arrived(2)
    ys_sc[2 * third :] = scale_all(2, jnp.zeros((L, L), F32), 0).T[:third]
    pl.semaphore_wait(barrier, len(near))

    known = [
        near,
        [at(**{a: d}) for a in AXES for d in (2, -2) if sizes[a] > 4 or (sizes[a] == 4 and d > 0)],
        [at(gz=d) for d in (4, -4) if sizes["gz"] > 8],
    ]

    def tell(i):
        for other in known[i]:
            pl.semaphore_signal(present.at[i], inc=1, device_id=other, device_id_type=MESH)

    def told(i):
        if known[i]:
            pl.semaphore_wait(present.at[i], len(known[i]))

    for m in (sc_yu2, sc_xu1, sc_zu0):
        m.start()
    tell(0)
    arrived(3)
    packed = scale_all(1, jnp.zeros((L, L), F32), NB)
    arrived(4)

    def bulk(b, packed):
        block = [scale(0, 2 * b), scale(0, 2 * b + 1)]
        return put(packed, jnp.concatenate(block, axis=0), b)

    packed = each(NB - 1, bulk, packed)
    block = [scale(0, Z - 2), sc[0, Z, 8 : 8 + X, :]]
    packed = put(packed, jnp.concatenate(block, axis=0), NB - 1)
    ys_sc[0 : 2 * third] = packed.T[: 2 * third]
    for m in rest:
        m.start()

    load_ns.wait()
    load_cs.wait()

    def invert(z, _):
        ns[z] = 1.0 / (6.0 + ns[z])
        return 0

    lax.fori_loop(0, Z, invert, 0, unroll=2)
    twice = (iota((L // 2, L), 0) == iota((L // 2, L), 1) // 2).astype(F32)
    wide = jnp.dot(
        cs[...].reshape(ZC * XC, L // 2), twice,
        precision=lax.Precision.HIGHEST, preferred_element_type=F32,
    )
    cd[...] = (1.0 / (6.0 + wide)).reshape(ZC, XC, L)

    def pack_coarse(planes):
        packed = jnp.zeros((L, L), F32)
        for q in range(NBC):
            packed = put(packed, planes(PC * q, PC * (q + 1)).reshape(L, L), q)
        return packed

    cdxs[...] = cd[:, XC - 1, :]
    cdys[...] = pack_coarse(lambda a, b: cd[a:b]).T[:8]
    fixed = [
        message(cd.at[ZC - 1], cdz, "gz", 1),
        message(cdxs, cdx, "gx", 1),
        message(cdys, cdy, "gy", 1),
    ]
    for m in fixed:
        m.start()

    for m in (sc_yu2, sc_xu1, sc_zu0):
        m.wait_recv()
    told(0)
    tell(1)
    sc[1, 1 : Z + 1, 7, :] = xr_sc[0, 1]
    low = yr_sc[0, 2 * third :]
    unpack(rt_g, low, jnp.zeros_like(low))

    def guess(b, packed):
        block = []
        for p in range(2):
            z = 2 * b + p
            s0, s0m = sc[0, z + 1, 8 : 8 + X, :], sc[0, z, 8 : 8 + X, :]
            s1, s1m = sc[1, z + 1, 8 : 8 + X, :], sc[1, z + 1, 7 : 7 + X, :]
            s2 = sc[2, z + 1, 8 : 8 + X, :]
            s2m = before(s2, halo(rt_g, p * X, X, b), lane)
            g = ((s0m - s0) + (s1m - s1) + (s2m - s2)) * ns[z]
            fg[z + 1, 8 : 8 + X, :] = g
            xs_fg[0, pl.ds(z, 1), :] = g[0:1]
            xs_fg[1, pl.ds(z, 1), :] = g[X - 1 : X]
            block.append(g)
        return put(packed, jnp.concatenate(block, axis=0), b)

    packed = each(NB, guess, jnp.zeros((L, L), F32))
    ys_fg[...] = packed.T[: 2 * NB]
    fg_m = [
        message(ys_fg, yr_fg.at[0], "gy", 1),
        message(ys_fg, yr_fg.at[1], "gy", -1),
        message(xs_fg.at[1], xr_fg.at[0], "gx", 1),
        message(xs_fg.at[0], xr_fg.at[1], "gx", -1),
        message(fg.at[Z, inner, :], fg.at[0, inner, :], "gz", 1),
        message(fg.at[1, inner, :], fg.at[Z + 1, inner, :], "gz", -1),
    ]
    for m in fg_m:
        m.start()

    for m in fg_m:
        m.wait_recv()
    told(1)
    tell(2)
    fg[1 : Z + 1, 7, :] = xr_fg[0]
    fg[1 : Z + 1, 8 + X, :] = xr_fg[1]
    unpack(rt_fg, yr_fg[0], yr_fg[1])

    def swap(x):
        return jnp.where(evenc, pltpu.roll(x, L - 1, 1), pltpu.roll(x, 1, 1))

    def restrict(b, _):
        total = None
        for p in range(2):
            z = 2 * b + p
            g = fg[z + 1, 8 : 8 + X, :]
            h = halo(rt_fg, p * X, X, b)
            n = fg[z, 8 : 8 + X, :] + fg[z + 2, 8 : 8 + X, :]
            n += fg[z + 1, 7 : 7 + X, :] + fg[z + 1, 9 : 9 + X, :]
            n += before(g, h, lane) + after(g, h, lane)
            ab[0, z, 0:X, :] = g + n * ns[z]
            total = n if p == 0 else total + n
        tmp[b] = total
        return 0

    each(ZC, restrict, 0)

    def direction(b, _):
        u = tmp[b, pl.ds(0, XC, 2), :] + tmp[b, pl.ds(1, XC, 2), :]
        u = u + swap(u)
        cr[b] = u
        v = u * cd[b]
        v1[b + 1, 8 : 8 + XC, :] = v
        xs_v1[0, pl.ds(b, 1), :] = v[0:1]
        xs_v1[1, pl.ds(b, 1), :] = v[XC - 1 : XC]
        x2s[pl.ds(b, 1), :] = v[XC - 2 : XC - 1]
        return 0

    each(ZC, direction, 0)

    def coarse_faces(v, xs, xr, ys, yr):
        mid = pl.ds(8, XC)
        return [
            message(ys, yr.at[0], "gy", 1),
            message(ys, yr.at[1], "gy", -1),
            message(xs.at[1], xr.at[0], "gx", 1),
            message(xs.at[0], xr.at[1], "gx", -1),
            message(v.at[ZC, mid, :], v.at[0, mid, :], "gz", 1),
            message(v.at[1, mid, :], v.at[ZC + 1, mid, :], "gz", -1),
        ]

    def coarse_arrive(sent, v, xr, yr, rt):
        for m in sent:
            m.wait_recv()
        v[1 : ZC + 1, 7, :] = xr[0]
        v[1 : ZC + 1, 8 + XC, :] = xr[1]
        unpack(rt, yr[0], yr[1])

    def around(v, wy, rt, b):
        c = v[b + 1, 8 : 8 + XC, :]
        h = halo(rt, (b % PC) * XC, XC, b // PC)
        w = jnp.where(evenc, before(c, h, lanec), after(c, h, lanec))
        wy[b] = w
        n = v[b, 8 : 8 + XC, :] + v[b + 2, 8 : 8 + XC, :]
        n += v[b + 1, 7 : 7 + XC, :] + v[b + 1, 9 : 9 + XC, :]
        return c, n + (w + swap(w))

    v1_x = [
        message(xs_v1.at[1], dv.at[0], "gz", 1, "gx", 1),
        message(xs_v1.at[0], dv.at[1], "gz", 1, "gx", -1),
        message(xs_v1.at[1], dv.at[2], "gz", -1, "gx", 1),
        message(xs_v1.at[1], dv.at[3], "gx", 1, "gy", 1),
        message(xs_v1.at[1], dv.at[4], "gx", 1, "gy", -1),
        message(x2s, x2r, "gx", 1),
        message(v1.at[ZC - 1, pl.ds(8, XC), :], v1b, "gz", 1),
    ]
    v1_y = [
        message(ys_v1, dv.at[5], "gz", 1, "gy", 1),
        message(ys_v1, dv.at[6], "gz", 1, "gy", -1),
        message(ys_v1, dv.at[7], "gz", -1, "gy", 1),
        message(ys_v1, dv.at[8], "gx", 1, "gy", 1),
        message(ys_v1, dv.at[9], "gx", -1, "gy", 1),
        message(y2s, y2r, "gy", 1),
    ]
    v1_f = coarse_faces(v1, xs_v1, xr_v1, ys_v1, yr_v1)
    for m in v1_x + v1_f[2:]:
        m.start()
    packed = pack_coarse(lambda a, b: v1[1 + a : 1 + b, 8 : 8 + XC, :])
    for q in range(NBC):
        block = v1[1 + PC * q : 1 + PC * (q + 1), 8 : 8 + XC, :].reshape(L, L)
        to = L // 4 + q
        packed = jnp.where(
            lax.shift_right_logical(lane2, 1) == to, pltpu.roll(block, 2 * to + 3, 1), packed
        )
    turned = packed.T
    ys_v1[...] = turned[:8]
    y2s[...] = turned[L // 2 : L // 2 + 8]
    for m in v1_y + v1_f[:2]:
        m.start()
    coarse_arrive(v1_f, v1, xr_v1, yr_v1, rt_v1)

    def first(b, sums):
        g1, g2, h11, h12 = sums
        c, n = around(v1, wy1, rt_v1, b)
        r = cr[b]
        a = r - n
        w = a * cd[b]
        v2[b + 1, 8 : 8 + XC, :] = w
        xs_v2[pl.ds(b, 1), :] = w[0:1]
        return g1 + c * r, g2 + w * r, h11 + c * a, h12 + w * a

    sums = each(ZC, first, (zero_coarse,) * 4)
    for m in v1_x + v1_y + fixed:
        m.wait_recv()
    v1[0, 7:8, :] = dv[0, 7:8, :]
    v1[0, 8 + XC : 9 + XC, :] = dv[1, 7:8, :]
    unpack(rt_d, dv[5], dv[6])
    c = v1[0, 8 : 8 + XC, :]
    h = halo(rt_d, ((ZC - 1) % PC) * XC, XC, (ZC - 1) // PC)
    w = jnp.where(evenc, before(c, h, lanec), after(c, h, lanec))
    n = v1b[...] + v1[1, 8 : 8 + XC, :] + v1[0, 7 : 7 + XC, :] + v1[0, 9 : 9 + XC, :]
    below_z = c - cdz[...] * (n + (w + swap(w)))

    row, line = iota((8, L), 0), iota((8, L), 1)
    even = line % 2 == 0
    c = xr_v1[0]
    n = x2r[...] + xs_v1[0]
    n += jnp.where(row == 0, pltpu.roll(dv[0], 1, 0), pltpu.roll(c, 1, 0))
    n += jnp.where(row == 7, pltpu.roll(dv[2], 7, 0), pltpu.roll(c, 7, 0))
    low = jnp.where(line == 0, pltpu.roll(dv[3], 1, 1), pltpu.roll(c, 1, 1))
    high = jnp.where(line == L - 1, pltpu.roll(dv[4], L - 1, 1), pltpu.roll(c, L - 1, 1))
    w = jnp.where(even, low, high)
    n += w + jnp.where(even, pltpu.roll(w, L - 1, 1), pltpu.roll(w, 1, 1))
    below_x = c - cdx[...] * n

    c = yr_v1[0]
    n = y2r[...] + pltpu.roll(ys_v1[...], 7, 0)
    down = jnp.where(row >= 2, pltpu.roll(c, 2, 0), pltpu.roll(dv[5], 6, 0))
    up = jnp.where(row < 2, pltpu.roll(c, 6, 0), pltpu.roll(dv[7], 2, 0))
    n += pltpu.roll(jnp.where(line < L - XC, c, down), XC, 1)
    n += pltpu.roll(jnp.where(line >= XC, c, up), L - XC, 1)
    n += jnp.where(line % XC == 0, pltpu.roll(dv[8], L - XC + 1, 1), pltpu.roll(c, 1, 1))
    n += jnp.where(line % XC == XC - 1, pltpu.roll(dv[9], XC - 1, 1), pltpu.roll(c, L - 1, 1))
    below_y = c - cdy[...] * n

    packed = pack_coarse(lambda a, b: v2[1 + a : 1 + b, 8 : 8 + XC, :])
    ys_v2[...] = packed.T[:8]
    v2_m = [
        message(ys_v2, yr_v2, "gy", -1),
        message(xs_v2, xr_v2, "gx", -1),
        message(v2.at[1, pl.ds(8, XC), :], v2.at[ZC + 1, pl.ds(8, XC), :], "gz", -1),
    ]
    for m in v2_m:
        m.start()
    nothing = jnp.zeros((XC, L), F32)
    v2[0, 8 : 8 + XC, :] = below_z
    v2[1 : ZC + 1, 7, :] = below_x

    def pairs(b, sums):
        c = v2[b + 1, 8 : 8 + XC, :]
        w = jnp.where(evenc, before(c, nothing, lanec), after(c, nothing, lanec))
        n = v2[b, 8 : 8 + XC, :] + v2[b + 1, 7 : 7 + XC, :]
        return sums + c * (2.0 * n + 2.0 * w)

    inside = each(ZC, pairs, zero_coarse)
    side = jnp.where((row == 0) | (row == 2), pltpu.roll(ys_v2[...], 7, 0) * below_y, 0.0)
    total = sums[3] - inside
    total = total - jnp.concatenate([4.0 * side, jnp.zeros((XC - 8, L), F32)], axis=0)
    sums += (total,)

    row = jnp.zeros((1, L), F32)
    for i, s in enumerate(sums):
        one = jnp.sum(jnp.sum(s, axis=0, keepdims=True), axis=1, keepdims=True)
        row = jnp.where(iota((1, L), 1) == i, one, row)
    ar1[0] = row

    def spread_round(buf, others, base):
        copies = [
            pltpu.make_async_remote_copy(
                src_ref=buf.at[0], dst_ref=buf.at[d + 1], send_sem=ar_send.at[base + d],
                recv_sem=ar_recv.at[base + d], device_id=other, device_id_type=MESH,
            )
            for d, other in enumerate(others)
        ]
        for copy in copies:
            copy.start()
        return copies

    round1 = spread_round(ar1, plane, 0)

    def prolong(v, wy, j):
        def body(b, _):
            w = 3.0 * v[b + 1, 8 : 8 + XC, :] + wy[b]
            for px in range(2):
                wx = w + v[b + 1, 7 + 2 * px : 7 + 2 * px + XC, :]
                for pz in range(2):
                    z = 2 * b + pz
                    n = wx + v[b + 2 * pz, 8 : 8 + XC, :]
                    ab[j, z, pl.ds(px, XC, 2), :] = n * ns[z, pl.ds(px, XC, 2), :]
            return 0

        each(ZC, body, 0)

    prolong(v1, wy1, 1)
    def smooth(k):
        def body(b, _):
            for p in range(2):
                z = 2 * b + p
                s = sc[k, z + 1, 8 : 8 + X, :]
                h = halo(rt_sc, p * X, X, k * NB + b)
                n = sc[k, z, 8 : 8 + X, :] + sc[k, z + 2, 8 : 8 + X, :]
                n += sc[k, z + 1, 7 : 7 + X, :] + sc[k, z + 1, 9 : 9 + X, :]
                n += before(s, h, lane) + after(s, h, lane)
                out[k, z] = s + n * ed[k, z]
            return 0

        each(NB, body, 0)

    def fill_rows():
        for m in rest:
            m.wait_recv()
        for k in range(3):
            if k != 1:
                sc[k, 1 : Z + 1, 7, :] = xr_sc[0, k]
            sc[k, 1 : Z + 1, 8 + X, :] = xr_sc[1, k]
        unpack(rt_sc, yr_sc[0], yr_sc[1])

    fill_rows()
    smooth(0)

    for copy in round1:
        copy.wait_recv()
    ar2[0] = jnp.sum(ar1[...], axis=0)
    told(2)
    round2 = spread_round(ar2, partners, len(plane))

    for m in v2_m:
        m.wait_recv()
    v2[1 : ZC + 1, 8 + XC, :] = xr_v2[...]
    unpack(rt_v2, below_y, yr_v2[...])

    def sides(b, _):
        c = v2[b + 1, 8 : 8 + XC, :]
        h = halo(rt_v2, (b % PC) * XC, XC, b // PC)
        wy2[b] = jnp.where(evenc, before(c, h, lanec), after(c, h, lanec))
        return 0

    each(ZC, sides, 0)
    prolong(v2, wy2, 2)

    def fill(j):
        def body(b, packed):
            block = []
            for p in range(2):
                z = 2 * b + p
                x = ab[j, z, 0:X, :]
                xs_ab[j, pl.ds(z, 1), :] = x[0:1]
                block.append(x)
            return put(packed, jnp.concatenate(block, axis=0), j * NB + b)

        return body

    packed = jnp.zeros((L, L), F32)
    for j in range(3):
        packed = each(NB, fill(j), packed)
    ys_ab[...] = packed.T[: 6 * NB]
    ab_m = [
        message(ab.at[:, 0, pl.ds(0, X), :], ab.at[:, Z, pl.ds(0, X), :], "gz", -1),
        message(xs_ab, xr_ab, "gx", -1),
        message(ys_ab, yr_ab, "gy", -1),
    ]
    for m in ab_m:
        m.start()

    smooth(1)
    smooth(2)
    for m in ab_m:
        m.wait_recv()
    ab[:, 0:Z, X, :] = xr_ab[...]
    rt_ab[...] = jnp.concatenate(
        [pltpu.roll(yr_ab[...], 6 * NB - 1, 0), jnp.zeros((L - 6 * NB, L), F32)], axis=0
    ).T

    def gradient(j, into, add):
        def body(b, _):
            for p in range(2):
                z = 2 * b + p
                f = ab[j, z, 0:X, :]
                h = halo(rt_ab, p * X, X, j * NB + b)
                d = (ab[j, z + 1, 0:X, :] - f, ab[j, z, 1 : X + 1, :] - f, after(f, h, lane) - f)
                for k in range(3):
                    into[k, z] = into[k, z] + d[k] if add else d[k]
            return 0

        each(NB, body, 0)

    gradient(0, out, True)
    gradient(1, res, False)
    gradient(2, ed, False)

    for copy in round2:
        copy.wait_recv()
    total = jnp.sum(ar2[...], axis=0)
    g1, g2, h11, h12, h22 = (
        jnp.sum(jnp.where(iota((1, L), 1) == i, total, 0.0), axis=1, keepdims=True) for i in range(5)
    )
    c2 = (g2 - h12 * g1 / h11) / (h22 - h12 * h12 / h11)
    c1 = (g1 - h12 * c2) / h11

    def finish(z, _):
        for k in range(3):
            out[k, z] = out[k, z] + c1 * res[k, z] + c2 * ed[k, z]
        return 0

    lax.fori_loop(0, Z, finish, 0, unroll=2)

    for m in used:
        m.wait_send()
    for copy in round1 + round2:
        copy.wait_send()


def solution(mesh):
    sizes = dict(mesh.shape)
    n_ar = sizes["gz"] - 1 + sizes["gx"] * sizes["gy"] - 1

    def local(residual, edge_diag, node_shift, coarse_shift):
        _, Z, X, Y = residual.shape
        ZC, XC, NB = Z // 2, X // 2, Z // 2
        assert X == 64 and Y == L and Z % 8 == 0

        def v(*shape):
            return pltpu.VMEM(shape, F32)

        scratch = [
            v(3, Z, X, L), v(3, Z, X, L), v(Z, X, L), v(ZC, XC, L // 2),
            v(3, Z + 2, X + 16, L), v(Z + 2, X + 16, L), v(ZC, X, L),
            v(ZC, XC, L), v(ZC, XC, L),
            v(ZC + 2, XC + 16, L), v(ZC + 2, XC + 16, L),
            v(ZC, XC, L), v(ZC, XC, L),
            v(3, Z + 1, X + 8, L), v(Z, 8, L), v(Z, 8, L),
            v(L, L), v(L, L), v(L, L), v(L, L), v(L, L), v(L, L), v(L, L),
            v(10, 8, L), v(XC, L), v(ZC, L), v(ZC, L), v(8, L), v(8, L),
            v(XC, L), v(ZC, L), v(ZC, L), v(8, L), v(8, L),
            v(2, 3, Z, L), v(2, 3, Z, L), v(2, Z, L), v(2, Z, L),
            v(2, ZC, L), v(2, ZC, L), v(ZC, L), v(ZC, L), v(3, Z, L), v(3, Z, L),
            v(6 * NB, L), v(2, 6 * NB, L), v(2 * NB, L), v(2, 2 * NB, L),
            v(8, L), v(2, 8, L), v(8, L), v(8, L), v(6 * NB, L), v(6 * NB, L),
            v(sizes["gx"] * sizes["gy"], 1, L), v(sizes["gz"], 1, L), pltpu.SemaphoreType.REGULAR((3,)),
            pltpu.SemaphoreType.DMA((12,)),
            pltpu.SemaphoreType.DMA((56,)), pltpu.SemaphoreType.DMA((56,)),
            pltpu.SemaphoreType.DMA((n_ar,)), pltpu.SemaphoreType.DMA((n_ar,)),
        ]
        return pl.pallas_call(
            functools.partial(kernel, sizes),
            out_shape=jax.ShapeDtypeStruct(residual.shape, F32),
            in_specs=[pl.BlockSpec(memory_space=pl.ANY)] * 4,
            out_specs=pl.BlockSpec(memory_space=pltpu.VMEM),
            scratch_shapes=scratch,
            compiler_params=pltpu.CompilerParams(
                collective_id=0, has_side_effects=True, vmem_limit_bytes=48 * 1024 * 1024
            ),
        )(*(
            pltpu.with_memory_space_constraint(x, pltpu.HBM)
            for x in (residual, edge_diag, node_shift, coarse_shift)
        ))

    fine, coarse = P(None, "gz", "gx", "gy"), P("gz", "gx", "gy")
    return jax.shard_map(
        local, mesh=mesh, in_specs=(fine, fine, coarse, coarse), out_specs=fine, check_vma=False
    )
```

```python
import functools

import jax
import jax.numpy as jnp
from jax import lax
from jax.experimental import pallas as pl
from jax.experimental.pallas import tpu as pltpu
from jax.sharding import PartitionSpec as P

MESH = pl.DeviceIdType.MESH
AXES = ("gx", "gy", "gz")
L = 128
F32 = jnp.float32


def iota(shape, dim):
    return lax.broadcasted_iota(jnp.int32, shape, dim)


class Message:
    def __init__(self, copy, sends, receives):
        self.copy, self.sends, self.receives = copy, sends, receives

    def start(self):
        pl.when(self.sends)(lambda: self.copy.start())

    def wait_recv(self):
        pl.when(self.receives)(lambda: self.copy.wait_recv())

    def wait_send(self):
        pl.when(self.sends)(lambda: self.copy.wait_send())


def kernel(
    sizes, res_h, ed_h, ns_h, cs_h, out,
    res, ed, ns, cs, sc, fg, tmp, cr, cd, v1, v2, wy1, wy2, ab, face_e, face_r,
    rt_g, rt_sc, rt_fg, rt_v1, rt_v2, rt_ab, rt_d,
    dv, v1b, x2s, x2r, y2s, y2r, cdz, cdxs, cdx, cdys, cdy,
    xs_sc, xr_sc, xs_fg, xr_fg, xs_v1, xr_v1, xs_v2, xr_v2, xs_ab, xr_ab,
    ys_sc, yr_sc, ys_fg, yr_fg, ys_v1, yr_v1, ys_v2, yr_v2, ys_ab, yr_ab,
    arow, ar1, ar2, present, in_sem, send_sem, recv_sem, ar_send, ar_recv, out_send, out_recv,
):
    _, Z, X, _ = res.shape
    ZC, XC = Z // 2, X // 2
    NB = Z // 2
    PC = L // XC
    NBC = ZC // PC
    me = {a: lax.axis_index(a) for a in AXES}
    core = lax.rem(me["gz"], 2)
    used = []

    def both(flags):
        return functools.reduce(jnp.logical_and, flags)

    def message(src, dst, *steps):
        i = len(used)
        steps = dict(zip(steps[::2], steps[1::2]))
        copy = pltpu.make_async_remote_copy(
            src_ref=src, dst_ref=dst, send_sem=send_sem.at[i], recv_sem=recv_sem.at[i],
            device_id={a: me[a] + d for a, d in steps.items()}, device_id_type=MESH,
        )
        low = {a: me[a] > 0 for a in steps}
        high = {a: me[a] < sizes[a] - 1 for a in steps}
        made = Message(
            copy,
            both([high[a] if d > 0 else low[a] for a, d in steps.items()]),
            both([low[a] if d > 0 else high[a] for a, d in steps.items()]),
        )
        used.append(made)
        return made

    def load(i, pick, into):
        return (
            pltpu.make_async_copy(pick(ed_h), into(ed, face_e), in_sem.at[2 * i]),
            pltpu.make_async_copy(pick(res_h), into(res, face_r), in_sem.at[2 * i + 1]),
        )

    loads = [
        load(0, lambda h: h.at[0, Z - 1], lambda v, f: v.at[0, Z - 1]),
        load(1, lambda h: h.at[1, :, pl.ds(X - 8, 8), :], lambda v, f: f),
        load(2, lambda h: h.at[2], lambda v, f: v.at[2]),
        load(3, lambda h: h.at[1], lambda v, f: v.at[1]),
        load(4, lambda h: h.at[0, pl.ds(0, Z - 1)], lambda v, f: v.at[0, pl.ds(0, Z - 1)]),
    ]
    load_ns = pltpu.make_async_copy(ns_h, ns, in_sem.at[10])
    load_cs = pltpu.make_async_copy(cs_h, cs, in_sem.at[11])
    for pair in loads[:3]:
        for copy in pair:
            copy.start()

    def at(**steps):
        return {a: lax.rem(me[a] + d + sizes[a], sizes[a]) for a, d in steps.items()}

    near = [at(**{a: d}) for a in AXES for d in (1, -1)]
    barrier = pltpu.get_barrier_semaphore()

    zero_coarse = jnp.zeros((XC, L), F32)

    @pl.when(me["gz"] >= 0)
    def _():
        zero_plane = jnp.zeros((X, L), F32)
        for k in range(3):
            for z in (0, Z + 1):
                sc[k, z, 8 : 8 + X, :] = zero_plane
            ab[k, Z, 0:X, :] = zero_plane
        for z in (0, Z + 1):
            fg[z, 8 : 8 + X, :] = zero_plane
        for z in (0, ZC + 1):
            v1[z, 8 : 8 + XC, :] = zero_coarse
        v2[ZC + 1, 8 : 8 + XC, :] = zero_coarse
        for ref in (
            xr_sc, xr_fg, xr_v1, xr_v2, xr_ab, yr_sc, yr_fg, yr_v1, yr_v2, yr_ab,
            dv, v1b, x2r, y2r, cdz, cdx, cdy,
        ):
            ref[...] = jnp.zeros(ref.shape, F32)

    for other in near:
        pl.semaphore_signal(barrier, inc=1, device_id=other, device_id_type=MESH)

    lane = iota((X, L), 1)
    lane2 = iota((L, L), 1)
    lanec = iota((XC, L), 1)
    evenc = lanec % 2 == 0

    def put(packed, block, q):
        return jnp.where(lax.shift_right_logical(lane2, 1) == q, pltpu.roll(block, 2 * q + 1, 1), packed)

    def halo(rt, row, rows, q):
        return pltpu.roll(rt[pl.ds(row, rows), :], L - 1 - 2 * q, 1)

    def before(x, h, at):
        return jnp.where(at == 0, h, pltpu.roll(x, 1, 1))

    def after(x, h, at):
        return jnp.where(at == L - 1, h, pltpu.roll(x, L - 1, 1))

    def unpack(rt, low, high):
        n = low.shape[0]
        mixed = jnp.where(iota((n, L), 0) % 2 == 1, pltpu.roll(low, 1, 0), pltpu.roll(high, n - 1, 0))
        rt[...] = jnp.concatenate([mixed, jnp.zeros((L - n, L), F32)], axis=0).T

    def each(n, body, init):
        return lax.fori_loop(0, n, body, init, unroll=True)

    inner = pl.ds(8, X)
    third = 2 * NB
    sc_zu0 = message(sc.at[0, Z, inner, :], sc.at[0, 0, inner, :], "gz", 1)
    sc_xu1 = message(xs_sc.at[1, 1], xr_sc.at[0, 1], "gx", 1)
    sc_yu2 = message(ys_sc.at[pl.ds(2 * third, third)], yr_sc.at[0, pl.ds(2 * third, third)], "gy", 1)
    rest = [
        message(xs_sc.at[1, 0], xr_sc.at[0, 0], "gx", 1),
        message(xs_sc.at[1, 2], xr_sc.at[0, 2], "gx", 1),
        message(xs_sc.at[0], xr_sc.at[1], "gx", -1),
        message(ys_sc.at[pl.ds(0, 2 * third)], yr_sc.at[0, pl.ds(0, 2 * third)], "gy", 1),
        message(ys_sc, yr_sc.at[1], "gy", -1),
        message(sc.at[1:3, Z, inner, :], sc.at[1:3, 0, inner, :], "gz", 1),
        message(sc.at[:, 1, inner, :], sc.at[:, Z + 1, inner, :], "gz", -1),
    ]

    def arrived(i):
        for copy in loads[i]:
            copy.wait()

    def scale(k, z):
        r = 1.0 / ed[k, z]
        ed[k, z] = r
        s = res[k, z] * r
        sc[k, z + 1, 8 : 8 + X, :] = s
        xs_sc[0, k, pl.ds(z, 1), :] = s[0:1]
        if k != 1:
            xs_sc[1, k, pl.ds(z, 1), :] = s[X - 1 : X]
        return s

    def scale_all(k, packed, first):
        def body(b, packed):
            block = []
            for p in range(2):
                z = 2 * b + p
                block.append(scale(k, z))
            return put(packed, jnp.concatenate(block, axis=0), first + b)

        return each(NB, body, packed)

    arrived(0)
    scale(0, Z - 1)
    arrived(1)
    xs_sc[1, 1] = face_r[:, 7, :] * (1.0 / face_e[:, 7, :])
    arrived(2)
    for pair in loads[3:]:
        for copy in pair:
            copy.start()
    load_ns.start()
    load_cs.start()
    ys_sc[2 * third :] = scale_all(2, jnp.zeros((L, L), F32), 0).T[:third]
    pl.semaphore_wait(barrier, len(near))

    known = [
        near,
        [at(**{a: d}) for a in AXES for d in (2, -2) if sizes[a] > 4 or (sizes[a] == 4 and d > 0)],
        [at(gz=d) for d in (4, -4) if sizes["gz"] > 8] + [{"gz": me["gz"] + 1 - 2 * core}],
    ]

    def tell(i):
        for other in known[i]:
            pl.semaphore_signal(present.at[i], inc=1, device_id=other, device_id_type=MESH)

    def told(i):
        if known[i]:
            pl.semaphore_wait(present.at[i], len(known[i]))

    for m in (sc_yu2, sc_xu1, sc_zu0):
        m.start()
    tell(0)
    arrived(3)
    packed = scale_all(1, jnp.zeros((L, L), F32), NB)
    arrived(4)

    def bulk(b, packed):
        block = [scale(0, 2 * b), scale(0, 2 * b + 1)]
        return put(packed, jnp.concatenate(block, axis=0), b)

    packed = each(NB - 1, bulk, packed)
    block = [scale(0, Z - 2), sc[0, Z, 8 : 8 + X, :]]
    packed = put(packed, jnp.concatenate(block, axis=0), NB - 1)
    ys_sc[0 : 2 * third] = packed.T[: 2 * third]
    for m in rest:
        m.start()

    load_ns.wait()
    load_cs.wait()

    def invert(z, _):
        ns[z] = 1.0 / (6.0 + ns[z])
        return 0

    lax.fori_loop(0, Z, invert, 0, unroll=2)
    twice = (iota((L // 2, L), 0) == iota((L // 2, L), 1) // 2).astype(F32)
    wide = jnp.dot(
        cs[...].reshape(ZC * XC, L // 2), twice,
        precision=lax.Precision.HIGHEST, preferred_element_type=F32,
    )
    cd[...] = (1.0 / (6.0 + wide)).reshape(ZC, XC, L)

    def pack_coarse(planes):
        packed = jnp.zeros((L, L), F32)
        for q in range(NBC):
            packed = put(packed, planes(PC * q, PC * (q + 1)).reshape(L, L), q)
        return packed

    cdxs[...] = cd[:, XC - 1, :]
    cdys[...] = pack_coarse(lambda a, b: cd[a:b]).T[:8]
    fixed = [
        message(cd.at[ZC - 1], cdz, "gz", 1),
        message(cdxs, cdx, "gx", 1),
        message(cdys, cdy, "gy", 1),
    ]
    for m in fixed:
        m.start()

    for m in (sc_yu2, sc_xu1, sc_zu0):
        m.wait_recv()
    told(0)
    sc[1, 1 : Z + 1, 7, :] = xr_sc[0, 1]
    low = yr_sc[0, 2 * third :]
    unpack(rt_g, low, jnp.zeros_like(low))

    def guess(b, packed):
        block = []
        for p in range(2):
            z = 2 * b + p
            s0, s0m = sc[0, z + 1, 8 : 8 + X, :], sc[0, z, 8 : 8 + X, :]
            s1, s1m = sc[1, z + 1, 8 : 8 + X, :], sc[1, z + 1, 7 : 7 + X, :]
            s2 = sc[2, z + 1, 8 : 8 + X, :]
            s2m = before(s2, halo(rt_g, p * X, X, b), lane)
            g = ((s0m - s0) + (s1m - s1) + (s2m - s2)) * ns[z]
            fg[z + 1, 8 : 8 + X, :] = g
            xs_fg[0, pl.ds(z, 1), :] = g[0:1]
            xs_fg[1, pl.ds(z, 1), :] = g[X - 1 : X]
            block.append(g)
        return put(packed, jnp.concatenate(block, axis=0), b)

    packed = each(NB, guess, jnp.zeros((L, L), F32))
    ys_fg[...] = packed.T[: 2 * NB]
    fg_m = [
        message(ys_fg, yr_fg.at[0], "gy", 1),
        message(ys_fg, yr_fg.at[1], "gy", -1),
        message(xs_fg.at[1], xr_fg.at[0], "gx", 1),
        message(xs_fg.at[0], xr_fg.at[1], "gx", -1),
        message(fg.at[Z, inner, :], fg.at[0, inner, :], "gz", 1),
        message(fg.at[1, inner, :], fg.at[Z + 1, inner, :], "gz", -1),
    ]
    for m in fg_m:
        m.start()
    tell(1)

    for m in fg_m:
        m.wait_recv()
    told(1)
    fg[1 : Z + 1, 7, :] = xr_fg[0]
    fg[1 : Z + 1, 8 + X, :] = xr_fg[1]
    unpack(rt_fg, yr_fg[0], yr_fg[1])

    def swap(x):
        return jnp.where(evenc, pltpu.roll(x, L - 1, 1), pltpu.roll(x, 1, 1))

    def restrict(b, _):
        total = None
        for p in range(2):
            z = 2 * b + p
            g = fg[z + 1, 8 : 8 + X, :]
            h = halo(rt_fg, p * X, X, b)
            n = fg[z, 8 : 8 + X, :] + fg[z + 2, 8 : 8 + X, :]
            n += fg[z + 1, 7 : 7 + X, :] + fg[z + 1, 9 : 9 + X, :]
            n += before(g, h, lane) + after(g, h, lane)
            ab[0, z, 0:X, :] = g + n * ns[z]
            total = n if p == 0 else total + n
        tmp[b] = total
        return 0

    each(ZC, restrict, 0)

    def direction(b, _):
        u = tmp[b, pl.ds(0, XC, 2), :] + tmp[b, pl.ds(1, XC, 2), :]
        u = u + swap(u)
        cr[b] = u
        v = u * cd[b]
        v1[b + 1, 8 : 8 + XC, :] = v
        xs_v1[0, pl.ds(b, 1), :] = v[0:1]
        xs_v1[1, pl.ds(b, 1), :] = v[XC - 1 : XC]
        x2s[pl.ds(b, 1), :] = v[XC - 2 : XC - 1]
        return 0

    each(ZC, direction, 0)

    def coarse_faces(v, xs, xr, ys, yr):
        mid = pl.ds(8, XC)
        return [
            message(ys, yr.at[0], "gy", 1),
            message(ys, yr.at[1], "gy", -1),
            message(xs.at[1], xr.at[0], "gx", 1),
            message(xs.at[0], xr.at[1], "gx", -1),
            message(v.at[ZC, mid, :], v.at[0, mid, :], "gz", 1),
            message(v.at[1, mid, :], v.at[ZC + 1, mid, :], "gz", -1),
        ]

    def coarse_arrive(sent, v, xr, yr, rt):
        for m in sent:
            m.wait_recv()
        v[1 : ZC + 1, 7, :] = xr[0]
        v[1 : ZC + 1, 8 + XC, :] = xr[1]
        unpack(rt, yr[0], yr[1])

    def around(v, wy, rt, b):
        c = v[b + 1, 8 : 8 + XC, :]
        h = halo(rt, (b % PC) * XC, XC, b // PC)
        w = jnp.where(evenc, before(c, h, lanec), after(c, h, lanec))
        wy[b] = w
        n = v[b, 8 : 8 + XC, :] + v[b + 2, 8 : 8 + XC, :]
        n += v[b + 1, 7 : 7 + XC, :] + v[b + 1, 9 : 9 + XC, :]
        return c, n + (w + swap(w))

    v1_x = [
        message(xs_v1.at[1], dv.at[0], "gz", 1, "gx", 1),
        message(xs_v1.at[0], dv.at[1], "gz", 1, "gx", -1),
        message(xs_v1.at[1], dv.at[2], "gz", -1, "gx", 1),
        message(xs_v1.at[1], dv.at[3], "gx", 1, "gy", 1),
        message(xs_v1.at[1], dv.at[4], "gx", 1, "gy", -1),
        message(x2s, x2r, "gx", 1),
        message(v1.at[ZC - 1, pl.ds(8, XC), :], v1b, "gz", 1),
    ]
    v1_y = [
        message(ys_v1, dv.at[5], "gz", 1, "gy", 1),
        message(ys_v1, dv.at[6], "gz", 1, "gy", -1),
        message(ys_v1, dv.at[7], "gz", -1, "gy", 1),
        message(ys_v1, dv.at[8], "gx", 1, "gy", 1),
        message(ys_v1, dv.at[9], "gx", -1, "gy", 1),
        message(y2s, y2r, "gy", 1),
    ]
    v1_f = coarse_faces(v1, xs_v1, xr_v1, ys_v1, yr_v1)
    for m in v1_x + v1_f[2:]:
        m.start()
    packed = pack_coarse(lambda a, b: v1[1 + a : 1 + b, 8 : 8 + XC, :])
    for q in range(NBC):
        block = v1[1 + PC * q : 1 + PC * (q + 1), 8 : 8 + XC, :].reshape(L, L)
        to = L // 4 + q
        packed = jnp.where(
            lax.shift_right_logical(lane2, 1) == to, pltpu.roll(block, 2 * to + 3, 1), packed
        )
    turned = packed.T
    ys_v1[...] = turned[:8]
    y2s[...] = turned[L // 2 : L // 2 + 8]
    for m in v1_y + v1_f[:2]:
        m.start()
    tell(2)
    coarse_arrive(v1_f, v1, xr_v1, yr_v1, rt_v1)

    def first(b, sums):
        g1, g2, h11, h12 = sums
        c, n = around(v1, wy1, rt_v1, b)
        r = cr[b]
        a = r - n
        w = a * cd[b]
        v2[b + 1, 8 : 8 + XC, :] = w
        xs_v2[pl.ds(b, 1), :] = w[0:1]
        return g1 + c * r, g2 + w * r, h11 + c * a, h12 + w * a

    sums = each(ZC, first, (zero_coarse,) * 4)
    for m in v1_x + v1_y + fixed:
        m.wait_recv()
    v1[0, 7:8, :] = dv[0, 7:8, :]
    v1[0, 8 + XC : 9 + XC, :] = dv[1, 7:8, :]
    unpack(rt_d, dv[5], dv[6])
    c = v1[0, 8 : 8 + XC, :]
    h = halo(rt_d, ((ZC - 1) % PC) * XC, XC, (ZC - 1) // PC)
    w = jnp.where(evenc, before(c, h, lanec), after(c, h, lanec))
    n = v1b[...] + v1[1, 8 : 8 + XC, :] + v1[0, 7 : 7 + XC, :] + v1[0, 9 : 9 + XC, :]
    below_z = c - cdz[...] * (n + (w + swap(w)))

    row, line = iota((8, L), 0), iota((8, L), 1)
    even = line % 2 == 0
    c = xr_v1[0]
    n = x2r[...] + xs_v1[0]
    n += jnp.where(row == 0, pltpu.roll(dv[0], 1, 0), pltpu.roll(c, 1, 0))
    n += jnp.where(row == 7, pltpu.roll(dv[2], 7, 0), pltpu.roll(c, 7, 0))
    low = jnp.where(line == 0, pltpu.roll(dv[3], 1, 1), pltpu.roll(c, 1, 1))
    high = jnp.where(line == L - 1, pltpu.roll(dv[4], L - 1, 1), pltpu.roll(c, L - 1, 1))
    w = jnp.where(even, low, high)
    n += w + jnp.where(even, pltpu.roll(w, L - 1, 1), pltpu.roll(w, 1, 1))
    below_x = c - cdx[...] * n

    c = yr_v1[0]
    n = y2r[...] + pltpu.roll(ys_v1[...], 7, 0)
    down = jnp.where(row >= 2, pltpu.roll(c, 2, 0), pltpu.roll(dv[5], 6, 0))
    up = jnp.where(row < 2, pltpu.roll(c, 6, 0), pltpu.roll(dv[7], 2, 0))
    n += pltpu.roll(jnp.where(line < L - XC, c, down), XC, 1)
    n += pltpu.roll(jnp.where(line >= XC, c, up), L - XC, 1)
    n += jnp.where(line % XC == 0, pltpu.roll(dv[8], L - XC + 1, 1), pltpu.roll(c, 1, 1))
    n += jnp.where(line % XC == XC - 1, pltpu.roll(dv[9], XC - 1, 1), pltpu.roll(c, L - 1, 1))
    below_y = c - cdy[...] * n

    packed = pack_coarse(lambda a, b: v2[1 + a : 1 + b, 8 : 8 + XC, :])
    ys_v2[...] = packed.T[:8]
    v2_m = [
        message(ys_v2, yr_v2, "gy", -1),
        message(xs_v2, xr_v2, "gx", -1),
        message(v2.at[1, pl.ds(8, XC), :], v2.at[ZC + 1, pl.ds(8, XC), :], "gz", -1),
    ]
    for m in v2_m:
        m.start()
    nothing = jnp.zeros((XC, L), F32)
    v2[0, 8 : 8 + XC, :] = below_z
    v2[1 : ZC + 1, 7, :] = below_x

    def pairs(b, sums):
        c = v2[b + 1, 8 : 8 + XC, :]
        w = jnp.where(evenc, before(c, nothing, lanec), after(c, nothing, lanec))
        n = v2[b, 8 : 8 + XC, :] + v2[b + 1, 7 : 7 + XC, :]
        return sums + c * (2.0 * n + 2.0 * w)

    inside = each(ZC, pairs, zero_coarse)
    side = jnp.where((row == 0) | (row == 2), pltpu.roll(ys_v2[...], 7, 0) * below_y, 0.0)
    total = sums[3] - inside
    total = total - jnp.concatenate([4.0 * side, jnp.zeros((XC - 8, L), F32)], axis=0)
    sums += (total,)

    row = jnp.zeros((1, L), F32)
    for i, s in enumerate(sums):
        one = jnp.sum(jnp.sum(s, axis=0, keepdims=True), axis=1, keepdims=True)
        row = jnp.where(iota((1, L), 1) == i, one, row)
    arow[...] = row

    spots = [(dx, dy) for dx in range(sizes["gx"]) for dy in range(sizes["gy"])]
    n_spots, n_chips = len(spots), sizes["gz"] // 2

    def remote(src, dst, i, j, sends, receives, other):
        return pltpu.make_async_remote_copy(
            src_ref=src, dst_ref=dst, send_sem=sends.at[i], recv_sem=receives.at[j],
            device_id=other, device_id_type=MESH,
        )

    gather = [
        [
            remote(arow, ar1.at[n_spots * c + i], i, n_spots * c + i, ar_send, ar_recv, at(gx=dx, gy=dy, gz=1 - c))
            for i, (dx, dy) in enumerate(spots) if c == 0 or i > 0
        ]
        for c in range(2)
    ]
    scatter = [
        remote(ar2.at[0], ar2.at[d], 2 * d + c, d, out_send, out_recv, at(gz=2 * d - c))
        for d in range(n_chips) for c in range(2) if d or c
    ]
    told(2)

    @pl.when(core == 0)
    def _():
        for copy in gather[0]:
            copy.start()

    @pl.when(core == 1)
    def _():
        for copy in gather[1]:
            copy.start()
        ar1[n_spots] = arow[...]

    def prolong(v, wy, j):
        def body(b, _):
            w = 3.0 * v[b + 1, 8 : 8 + XC, :] + wy[b]
            for px in range(2):
                wx = w + v[b + 1, 7 + 2 * px : 7 + 2 * px + XC, :]
                for pz in range(2):
                    z = 2 * b + pz
                    n = wx + v[b + 2 * pz, 8 : 8 + XC, :]
                    ab[j, z, pl.ds(px, XC, 2), :] = n * ns[z, pl.ds(px, XC, 2), :]
            return 0

        each(ZC, body, 0)

    prolong(v1, wy1, 1)
    def smooth(k):
        def body(b, _):
            for p in range(2):
                z = 2 * b + p
                s = sc[k, z + 1, 8 : 8 + X, :]
                h = halo(rt_sc, p * X, X, k * NB + b)
                n = sc[k, z, 8 : 8 + X, :] + sc[k, z + 2, 8 : 8 + X, :]
                n += sc[k, z + 1, 7 : 7 + X, :] + sc[k, z + 1, 9 : 9 + X, :]
                n += before(s, h, lane) + after(s, h, lane)
                out[k, z] = s + n * ed[k, z]
            return 0

        each(NB, body, 0)

    def fill_rows():
        for m in rest:
            m.wait_recv()
        for k in range(3):
            if k != 1:
                sc[k, 1 : Z + 1, 7, :] = xr_sc[0, k]
            sc[k, 1 : Z + 1, 8 + X, :] = xr_sc[1, k]
        unpack(rt_sc, yr_sc[0], yr_sc[1])

    fill_rows()
    smooth(0)

    @pl.when(core == 1)
    def _():
        for copy in gather[0] + gather[1]:
            copy.wait_recv()
        ar2[0] = jnp.sum(ar1[...], axis=0)
        for copy in scatter:
            copy.start()

    for m in v2_m:
        m.wait_recv()
    v2[1 : ZC + 1, 8 + XC, :] = xr_v2[...]
    unpack(rt_v2, below_y, yr_v2[...])

    def sides(b, _):
        c = v2[b + 1, 8 : 8 + XC, :]
        h = halo(rt_v2, (b % PC) * XC, XC, b // PC)
        wy2[b] = jnp.where(evenc, before(c, h, lanec), after(c, h, lanec))
        return 0

    each(ZC, sides, 0)
    prolong(v2, wy2, 2)

    def fill(j):
        def body(b, packed):
            block = []
            for p in range(2):
                z = 2 * b + p
                x = ab[j, z, 0:X, :]
                xs_ab[j, pl.ds(z, 1), :] = x[0:1]
                block.append(x)
            return put(packed, jnp.concatenate(block, axis=0), j * NB + b)

        return body

    packed = jnp.zeros((L, L), F32)
    for j in range(3):
        packed = each(NB, fill(j), packed)
    ys_ab[...] = packed.T[: 6 * NB]
    ab_m = [
        message(ab.at[:, 0, pl.ds(0, X), :], ab.at[:, Z, pl.ds(0, X), :], "gz", -1),
        message(xs_ab, xr_ab, "gx", -1),
        message(ys_ab, yr_ab, "gy", -1),
    ]
    for m in ab_m:
        m.start()

    smooth(1)
    smooth(2)
    for m in ab_m:
        m.wait_recv()
    ab[:, 0:Z, X, :] = xr_ab[...]
    rt_ab[...] = jnp.concatenate(
        [pltpu.roll(yr_ab[...], 6 * NB - 1, 0), jnp.zeros((L - 6 * NB, L), F32)], axis=0
    ).T

    def gradient(j, into, add):
        def body(b, _):
            for p in range(2):
                z = 2 * b + p
                f = ab[j, z, 0:X, :]
                h = halo(rt_ab, p * X, X, j * NB + b)
                d = (ab[j, z + 1, 0:X, :] - f, ab[j, z, 1 : X + 1, :] - f, after(f, h, lane) - f)
                for k in range(3):
                    into[k, z] = into[k, z] + d[k] if add else d[k]
            return 0

        each(NB, body, 0)

    gradient(0, out, True)
    gradient(1, res, False)
    gradient(2, ed, False)

    for d in range(1, n_chips):
        scatter[2 * d].wait_recv()

    @pl.when(core == 0)
    def _():
        scatter[0].wait_recv()

    total = jnp.sum(ar2[...], axis=0)
    g1, g2, h11, h12, h22 = (
        jnp.sum(jnp.where(iota((1, L), 1) == i, total, 0.0), axis=1, keepdims=True) for i in range(5)
    )
    c2 = (g2 - h12 * g1 / h11) / (h22 - h12 * h12 / h11)
    c1 = (g1 - h12 * c2) / h11

    def finish(z, _):
        for k in range(3):
            out[k, z] = out[k, z] + c1 * res[k, z] + c2 * ed[k, z]
        return 0

    lax.fori_loop(0, Z, finish, 0, unroll=2)

    for m in used:
        m.wait_send()

    @pl.when(core == 0)
    def _():
        for copy in gather[0]:
            copy.wait_send()

    @pl.when(core == 1)
    def _():
        for copy in gather[1] + scatter:
            copy.wait_send()


def solution(mesh):
    sizes = dict(mesh.shape)
    n_spots, n_chips = sizes["gx"] * sizes["gy"], sizes["gz"] // 2

    def local(residual, edge_diag, node_shift, coarse_shift):
        _, Z, X, Y = residual.shape
        ZC, XC, NB = Z // 2, X // 2, Z // 2
        assert X == 64 and Y == L and Z % 8 == 0

        def v(*shape):
            return pltpu.VMEM(shape, F32)

        scratch = [
            v(3, Z, X, L), v(3, Z, X, L), v(Z, X, L), v(ZC, XC, L // 2),
            v(3, Z + 2, X + 16, L), v(Z + 2, X + 16, L), v(ZC, X, L),
            v(ZC, XC, L), v(ZC, XC, L),
            v(ZC + 2, XC + 16, L), v(ZC + 2, XC + 16, L),
            v(ZC, XC, L), v(ZC, XC, L),
            v(3, Z + 1, X + 8, L), v(Z, 8, L), v(Z, 8, L),
            v(L, L), v(L, L), v(L, L), v(L, L), v(L, L), v(L, L), v(L, L),
            v(10, 8, L), v(XC, L), v(ZC, L), v(ZC, L), v(8, L), v(8, L),
            v(XC, L), v(ZC, L), v(ZC, L), v(8, L), v(8, L),
            v(2, 3, Z, L), v(2, 3, Z, L), v(2, Z, L), v(2, Z, L),
            v(2, ZC, L), v(2, ZC, L), v(ZC, L), v(ZC, L), v(3, Z, L), v(3, Z, L),
            v(6 * NB, L), v(2, 6 * NB, L), v(2 * NB, L), v(2, 2 * NB, L),
            v(8, L), v(2, 8, L), v(8, L), v(8, L), v(6 * NB, L), v(6 * NB, L),
            v(1, L), v(2 * n_spots, 1, L), v(n_chips, 1, L), pltpu.SemaphoreType.REGULAR((3,)),
            pltpu.SemaphoreType.DMA((12,)),
            pltpu.SemaphoreType.DMA((56,)), pltpu.SemaphoreType.DMA((56,)),
            pltpu.SemaphoreType.DMA((n_spots,)), pltpu.SemaphoreType.DMA((2 * n_spots,)),
            pltpu.SemaphoreType.DMA((2 * n_chips,)), pltpu.SemaphoreType.DMA((n_chips,)),
        ]
        return pl.pallas_call(
            functools.partial(kernel, sizes),
            out_shape=jax.ShapeDtypeStruct(residual.shape, F32),
            in_specs=[pl.BlockSpec(memory_space=pl.ANY)] * 4,
            out_specs=pl.BlockSpec(memory_space=pltpu.VMEM),
            scratch_shapes=scratch,
            compiler_params=pltpu.CompilerParams(
                collective_id=0, has_side_effects=True, vmem_limit_bytes=48 * 1024 * 1024
            ),
        )(*(
            pltpu.with_memory_space_constraint(x, pltpu.HBM)
            for x in (residual, edge_diag, node_shift, coarse_shift)
        ))

    fine, coarse = P(None, "gz", "gx", "gy"), P("gz", "gx", "gy")
    return jax.shard_map(
        local, mesh=mesh, in_specs=(fine, fine, coarse, coarse), out_specs=fine, check_vma=False
    )
```

```python
import functools

import jax
import jax.numpy as jnp
from jax import lax
from jax.experimental import pallas as pl
from jax.experimental.pallas import tpu as pltpu
from jax.sharding import PartitionSpec as P

MESH = pl.DeviceIdType.MESH
AXES = ("gx", "gy", "gz")
L = 128
F32 = jnp.float32


def iota(shape, dim):
    return lax.broadcasted_iota(jnp.int32, shape, dim)


class Message:
    def __init__(self, copy, sends, receives):
        self.copy, self.sends, self.receives = copy, sends, receives

    def start(self):
        pl.when(self.sends)(lambda: self.copy.start())

    def wait_recv(self):
        pl.when(self.receives)(lambda: self.copy.wait_recv())

    def wait_send(self):
        pl.when(self.sends)(lambda: self.copy.wait_send())


def kernel(
    sizes, res_h, ed_h, ns_h, cs_h, out,
    res, ed, ns, cs, sc, fg, tmp, cr, cd, v1, v2, wy1, wy2, ab, face_e, face_r,
    rt_g, rt_sc, rt_fg, rt_v1, rt_v2, rt_ab, rt_d,
    dv, v1b, x2s, x2r, y2s, y2r, cdz, cdxs, cdx, cdys, cdy,
    xs_sc, xr_sc, xs_fg, xr_fg, xs_v1, xr_v1, xs_v2, xr_v2, xs_ab, xr_ab,
    ys_sc, yr_sc, ys_fg, yr_fg, ys_v1, yr_v1, ys_v2, yr_v2, ys_ab, yr_ab,
    arow, ar1, ar2, present, in_sem, send_sem, recv_sem, ar_send, ar_recv, out_send, out_recv,
):
    _, Z, X, _ = res.shape
    ZC, XC = Z // 2, X // 2
    NB = Z // 2
    PC = L // XC
    NBC = ZC // PC
    me = {a: lax.axis_index(a) for a in AXES}
    core = lax.rem(me["gz"], 2)
    used = []

    def both(flags):
        return functools.reduce(jnp.logical_and, flags)

    def message(src, dst, *steps):
        i = len(used)
        steps = dict(zip(steps[::2], steps[1::2]))
        copy = pltpu.make_async_remote_copy(
            src_ref=src, dst_ref=dst, send_sem=send_sem.at[i], recv_sem=recv_sem.at[i],
            device_id={a: me[a] + d for a, d in steps.items()}, device_id_type=MESH,
        )
        low = {a: me[a] > 0 for a in steps}
        high = {a: me[a] < sizes[a] - 1 for a in steps}
        made = Message(
            copy,
            both([high[a] if d > 0 else low[a] for a, d in steps.items()]),
            both([low[a] if d > 0 else high[a] for a, d in steps.items()]),
        )
        used.append(made)
        return made

    def load(i, pick, into):
        return (
            pltpu.make_async_copy(pick(ed_h), into(ed, face_e), in_sem.at[2 * i]),
            pltpu.make_async_copy(pick(res_h), into(res, face_r), in_sem.at[2 * i + 1]),
        )

    loads = [
        load(0, lambda h: h.at[0, Z - 1], lambda v, f: v.at[0, Z - 1]),
        load(1, lambda h: h.at[1, :, pl.ds(X - 8, 8), :], lambda v, f: f),
        load(2, lambda h: h.at[2], lambda v, f: v.at[2]),
        load(3, lambda h: h.at[1], lambda v, f: v.at[1]),
        load(4, lambda h: h.at[0, pl.ds(0, Z - 1)], lambda v, f: v.at[0, pl.ds(0, Z - 1)]),
    ]
    load_ns = pltpu.make_async_copy(ns_h, ns, in_sem.at[10])
    load_cs = pltpu.make_async_copy(cs_h, cs, in_sem.at[11])
    for pair in loads[:3]:
        for copy in pair:
            copy.start()

    def at(**steps):
        return {a: lax.rem(me[a] + d + sizes[a], sizes[a]) for a, d in steps.items()}

    near = [at(**{a: d}) for a in AXES for d in (1, -1)]
    barrier = pltpu.get_barrier_semaphore()

    zero_coarse = jnp.zeros((XC, L), F32)

    @pl.when(me["gz"] >= 0)
    def _():
        zero_plane = jnp.zeros((X, L), F32)
        for k in range(3):
            for z in (0, Z + 1):
                sc[k, z, 8 : 8 + X, :] = zero_plane
            ab[k, Z, 0:X, :] = zero_plane
        for z in (0, Z + 1):
            fg[z, 8 : 8 + X, :] = zero_plane
        for z in (0, ZC + 1):
            v1[z, 8 : 8 + XC, :] = zero_coarse
        v2[ZC + 1, 8 : 8 + XC, :] = zero_coarse
        for ref in (
            xr_sc, xr_fg, xr_v1, xr_v2, xr_ab, yr_sc, yr_fg, yr_v1, yr_v2, yr_ab,
            dv, v1b, x2r, y2r, cdz, cdx, cdy,
        ):
            ref[...] = jnp.zeros(ref.shape, F32)

    for other in near:
        pl.semaphore_signal(barrier, inc=1, device_id=other, device_id_type=MESH)

    lane = iota((X, L), 1)
    lane2 = iota((L, L), 1)
    lanec = iota((XC, L), 1)
    evenc = lanec % 2 == 0

    def put(packed, block, q):
        return jnp.where(lax.shift_right_logical(lane2, 1) == q, pltpu.roll(block, 2 * q + 1, 1), packed)

    def halo(rt, row, rows, q):
        return pltpu.roll(rt[pl.ds(row, rows), :], L - 1 - 2 * q, 1)

    def before(x, h, at):
        return jnp.where(at == 0, h, pltpu.roll(x, 1, 1))

    def after(x, h, at):
        return jnp.where(at == L - 1, h, pltpu.roll(x, L - 1, 1))

    def unpack(rt, low, high):
        n = low.shape[0]
        mixed = jnp.where(iota((n, L), 0) % 2 == 1, pltpu.roll(low, 1, 0), pltpu.roll(high, n - 1, 0))
        rt[...] = jnp.concatenate([mixed, jnp.zeros((L - n, L), F32)], axis=0).T

    def each(n, body, init, start=0):
        return lax.fori_loop(start, n, body, init, unroll=True)

    inner = pl.ds(8, X)
    third = 2 * NB
    sc_zu0 = message(sc.at[0, Z, inner, :], sc.at[0, 0, inner, :], "gz", 1)
    sc_xu1 = message(xs_sc.at[1, 1], xr_sc.at[0, 1], "gx", 1)
    sc_yu2 = message(ys_sc.at[pl.ds(2 * third, third)], yr_sc.at[0, pl.ds(2 * third, third)], "gy", 1)
    rest = [
        message(xs_sc.at[1, 0], xr_sc.at[0, 0], "gx", 1),
        message(xs_sc.at[1, 2], xr_sc.at[0, 2], "gx", 1),
        message(xs_sc.at[0], xr_sc.at[1], "gx", -1),
        message(ys_sc.at[pl.ds(0, 2 * third)], yr_sc.at[0, pl.ds(0, 2 * third)], "gy", 1),
        message(ys_sc, yr_sc.at[1], "gy", -1),
        message(sc.at[1:3, Z, inner, :], sc.at[1:3, 0, inner, :], "gz", 1),
        message(sc.at[:, 1, inner, :], sc.at[:, Z + 1, inner, :], "gz", -1),
    ]

    def arrived(i):
        for copy in loads[i]:
            copy.wait()

    def scale(k, z):
        r = 1.0 / ed[k, z]
        ed[k, z] = r
        s = res[k, z] * r
        sc[k, z + 1, 8 : 8 + X, :] = s
        xs_sc[0, k, pl.ds(z, 1), :] = s[0:1]
        if k != 1:
            xs_sc[1, k, pl.ds(z, 1), :] = s[X - 1 : X]
        return s

    def scale_all(k, packed, first):
        def body(b, packed):
            block = []
            for p in range(2):
                z = 2 * b + p
                block.append(scale(k, z))
            return put(packed, jnp.concatenate(block, axis=0), first + b)

        return each(NB, body, packed)

    arrived(0)
    scale(0, Z - 1)
    arrived(1)
    xs_sc[1, 1] = face_r[:, 7, :] * (1.0 / face_e[:, 7, :])
    arrived(2)
    for pair in loads[3:]:
        for copy in pair:
            copy.start()
    load_ns.start()
    load_cs.start()
    ys_sc[2 * third :] = scale_all(2, jnp.zeros((L, L), F32), 0).T[:third]
    pl.semaphore_wait(barrier, len(near))

    known = [
        near,
        [at(**{a: d}) for a in AXES for d in (2, -2) if sizes[a] > 4 or (sizes[a] == 4 and d > 0)],
        [at(gz=d) for d in (4, -4) if sizes["gz"] > 8] + [{"gz": me["gz"] + 1 - 2 * core}],
    ]

    def tell(i):
        for other in known[i]:
            pl.semaphore_signal(present.at[i], inc=1, device_id=other, device_id_type=MESH)

    def told(i):
        if known[i]:
            pl.semaphore_wait(present.at[i], len(known[i]))

    for m in (sc_yu2, sc_xu1, sc_zu0):
        m.start()
    tell(0)
    arrived(3)
    packed = scale_all(1, jnp.zeros((L, L), F32), NB)
    arrived(4)

    def bulk(b, packed):
        block = [scale(0, 2 * b), scale(0, 2 * b + 1)]
        return put(packed, jnp.concatenate(block, axis=0), b)

    packed = each(NB - 1, bulk, packed)
    block = [scale(0, Z - 2), sc[0, Z, 8 : 8 + X, :]]
    packed = put(packed, jnp.concatenate(block, axis=0), NB - 1)
    ys_sc[0 : 2 * third] = packed.T[: 2 * third]
    for m in rest:
        m.start()

    load_ns.wait()
    load_cs.wait()

    def invert(z, _):
        ns[z] = 1.0 / (6.0 + ns[z])
        return 0

    lax.fori_loop(0, Z, invert, 0, unroll=2)
    twice = (iota((L // 2, L), 0) == iota((L // 2, L), 1) // 2).astype(F32)
    wide = jnp.dot(
        cs[...].reshape(ZC * XC, L // 2), twice,
        precision=lax.Precision.HIGHEST, preferred_element_type=F32,
    )
    cd[...] = (1.0 / (6.0 + wide)).reshape(ZC, XC, L)

    def pack_coarse(planes):
        packed = jnp.zeros((L, L), F32)
        for q in range(NBC):
            packed = put(packed, planes(PC * q, PC * (q + 1)).reshape(L, L), q)
        return packed

    cdxs[...] = cd[:, XC - 1, :]
    cdys[...] = pack_coarse(lambda a, b: cd[a:b]).T[:8]
    fixed = [
        message(cd.at[ZC - 1], cdz, "gz", 1),
        message(cdxs, cdx, "gx", 1),
        message(cdys, cdy, "gy", 1),
    ]
    for m in fixed:
        m.start()

    for m in (sc_yu2, sc_xu1, sc_zu0):
        m.wait_recv()
    told(0)
    sc[1, 1 : Z + 1, 7, :] = xr_sc[0, 1]
    low = yr_sc[0, 2 * third :]
    unpack(rt_g, low, jnp.zeros_like(low))

    def guess(b, packed):
        block = []
        for p in range(2):
            z = 2 * b + p
            s0, s0m = sc[0, z + 1, 8 : 8 + X, :], sc[0, z, 8 : 8 + X, :]
            s1, s1m = sc[1, z + 1, 8 : 8 + X, :], sc[1, z + 1, 7 : 7 + X, :]
            s2 = sc[2, z + 1, 8 : 8 + X, :]
            s2m = before(s2, halo(rt_g, p * X, X, b), lane)
            g = ((s0m - s0) + (s1m - s1) + (s2m - s2)) * ns[z]
            fg[z + 1, 8 : 8 + X, :] = g
            xs_fg[0, pl.ds(z, 1), :] = g[0:1]
            xs_fg[1, pl.ds(z, 1), :] = g[X - 1 : X]
            block.append(g)
        return put(packed, jnp.concatenate(block, axis=0), b)

    fg_z = [
        message(fg.at[Z, inner, :], fg.at[0, inner, :], "gz", 1),
        message(fg.at[1, inner, :], fg.at[Z + 1, inner, :], "gz", -1),
    ]
    fg_m = [
        message(ys_fg, yr_fg.at[0], "gy", 1),
        message(ys_fg, yr_fg.at[1], "gy", -1),
        message(xs_fg.at[1], xr_fg.at[0], "gx", 1),
        message(xs_fg.at[0], xr_fg.at[1], "gx", -1),
    ]
    packed = guess(NB - 1, guess(0, jnp.zeros((L, L), F32)))
    for m in fg_z:
        m.start()
    packed = each(NB - 1, guess, packed, 1)
    ys_fg[...] = packed.T[: 2 * NB]
    for m in fg_m:
        m.start()
    fg_m += fg_z
    tell(1)

    for m in fg_m:
        m.wait_recv()
    told(1)
    fg[1 : Z + 1, 7, :] = xr_fg[0]
    fg[1 : Z + 1, 8 + X, :] = xr_fg[1]
    unpack(rt_fg, yr_fg[0], yr_fg[1])

    def swap(x):
        return jnp.where(evenc, pltpu.roll(x, L - 1, 1), pltpu.roll(x, 1, 1))

    def restrict(b, _):
        total = None
        for p in range(2):
            z = 2 * b + p
            g = fg[z + 1, 8 : 8 + X, :]
            h = halo(rt_fg, p * X, X, b)
            n = fg[z, 8 : 8 + X, :] + fg[z + 2, 8 : 8 + X, :]
            n += fg[z + 1, 7 : 7 + X, :] + fg[z + 1, 9 : 9 + X, :]
            n += before(g, h, lane) + after(g, h, lane)
            ab[0, z, 0:X, :] = g + n * ns[z]
            total = n if p == 0 else total + n
        tmp[b] = total
        return 0

    def direction(b, _):
        u = tmp[b, pl.ds(0, XC, 2), :] + tmp[b, pl.ds(1, XC, 2), :]
        u = u + swap(u)
        cr[b] = u
        v = u * cd[b]
        v1[b + 1, 8 : 8 + XC, :] = v
        xs_v1[0, pl.ds(b, 1), :] = v[0:1]
        xs_v1[1, pl.ds(b, 1), :] = v[XC - 1 : XC]
        x2s[pl.ds(b, 1), :] = v[XC - 2 : XC - 1]
        return 0

    def coarse_faces(v, xs, xr, ys, yr):
        mid = pl.ds(8, XC)
        return [
            message(ys, yr.at[0], "gy", 1),
            message(ys, yr.at[1], "gy", -1),
            message(xs.at[1], xr.at[0], "gx", 1),
            message(xs.at[0], xr.at[1], "gx", -1),
            message(v.at[ZC, mid, :], v.at[0, mid, :], "gz", 1),
            message(v.at[1, mid, :], v.at[ZC + 1, mid, :], "gz", -1),
        ]

    def coarse_arrive(sent, v, xr, yr, rt):
        for m in sent:
            m.wait_recv()
        v[1 : ZC + 1, 7, :] = xr[0]
        v[1 : ZC + 1, 8 + XC, :] = xr[1]
        unpack(rt, yr[0], yr[1])

    def around(v, wy, rt, b):
        c = v[b + 1, 8 : 8 + XC, :]
        h = halo(rt, (b % PC) * XC, XC, b // PC)
        w = jnp.where(evenc, before(c, h, lanec), after(c, h, lanec))
        wy[b] = w
        n = v[b, 8 : 8 + XC, :] + v[b + 2, 8 : 8 + XC, :]
        n += v[b + 1, 7 : 7 + XC, :] + v[b + 1, 9 : 9 + XC, :]
        return c, n + (w + swap(w))

    v1_x = [
        message(xs_v1.at[1], dv.at[0], "gz", 1, "gx", 1),
        message(xs_v1.at[0], dv.at[1], "gz", 1, "gx", -1),
        message(xs_v1.at[1], dv.at[2], "gz", -1, "gx", 1),
        message(xs_v1.at[1], dv.at[3], "gx", 1, "gy", 1),
        message(xs_v1.at[1], dv.at[4], "gx", 1, "gy", -1),
        message(x2s, x2r, "gx", 1),
        message(v1.at[ZC - 1, pl.ds(8, XC), :], v1b, "gz", 1),
    ]
    v1_y = [
        message(ys_v1, dv.at[5], "gz", 1, "gy", 1),
        message(ys_v1, dv.at[6], "gz", 1, "gy", -1),
        message(ys_v1, dv.at[7], "gz", -1, "gy", 1),
        message(ys_v1, dv.at[8], "gx", 1, "gy", 1),
        message(ys_v1, dv.at[9], "gx", -1, "gy", 1),
        message(y2s, y2r, "gy", 1),
    ]
    v1_f = coarse_faces(v1, xs_v1, xr_v1, ys_v1, yr_v1)
    early = v1_f[4:] + v1_x[6:]
    for b in (0, ZC - 1, ZC - 2):
        restrict(b, 0)
    for b in (0, ZC - 1, ZC - 2):
        direction(b, 0)
    for m in early:
        m.start()
    each(ZC - 2, restrict, 0, 1)
    each(ZC - 2, direction, 0, 1)
    for m in v1_x[:6] + v1_f[2:4]:
        m.start()
    packed = pack_coarse(lambda a, b: v1[1 + a : 1 + b, 8 : 8 + XC, :])
    for q in range(NBC):
        block = v1[1 + PC * q : 1 + PC * (q + 1), 8 : 8 + XC, :].reshape(L, L)
        to = L // 4 + q
        packed = jnp.where(
            lax.shift_right_logical(lane2, 1) == to, pltpu.roll(block, 2 * to + 3, 1), packed
        )
    turned = packed.T
    ys_v1[...] = turned[:8]
    y2s[...] = turned[L // 2 : L // 2 + 8]
    for m in v1_y + v1_f[:2]:
        m.start()
    tell(2)
    coarse_arrive(v1_f, v1, xr_v1, yr_v1, rt_v1)

    def first(b, sums):
        g1, g2, h11, h12 = sums
        c, n = around(v1, wy1, rt_v1, b)
        r = cr[b]
        a = r - n
        w = a * cd[b]
        v2[b + 1, 8 : 8 + XC, :] = w
        xs_v2[pl.ds(b, 1), :] = w[0:1]
        return g1 + c * r, g2 + w * r, h11 + c * a, h12 + w * a

    sums = each(ZC, first, (zero_coarse,) * 4)
    for m in v1_x + v1_y + fixed:
        m.wait_recv()
    v1[0, 7:8, :] = dv[0, 7:8, :]
    v1[0, 8 + XC : 9 + XC, :] = dv[1, 7:8, :]
    unpack(rt_d, dv[5], dv[6])
    c = v1[0, 8 : 8 + XC, :]
    h = halo(rt_d, ((ZC - 1) % PC) * XC, XC, (ZC - 1) // PC)
    w = jnp.where(evenc, before(c, h, lanec), after(c, h, lanec))
    n = v1b[...] + v1[1, 8 : 8 + XC, :] + v1[0, 7 : 7 + XC, :] + v1[0, 9 : 9 + XC, :]
    below_z = c - cdz[...] * (n + (w + swap(w)))

    row, line = iota((8, L), 0), iota((8, L), 1)
    even = line % 2 == 0
    c = xr_v1[0]
    n = x2r[...] + xs_v1[0]
    n += jnp.where(row == 0, pltpu.roll(dv[0], 1, 0), pltpu.roll(c, 1, 0))
    n += jnp.where(row == 7, pltpu.roll(dv[2], 7, 0), pltpu.roll(c, 7, 0))
    low = jnp.where(line == 0, pltpu.roll(dv[3], 1, 1), pltpu.roll(c, 1, 1))
    high = jnp.where(line == L - 1, pltpu.roll(dv[4], L - 1, 1), pltpu.roll(c, L - 1, 1))
    w = jnp.where(even, low, high)
    n += w + jnp.where(even, pltpu.roll(w, L - 1, 1), pltpu.roll(w, 1, 1))
    below_x = c - cdx[...] * n

    c = yr_v1[0]
    n = y2r[...] + pltpu.roll(ys_v1[...], 7, 0)
    down = jnp.where(row >= 2, pltpu.roll(c, 2, 0), pltpu.roll(dv[5], 6, 0))
    up = jnp.where(row < 2, pltpu.roll(c, 6, 0), pltpu.roll(dv[7], 2, 0))
    n += pltpu.roll(jnp.where(line < L - XC, c, down), XC, 1)
    n += pltpu.roll(jnp.where(line >= XC, c, up), L - XC, 1)
    n += jnp.where(line % XC == 0, pltpu.roll(dv[8], L - XC + 1, 1), pltpu.roll(c, 1, 1))
    n += jnp.where(line % XC == XC - 1, pltpu.roll(dv[9], XC - 1, 1), pltpu.roll(c, L - 1, 1))
    below_y = c - cdy[...] * n

    unpack(rt_d, 2.0 * below_y, jnp.zeros((8, L), F32))
    nothing = jnp.zeros((XC, L), F32)
    v2[0, 8 : 8 + XC, :] = below_z
    v2[1 : ZC + 1, 7, :] = below_x

    def pairs(b, sums):
        c = v2[b + 1, 8 : 8 + XC, :]
        h = halo(rt_d, (b % PC) * XC, XC, b // PC)
        w = jnp.where(evenc, before(c, h, lanec), after(c, nothing, lanec))
        n = v2[b, 8 : 8 + XC, :] + v2[b + 1, 7 : 7 + XC, :]
        return sums + c * (2.0 * n + 2.0 * w)

    inside = each(ZC, pairs, zero_coarse)
    sums += (sums[3] - inside,)

    row = jnp.zeros((1, L), F32)
    for i, s in enumerate(sums):
        one = jnp.sum(jnp.sum(s, axis=0, keepdims=True), axis=1, keepdims=True)
        row = jnp.where(iota((1, L), 1) == i, one, row)
    arow[...] = row

    spots = [(dx, dy) for dx in range(sizes["gx"]) for dy in range(sizes["gy"])]
    n_spots, n_chips = len(spots), sizes["gz"] // 2

    def remote(src, dst, i, j, sends, receives, other):
        return pltpu.make_async_remote_copy(
            src_ref=src, dst_ref=dst, send_sem=sends.at[i], recv_sem=receives.at[j],
            device_id=other, device_id_type=MESH,
        )

    gather = [
        [
            remote(arow, ar1.at[n_spots * c + i], i, n_spots * c + i, ar_send, ar_recv, at(gx=dx, gy=dy, gz=1 - c))
            for i, (dx, dy) in enumerate(spots) if c == 0 or i > 0
        ]
        for c in range(2)
    ]
    scatter = [
        remote(ar2.at[0], ar2.at[d], 2 * d + c, d, out_send, out_recv, at(gz=2 * d - c))
        for d in range(n_chips) for c in range(2) if d or c
    ]
    told(2)

    @pl.when(core == 0)
    def _():
        for copy in gather[0]:
            copy.start()

    @pl.when(core == 1)
    def _():
        for copy in gather[1]:
            copy.start()
        ar1[n_spots] = arow[...]

    packed = pack_coarse(lambda a, b: v2[1 + a : 1 + b, 8 : 8 + XC, :])
    ys_v2[...] = packed.T[:8]
    v2_m = [
        message(ys_v2, yr_v2, "gy", -1),
        message(xs_v2, xr_v2, "gx", -1),
        message(v2.at[1, pl.ds(8, XC), :], v2.at[ZC + 1, pl.ds(8, XC), :], "gz", -1),
    ]
    for m in v2_m:
        m.start()

    def prolong(v, wy, j):
        def body(b, _):
            w = 3.0 * v[b + 1, 8 : 8 + XC, :] + wy[b]
            for px in range(2):
                wx = w + v[b + 1, 7 + 2 * px : 7 + 2 * px + XC, :]
                for pz in range(2):
                    z = 2 * b + pz
                    n = wx + v[b + 2 * pz, 8 : 8 + XC, :]
                    ab[j, z, pl.ds(px, XC, 2), :] = n * ns[z, pl.ds(px, XC, 2), :]
            return 0

        each(ZC, body, 0)

    prolong(v1, wy1, 1)
    def smooth(k):
        def body(b, _):
            for p in range(2):
                z = 2 * b + p
                s = sc[k, z + 1, 8 : 8 + X, :]
                h = halo(rt_sc, p * X, X, k * NB + b)
                n = sc[k, z, 8 : 8 + X, :] + sc[k, z + 2, 8 : 8 + X, :]
                n += sc[k, z + 1, 7 : 7 + X, :] + sc[k, z + 1, 9 : 9 + X, :]
                n += before(s, h, lane) + after(s, h, lane)
                out[k, z] = s + n * ed[k, z]
            return 0

        each(NB, body, 0)

    def fill_rows():
        for m in rest:
            m.wait_recv()
        for k in range(3):
            if k != 1:
                sc[k, 1 : Z + 1, 7, :] = xr_sc[0, k]
            sc[k, 1 : Z + 1, 8 + X, :] = xr_sc[1, k]
        unpack(rt_sc, yr_sc[0], yr_sc[1])

    fill_rows()
    smooth(0)

    @pl.when(core == 1)
    def _():
        for copy in gather[0] + gather[1]:
            copy.wait_recv()
        ar2[0] = jnp.sum(ar1[...], axis=0)
        for copy in scatter:
            copy.start()

    for m in v2_m:
        m.wait_recv()
    v2[1 : ZC + 1, 8 + XC, :] = xr_v2[...]
    unpack(rt_v2, below_y, yr_v2[...])

    def sides(b, _):
        c = v2[b + 1, 8 : 8 + XC, :]
        h = halo(rt_v2, (b % PC) * XC, XC, b // PC)
        wy2[b] = jnp.where(evenc, before(c, h, lanec), after(c, h, lanec))
        return 0

    each(ZC, sides, 0)
    prolong(v2, wy2, 2)

    def fill(j):
        def body(b, packed):
            block = []
            for p in range(2):
                z = 2 * b + p
                x = ab[j, z, 0:X, :]
                xs_ab[j, pl.ds(z, 1), :] = x[0:1]
                block.append(x)
            return put(packed, jnp.concatenate(block, axis=0), j * NB + b)

        return body

    packed = jnp.zeros((L, L), F32)
    for j in range(3):
        packed = each(NB, fill(j), packed)
    ys_ab[...] = packed.T[: 6 * NB]
    ab_m = [
        message(ab.at[:, 0, pl.ds(0, X), :], ab.at[:, Z, pl.ds(0, X), :], "gz", -1),
        message(xs_ab, xr_ab, "gx", -1),
        message(ys_ab, yr_ab, "gy", -1),
    ]
    for m in ab_m:
        m.start()

    smooth(1)
    smooth(2)
    for m in ab_m:
        m.wait_recv()
    ab[:, 0:Z, X, :] = xr_ab[...]
    rt_ab[...] = jnp.concatenate(
        [pltpu.roll(yr_ab[...], 6 * NB - 1, 0), jnp.zeros((L - 6 * NB, L), F32)], axis=0
    ).T

    def gradient(j, into, add):
        def body(b, _):
            for p in range(2):
                z = 2 * b + p
                f = ab[j, z, 0:X, :]
                h = halo(rt_ab, p * X, X, j * NB + b)
                d = (ab[j, z + 1, 0:X, :] - f, ab[j, z, 1 : X + 1, :] - f, after(f, h, lane) - f)
                for k in range(3):
                    into[k, z] = into[k, z] + d[k] if add else d[k]
            return 0

        each(NB, body, 0)

    gradient(0, out, True)
    gradient(1, res, False)
    gradient(2, ed, False)

    for d in range(1, n_chips):
        scatter[2 * d].wait_recv()

    @pl.when(core == 0)
    def _():
        scatter[0].wait_recv()

    total = jnp.sum(ar2[...], axis=0)
    g1, g2, h11, h12, h22 = (
        jnp.sum(jnp.where(iota((1, L), 1) == i, total, 0.0), axis=1, keepdims=True) for i in range(5)
    )
    c2 = (g2 - h12 * g1 / h11) / (h22 - h12 * h12 / h11)
    c1 = (g1 - h12 * c2) / h11

    def finish(z, _):
        for k in range(3):
            out[k, z] = out[k, z] + c1 * res[k, z] + c2 * ed[k, z]
        return 0

    lax.fori_loop(0, Z, finish, 0, unroll=2)

    for m in used:
        m.wait_send()

    @pl.when(core == 0)
    def _():
        for copy in gather[0]:
            copy.wait_send()

    @pl.when(core == 1)
    def _():
        for copy in gather[1] + scatter:
            copy.wait_send()


def solution(mesh):
    sizes = dict(mesh.shape)
    n_spots, n_chips = sizes["gx"] * sizes["gy"], sizes["gz"] // 2

    def local(residual, edge_diag, node_shift, coarse_shift):
        _, Z, X, Y = residual.shape
        ZC, XC, NB = Z // 2, X // 2, Z // 2
        assert X == 64 and Y == L and Z % 8 == 0

        def v(*shape):
            return pltpu.VMEM(shape, F32)

        scratch = [
            v(3, Z, X, L), v(3, Z, X, L), v(Z, X, L), v(ZC, XC, L // 2),
            v(3, Z + 2, X + 16, L), v(Z + 2, X + 16, L), v(ZC, X, L),
            v(ZC, XC, L), v(ZC, XC, L),
            v(ZC + 2, XC + 16, L), v(ZC + 2, XC + 16, L),
            v(ZC, XC, L), v(ZC, XC, L),
            v(3, Z + 1, X + 8, L), v(Z, 8, L), v(Z, 8, L),
            v(L, L), v(L, L), v(L, L), v(L, L), v(L, L), v(L, L), v(L, L),
            v(10, 8, L), v(XC, L), v(ZC, L), v(ZC, L), v(8, L), v(8, L),
            v(XC, L), v(ZC, L), v(ZC, L), v(8, L), v(8, L),
            v(2, 3, Z, L), v(2, 3, Z, L), v(2, Z, L), v(2, Z, L),
            v(2, ZC, L), v(2, ZC, L), v(ZC, L), v(ZC, L), v(3, Z, L), v(3, Z, L),
            v(6 * NB, L), v(2, 6 * NB, L), v(2 * NB, L), v(2, 2 * NB, L),
            v(8, L), v(2, 8, L), v(8, L), v(8, L), v(6 * NB, L), v(6 * NB, L),
            v(1, L), v(2 * n_spots, 1, L), v(n_chips, 1, L), pltpu.SemaphoreType.REGULAR((3,)),
            pltpu.SemaphoreType.DMA((12,)),
            pltpu.SemaphoreType.DMA((56,)), pltpu.SemaphoreType.DMA((56,)),
            pltpu.SemaphoreType.DMA((n_spots,)), pltpu.SemaphoreType.DMA((2 * n_spots,)),
            pltpu.SemaphoreType.DMA((2 * n_chips,)), pltpu.SemaphoreType.DMA((n_chips,)),
        ]
        return pl.pallas_call(
            functools.partial(kernel, sizes),
            out_shape=jax.ShapeDtypeStruct(residual.shape, F32),
            in_specs=[pl.BlockSpec(memory_space=pl.ANY)] * 4,
            out_specs=pl.BlockSpec(memory_space=pltpu.VMEM),
            scratch_shapes=scratch,
            compiler_params=pltpu.CompilerParams(
                collective_id=0, has_side_effects=True, vmem_limit_bytes=48 * 1024 * 1024
            ),
        )(*(
            pltpu.with_memory_space_constraint(x, pltpu.HBM)
            for x in (residual, edge_diag, node_shift, coarse_shift)
        ))

    fine, coarse = P(None, "gz", "gx", "gy"), P("gz", "gx", "gy")
    return jax.shard_map(
        local, mesh=mesh, in_specs=(fine, fine, coarse, coarse), out_specs=fine, check_vma=False
    )
```

```python
import functools

import jax
import jax.numpy as jnp
from jax import lax
from jax.experimental import pallas as pl
from jax.experimental.pallas import tpu as pltpu
from jax.sharding import PartitionSpec as P

MESH = pl.DeviceIdType.MESH
AXES = ("gx", "gy", "gz")
L = 128
F32 = jnp.float32


def iota(shape, dim):
    return lax.broadcasted_iota(jnp.int32, shape, dim)


class Message:
    def __init__(self, copy, sends, receives):
        self.copy, self.sends, self.receives = copy, sends, receives

    def start(self):
        pl.when(self.sends)(lambda: self.copy.start())

    def wait_recv(self):
        pl.when(self.receives)(lambda: self.copy.wait_recv())

    def wait_send(self):
        pl.when(self.sends)(lambda: self.copy.wait_send())


def kernel(
    sizes, res_h, ed_h, ns_h, cs_h, out,
    res, ed, ns, cs, sc, fg, tmp, cr, cd, v1, v2, wy1, wy2, ab, face_e, face_r,
    rt_g, rt_sc, rt_fg, rt_v1, rt_v2, rt_ab, rt_d,
    dv, v1b, x2s, x2r, y2s, y2r, cdz, cdxs, cdx, cdys, cdy,
    xs_sc, xr_sc, xs_fg, xr_fg, xs_v1, xr_v1, xs_v2, xr_v2, xs_ab, xr_ab,
    ys_sc, yr_sc, ys_fg, yr_fg, ys_v1, yr_v1, ys_v2, yr_v2, ys_ab, yr_ab,
    arow, ar1, ar2, present, in_sem, send_sem, recv_sem, ar_send, ar_recv, out_send, out_recv,
):
    _, Z, X, _ = res.shape
    ZC, XC = Z // 2, X // 2
    NB = Z // 2
    PC = L // XC
    NBC = ZC // PC
    me = {a: lax.axis_index(a) for a in AXES}
    core = lax.rem(me["gz"], 2)
    used = []

    def both(flags):
        return functools.reduce(jnp.logical_and, flags)

    def message(src, dst, *steps):
        i = len(used)
        steps = dict(zip(steps[::2], steps[1::2]))
        copy = pltpu.make_async_remote_copy(
            src_ref=src, dst_ref=dst, send_sem=send_sem.at[i], recv_sem=recv_sem.at[i],
            device_id={a: me[a] + d for a, d in steps.items()}, device_id_type=MESH,
        )
        low = {a: me[a] > 0 for a in steps}
        high = {a: me[a] < sizes[a] - 1 for a in steps}
        made = Message(
            copy,
            both([high[a] if d > 0 else low[a] for a, d in steps.items()]),
            both([low[a] if d > 0 else high[a] for a, d in steps.items()]),
        )
        used.append(made)
        return made

    def load(i, pick, into):
        return (
            pltpu.make_async_copy(pick(ed_h), into(ed, face_e), in_sem.at[2 * i]),
            pltpu.make_async_copy(pick(res_h), into(res, face_r), in_sem.at[2 * i + 1]),
        )

    loads = [
        load(0, lambda h: h.at[0, Z - 1], lambda v, f: v.at[0, Z - 1]),
        load(1, lambda h: h.at[1, :, pl.ds(X - 8, 8), :], lambda v, f: f),
        load(2, lambda h: h.at[2], lambda v, f: v.at[2]),
        load(3, lambda h: h.at[1], lambda v, f: v.at[1]),
        load(4, lambda h: h.at[0, pl.ds(0, Z - 1)], lambda v, f: v.at[0, pl.ds(0, Z - 1)]),
    ]
    load_ns = pltpu.make_async_copy(ns_h, ns, in_sem.at[10])
    load_cs = pltpu.make_async_copy(cs_h, cs, in_sem.at[11])
    for pair in loads[:3]:
        for copy in pair:
            copy.start()

    def at(**steps):
        return {a: lax.rem(me[a] + d + sizes[a], sizes[a]) for a, d in steps.items()}

    near = [at(**{a: d}) for a in AXES for d in (1, -1)]
    barrier = pltpu.get_barrier_semaphore()

    zero_coarse = jnp.zeros((XC, L), F32)

    @pl.when(me["gz"] >= 0)
    def _():
        zero_plane = jnp.zeros((X, L), F32)
        for k in range(3):
            for z in (0, Z + 1):
                sc[k, z, 8 : 8 + X, :] = zero_plane
            ab[k, Z, 0:X, :] = zero_plane
        for z in (0, Z + 1):
            fg[z, 8 : 8 + X, :] = zero_plane
        for z in (0, ZC + 1):
            v1[z, 8 : 8 + XC, :] = zero_coarse
        v2[ZC + 1, 8 : 8 + XC, :] = zero_coarse
        for ref in (
            xr_sc, xr_fg, xr_v1, xr_v2, xr_ab, yr_sc, yr_fg, yr_v1, yr_v2, yr_ab,
            dv, v1b, x2r, y2r, cdz, cdx, cdy,
        ):
            ref[...] = jnp.zeros(ref.shape, F32)

    for other in near:
        pl.semaphore_signal(barrier, inc=1, device_id=other, device_id_type=MESH)

    lane = iota((X, L), 1)
    lane2 = iota((L, L), 1)
    lanec = iota((XC, L), 1)
    evenc = lanec % 2 == 0

    def put(packed, block, q):
        return jnp.where(lax.shift_right_logical(lane2, 1) == q, pltpu.roll(block, 2 * q + 1, 1), packed)

    def halo(rt, row, rows, q):
        return pltpu.roll(rt[pl.ds(row, rows), :], L - 1 - 2 * q, 1)

    def before(x, h, at):
        return jnp.where(at == 0, h, pltpu.roll(x, 1, 1))

    def after(x, h, at):
        return jnp.where(at == L - 1, h, pltpu.roll(x, L - 1, 1))

    def unpack(rt, low, high):
        n = low.shape[0]
        mixed = jnp.where(iota((n, L), 0) % 2 == 1, pltpu.roll(low, 1, 0), pltpu.roll(high, n - 1, 0))
        rt[...] = jnp.concatenate([mixed, jnp.zeros((L - n, L), F32)], axis=0).T

    def each(n, body, init, start=0):
        return lax.fori_loop(start, n, body, init, unroll=True)

    inner = pl.ds(8, X)
    third = 2 * NB
    sc_zu0 = message(sc.at[0, Z, inner, :], sc.at[0, 0, inner, :], "gz", 1)
    sc_xu1 = message(xs_sc.at[1, 1], xr_sc.at[0, 1], "gx", 1)
    sc_yu2 = message(ys_sc.at[pl.ds(2 * third, third)], yr_sc.at[0, pl.ds(2 * third, third)], "gy", 1)
    rest = [
        message(xs_sc.at[1, 0], xr_sc.at[0, 0], "gx", 1),
        message(xs_sc.at[1, 2], xr_sc.at[0, 2], "gx", 1),
        message(xs_sc.at[0], xr_sc.at[1], "gx", -1),
        message(ys_sc.at[pl.ds(0, 2 * third)], yr_sc.at[0, pl.ds(0, 2 * third)], "gy", 1),
        message(ys_sc, yr_sc.at[1], "gy", -1),
        message(sc.at[1:3, Z, inner, :], sc.at[1:3, 0, inner, :], "gz", 1),
        message(sc.at[:, 1, inner, :], sc.at[:, Z + 1, inner, :], "gz", -1),
    ]

    def arrived(i):
        for copy in loads[i]:
            copy.wait()

    def scale(k, z):
        r = 1.0 / ed[k, z]
        ed[k, z] = r
        s = res[k, z] * r
        sc[k, z + 1, 8 : 8 + X, :] = s
        xs_sc[0, k, pl.ds(z, 1), :] = s[0:1]
        if k != 1:
            xs_sc[1, k, pl.ds(z, 1), :] = s[X - 1 : X]
        return s

    def scale_all(k, packed, first):
        def body(b, packed):
            block = []
            for p in range(2):
                z = 2 * b + p
                block.append(scale(k, z))
            return put(packed, jnp.concatenate(block, axis=0), first + b)

        return each(NB, body, packed)

    arrived(0)
    scale(0, Z - 1)
    arrived(1)
    xs_sc[1, 1] = face_r[:, 7, :] * (1.0 / face_e[:, 7, :])
    pl.semaphore_wait(barrier, len(near))
    for m in (sc_zu0, sc_xu1):
        m.start()

    known = [
        near,
        [at(**{a: d}) for a in AXES for d in (2, -2) if sizes[a] > 4 or (sizes[a] == 4 and d > 0)],
        [at(gz=d) for d in (4, -4) if sizes["gz"] > 8] + [{"gz": me["gz"] + 1 - 2 * core}],
    ]

    def tell(i):
        for other in known[i]:
            pl.semaphore_signal(present.at[i], inc=1, device_id=other, device_id_type=MESH)

    def told(i):
        if known[i]:
            pl.semaphore_wait(present.at[i], len(known[i]))

    arrived(2)
    for pair in loads[3:]:
        for copy in pair:
            copy.start()
    load_ns.start()
    load_cs.start()
    ys_sc[2 * third :] = scale_all(2, jnp.zeros((L, L), F32), 0).T[:third]
    sc_yu2.start()
    tell(0)
    arrived(3)
    packed = scale_all(1, jnp.zeros((L, L), F32), NB)
    arrived(4)

    def bulk(b, packed):
        block = [scale(0, 2 * b), scale(0, 2 * b + 1)]
        return put(packed, jnp.concatenate(block, axis=0), b)

    packed = each(NB - 1, bulk, packed)
    block = [scale(0, Z - 2), sc[0, Z, 8 : 8 + X, :]]
    packed = put(packed, jnp.concatenate(block, axis=0), NB - 1)
    ys_sc[0 : 2 * third] = packed.T[: 2 * third]
    for m in rest:
        m.start()

    load_ns.wait()
    load_cs.wait()

    def invert(z, _):
        ns[z] = 1.0 / (6.0 + ns[z])
        return 0

    lax.fori_loop(0, Z, invert, 0, unroll=2)
    twice = (iota((L // 2, L), 0) == iota((L // 2, L), 1) // 2).astype(F32)
    wide = jnp.dot(
        cs[...].reshape(ZC * XC, L // 2), twice,
        precision=lax.Precision.HIGHEST, preferred_element_type=F32,
    )
    cd[...] = (1.0 / (6.0 + wide)).reshape(ZC, XC, L)

    def pack_coarse(planes):
        packed = jnp.zeros((L, L), F32)
        for q in range(NBC):
            packed = put(packed, planes(PC * q, PC * (q + 1)).reshape(L, L), q)
        return packed

    cdxs[...] = cd[:, XC - 1, :]
    cdys[...] = pack_coarse(lambda a, b: cd[a:b]).T[:8]
    fixed = [
        message(cd.at[ZC - 1], cdz, "gz", 1),
        message(cdxs, cdx, "gx", 1),
        message(cdys, cdy, "gy", 1),
    ]
    for m in fixed:
        m.start()

    for m in (sc_yu2, sc_xu1, sc_zu0):
        m.wait_recv()
    told(0)
    sc[1, 1 : Z + 1, 7, :] = xr_sc[0, 1]
    low = yr_sc[0, 2 * third :]
    unpack(rt_g, low, jnp.zeros_like(low))

    def guess(b, packed):
        block = []
        for p in range(2):
            z = 2 * b + p
            s0, s0m = sc[0, z + 1, 8 : 8 + X, :], sc[0, z, 8 : 8 + X, :]
            s1, s1m = sc[1, z + 1, 8 : 8 + X, :], sc[1, z + 1, 7 : 7 + X, :]
            s2 = sc[2, z + 1, 8 : 8 + X, :]
            s2m = before(s2, halo(rt_g, p * X, X, b), lane)
            g = ((s0m - s0) + (s1m - s1) + (s2m - s2)) * ns[z]
            fg[z + 1, 8 : 8 + X, :] = g
            xs_fg[0, pl.ds(z, 1), :] = g[0:1]
            xs_fg[1, pl.ds(z, 1), :] = g[X - 1 : X]
            block.append(g)
        return put(packed, jnp.concatenate(block, axis=0), b)

    fg_z = [
        message(fg.at[Z, inner, :], fg.at[0, inner, :], "gz", 1),
        message(fg.at[1, inner, :], fg.at[Z + 1, inner, :], "gz", -1),
    ]
    fg_m = [
        message(ys_fg, yr_fg.at[0], "gy", 1),
        message(ys_fg, yr_fg.at[1], "gy", -1),
        message(xs_fg.at[1], xr_fg.at[0], "gx", 1),
        message(xs_fg.at[0], xr_fg.at[1], "gx", -1),
    ]
    packed = guess(NB - 1, guess(0, jnp.zeros((L, L), F32)))
    for m in fg_z:
        m.start()
    packed = each(NB - 1, guess, packed, 1)
    ys_fg[...] = packed.T[: 2 * NB]
    for m in fg_m:
        m.start()
    fg_m += fg_z
    tell(1)

    for m in fg_m:
        m.wait_recv()
    told(1)
    fg[1 : Z + 1, 7, :] = xr_fg[0]
    fg[1 : Z + 1, 8 + X, :] = xr_fg[1]
    unpack(rt_fg, yr_fg[0], yr_fg[1])

    def swap(x):
        return jnp.where(evenc, pltpu.roll(x, L - 1, 1), pltpu.roll(x, 1, 1))

    def restrict(b, _):
        total = None
        for p in range(2):
            z = 2 * b + p
            g = fg[z + 1, 8 : 8 + X, :]
            h = halo(rt_fg, p * X, X, b)
            n = fg[z, 8 : 8 + X, :] + fg[z + 2, 8 : 8 + X, :]
            n += fg[z + 1, 7 : 7 + X, :] + fg[z + 1, 9 : 9 + X, :]
            n += before(g, h, lane) + after(g, h, lane)
            ab[0, z, 0:X, :] = g + n * ns[z]
            total = n if p == 0 else total + n
        tmp[b] = total
        return 0

    def direction(b, _):
        u = tmp[b, pl.ds(0, XC, 2), :] + tmp[b, pl.ds(1, XC, 2), :]
        u = u + swap(u)
        cr[b] = u
        v = u * cd[b]
        v1[b + 1, 8 : 8 + XC, :] = v
        xs_v1[0, pl.ds(b, 1), :] = v[0:1]
        xs_v1[1, pl.ds(b, 1), :] = v[XC - 1 : XC]
        x2s[pl.ds(b, 1), :] = v[XC - 2 : XC - 1]
        return 0

    def coarse_faces(v, xs, xr, ys, yr):
        mid = pl.ds(8, XC)
        return [
            message(ys, yr.at[0], "gy", 1),
            message(ys, yr.at[1], "gy", -1),
            message(xs.at[1], xr.at[0], "gx", 1),
            message(xs.at[0], xr.at[1], "gx", -1),
            message(v.at[ZC, mid, :], v.at[0, mid, :], "gz", 1),
            message(v.at[1, mid, :], v.at[ZC + 1, mid, :], "gz", -1),
        ]

    def coarse_arrive(sent, v, xr, yr, rt):
        for m in sent:
            m.wait_recv()
        v[1 : ZC + 1, 7, :] = xr[0]
        v[1 : ZC + 1, 8 + XC, :] = xr[1]
        unpack(rt, yr[0], yr[1])

    def around(v, wy, rt, b):
        c = v[b + 1, 8 : 8 + XC, :]
        h = halo(rt, (b % PC) * XC, XC, b // PC)
        w = jnp.where(evenc, before(c, h, lanec), after(c, h, lanec))
        wy[b] = w
        n = v[b, 8 : 8 + XC, :] + v[b + 2, 8 : 8 + XC, :]
        n += v[b + 1, 7 : 7 + XC, :] + v[b + 1, 9 : 9 + XC, :]
        return c, n + (w + swap(w))

    v1_x = [
        message(xs_v1.at[1], dv.at[0], "gz", 1, "gx", 1),
        message(xs_v1.at[0], dv.at[1], "gz", 1, "gx", -1),
        message(xs_v1.at[1], dv.at[2], "gz", -1, "gx", 1),
        message(xs_v1.at[1], dv.at[3], "gx", 1, "gy", 1),
        message(xs_v1.at[1], dv.at[4], "gx", 1, "gy", -1),
        message(x2s, x2r, "gx", 1),
        message(v1.at[ZC - 1, pl.ds(8, XC), :], v1b, "gz", 1),
    ]
    v1_y = [
        message(ys_v1, dv.at[5], "gz", 1, "gy", 1),
        message(ys_v1, dv.at[6], "gz", 1, "gy", -1),
        message(ys_v1, dv.at[7], "gz", -1, "gy", 1),
        message(ys_v1, dv.at[8], "gx", 1, "gy", 1),
        message(ys_v1, dv.at[9], "gx", -1, "gy", 1),
        message(y2s, y2r, "gy", 1),
    ]
    v1_f = coarse_faces(v1, xs_v1, xr_v1, ys_v1, yr_v1)
    early = v1_f[4:] + v1_x[6:]
    for b in (0, ZC - 1, ZC - 2):
        restrict(b, 0)
    for b in (0, ZC - 1, ZC - 2):
        direction(b, 0)
    for m in early:
        m.start()
    each(ZC - 2, restrict, 0, 1)
    each(ZC - 2, direction, 0, 1)
    for m in v1_x[:6] + v1_f[2:4]:
        m.start()
    packed = pack_coarse(lambda a, b: v1[1 + a : 1 + b, 8 : 8 + XC, :])
    for q in range(NBC):
        block = v1[1 + PC * q : 1 + PC * (q + 1), 8 : 8 + XC, :].reshape(L, L)
        to = L // 4 + q
        packed = jnp.where(
            lax.shift_right_logical(lane2, 1) == to, pltpu.roll(block, 2 * to + 3, 1), packed
        )
    turned = packed.T
    ys_v1[...] = turned[:8]
    y2s[...] = turned[L // 2 : L // 2 + 8]
    for m in v1_y + v1_f[:2]:
        m.start()
    tell(2)
    coarse_arrive(v1_f, v1, xr_v1, yr_v1, rt_v1)

    def first(b, sums):
        g1, g2, h11, h12 = sums
        c, n = around(v1, wy1, rt_v1, b)
        r = cr[b]
        a = r - n
        w = a * cd[b]
        v2[b + 1, 8 : 8 + XC, :] = w
        xs_v2[pl.ds(b, 1), :] = w[0:1]
        return g1 + c * r, g2 + w * r, h11 + c * a, h12 + w * a

    sums = each(ZC, first, (zero_coarse,) * 4)
    for m in v1_x + v1_y + fixed:
        m.wait_recv()
    v1[0, 7:8, :] = dv[0, 7:8, :]
    v1[0, 8 + XC : 9 + XC, :] = dv[1, 7:8, :]
    unpack(rt_d, dv[5], dv[6])
    c = v1[0, 8 : 8 + XC, :]
    h = halo(rt_d, ((ZC - 1) % PC) * XC, XC, (ZC - 1) // PC)
    w = jnp.where(evenc, before(c, h, lanec), after(c, h, lanec))
    n = v1b[...] + v1[1, 8 : 8 + XC, :] + v1[0, 7 : 7 + XC, :] + v1[0, 9 : 9 + XC, :]
    below_z = c - cdz[...] * (n + (w + swap(w)))

    row, line = iota((8, L), 0), iota((8, L), 1)
    even = line % 2 == 0
    c = xr_v1[0]
    n = x2r[...] + xs_v1[0]
    n += jnp.where(row == 0, pltpu.roll(dv[0], 1, 0), pltpu.roll(c, 1, 0))
    n += jnp.where(row == 7, pltpu.roll(dv[2], 7, 0), pltpu.roll(c, 7, 0))
    low = jnp.where(line == 0, pltpu.roll(dv[3], 1, 1), pltpu.roll(c, 1, 1))
    high = jnp.where(line == L - 1, pltpu.roll(dv[4], L - 1, 1), pltpu.roll(c, L - 1, 1))
    w = jnp.where(even, low, high)
    n += w + jnp.where(even, pltpu.roll(w, L - 1, 1), pltpu.roll(w, 1, 1))
    below_x = c - cdx[...] * n

    c = yr_v1[0]
    n = y2r[...] + pltpu.roll(ys_v1[...], 7, 0)
    down = jnp.where(row >= 2, pltpu.roll(c, 2, 0), pltpu.roll(dv[5], 6, 0))
    up = jnp.where(row < 2, pltpu.roll(c, 6, 0), pltpu.roll(dv[7], 2, 0))
    n += pltpu.roll(jnp.where(line < L - XC, c, down), XC, 1)
    n += pltpu.roll(jnp.where(line >= XC, c, up), L - XC, 1)
    n += jnp.where(line % XC == 0, pltpu.roll(dv[8], L - XC + 1, 1), pltpu.roll(c, 1, 1))
    n += jnp.where(line % XC == XC - 1, pltpu.roll(dv[9], XC - 1, 1), pltpu.roll(c, L - 1, 1))
    below_y = c - cdy[...] * n

    unpack(rt_d, 2.0 * below_y, jnp.zeros((8, L), F32))
    nothing = jnp.zeros((XC, L), F32)
    v2[0, 8 : 8 + XC, :] = below_z
    v2[1 : ZC + 1, 7, :] = below_x

    def pairs(b, sums):
        c = v2[b + 1, 8 : 8 + XC, :]
        h = halo(rt_d, (b % PC) * XC, XC, b // PC)
        w = jnp.where(evenc, before(c, h, lanec), after(c, nothing, lanec))
        n = v2[b, 8 : 8 + XC, :] + v2[b + 1, 7 : 7 + XC, :]
        return sums + c * (2.0 * n + 2.0 * w)

    inside = each(ZC, pairs, zero_coarse)
    sums += (sums[3] - inside,)

    row = jnp.zeros((1, L), F32)
    for i, s in enumerate(sums):
        one = jnp.sum(jnp.sum(s, axis=0, keepdims=True), axis=1, keepdims=True)
        row = jnp.where(iota((1, L), 1) == i, one, row)
    arow[...] = row

    spots = [(dx, dy) for dx in range(sizes["gx"]) for dy in range(sizes["gy"])]
    n_spots, n_chips = len(spots), sizes["gz"] // 2

    def remote(src, dst, i, j, sends, receives, other):
        return pltpu.make_async_remote_copy(
            src_ref=src, dst_ref=dst, send_sem=sends.at[i], recv_sem=receives.at[j],
            device_id=other, device_id_type=MESH,
        )

    gather = [
        [
            remote(arow, ar1.at[n_spots * c + i], i, n_spots * c + i, ar_send, ar_recv, at(gx=dx, gy=dy, gz=1 - c))
            for i, (dx, dy) in enumerate(spots) if c == 0 or i > 0
        ]
        for c in range(2)
    ]
    scatter = [
        remote(ar2.at[0], ar2.at[d], 2 * d + c, d, out_send, out_recv, at(gz=2 * d - c))
        for d in range(n_chips) for c in range(2) if d or c
    ]
    told(2)

    @pl.when(core == 0)
    def _():
        for copy in gather[0]:
            copy.start()

    @pl.when(core == 1)
    def _():
        for copy in gather[1]:
            copy.start()
        ar1[n_spots] = arow[...]

    packed = pack_coarse(lambda a, b: v2[1 + a : 1 + b, 8 : 8 + XC, :])
    ys_v2[...] = packed.T[:8]
    v2_m = [
        message(ys_v2, yr_v2, "gy", -1),
        message(xs_v2, xr_v2, "gx", -1),
        message(v2.at[1, pl.ds(8, XC), :], v2.at[ZC + 1, pl.ds(8, XC), :], "gz", -1),
    ]
    for m in v2_m:
        m.start()

    def prolong(v, wy, j):
        def body(b, _):
            w = 3.0 * v[b + 1, 8 : 8 + XC, :] + wy[b]
            for px in range(2):
                wx = w + v[b + 1, 7 + 2 * px : 7 + 2 * px + XC, :]
                for pz in range(2):
                    z = 2 * b + pz
                    n = wx + v[b + 2 * pz, 8 : 8 + XC, :]
                    ab[j, z, pl.ds(px, XC, 2), :] = n * ns[z, pl.ds(px, XC, 2), :]
            return 0

        each(ZC, body, 0)

    prolong(v1, wy1, 1)
    def smooth(k):
        def body(b, _):
            for p in range(2):
                z = 2 * b + p
                s = sc[k, z + 1, 8 : 8 + X, :]
                h = halo(rt_sc, p * X, X, k * NB + b)
                n = sc[k, z, 8 : 8 + X, :] + sc[k, z + 2, 8 : 8 + X, :]
                n += sc[k, z + 1, 7 : 7 + X, :] + sc[k, z + 1, 9 : 9 + X, :]
                n += before(s, h, lane) + after(s, h, lane)
                out[k, z] = s + n * ed[k, z]
            return 0

        each(NB, body, 0)

    def fill_rows():
        for m in rest:
            m.wait_recv()
        for k in range(3):
            if k != 1:
                sc[k, 1 : Z + 1, 7, :] = xr_sc[0, k]
            sc[k, 1 : Z + 1, 8 + X, :] = xr_sc[1, k]
        unpack(rt_sc, yr_sc[0], yr_sc[1])

    fill_rows()
    smooth(0)

    @pl.when(core == 1)
    def _():
        for copy in gather[0] + gather[1]:
            copy.wait_recv()
        ar2[0] = jnp.sum(ar1[...], axis=0)
        for copy in scatter:
            copy.start()

    for m in v2_m:
        m.wait_recv()
    v2[1 : ZC + 1, 8 + XC, :] = xr_v2[...]
    unpack(rt_v2, below_y, yr_v2[...])

    def sides(b, _):
        c = v2[b + 1, 8 : 8 + XC, :]
        h = halo(rt_v2, (b % PC) * XC, XC, b // PC)
        wy2[b] = jnp.where(evenc, before(c, h, lanec), after(c, h, lanec))
        return 0

    each(ZC, sides, 0)
    prolong(v2, wy2, 2)

    def fill(j):
        def body(b, packed):
            block = []
            for p in range(2):
                z = 2 * b + p
                x = ab[j, z, 0:X, :]
                xs_ab[j, pl.ds(z, 1), :] = x[0:1]
                block.append(x)
            return put(packed, jnp.concatenate(block, axis=0), j * NB + b)

        return body

    packed = jnp.zeros((L, L), F32)
    for j in range(3):
        packed = each(NB, fill(j), packed)
    ys_ab[...] = packed.T[: 6 * NB]
    ab_m = [
        message(ab.at[:, 0, pl.ds(0, X), :], ab.at[:, Z, pl.ds(0, X), :], "gz", -1),
        message(xs_ab, xr_ab, "gx", -1),
        message(ys_ab, yr_ab, "gy", -1),
    ]
    for m in ab_m:
        m.start()

    smooth(1)
    smooth(2)
    for m in ab_m:
        m.wait_recv()
    ab[:, 0:Z, X, :] = xr_ab[...]
    rt_ab[...] = jnp.concatenate(
        [pltpu.roll(yr_ab[...], 6 * NB - 1, 0), jnp.zeros((L - 6 * NB, L), F32)], axis=0
    ).T

    def gradient(j, into, add):
        def body(b, _):
            for p in range(2):
                z = 2 * b + p
                f = ab[j, z, 0:X, :]
                h = halo(rt_ab, p * X, X, j * NB + b)
                d = (ab[j, z + 1, 0:X, :] - f, ab[j, z, 1 : X + 1, :] - f, after(f, h, lane) - f)
                for k in range(3):
                    into[k, z] = into[k, z] + d[k] if add else d[k]
            return 0

        each(NB, body, 0)

    gradient(0, out, True)
    gradient(1, res, False)
    gradient(2, ed, False)

    for d in range(1, n_chips):
        scatter[2 * d].wait_recv()

    @pl.when(core == 0)
    def _():
        scatter[0].wait_recv()

    total = jnp.sum(ar2[...], axis=0)
    g1, g2, h11, h12, h22 = (
        jnp.sum(jnp.where(iota((1, L), 1) == i, total, 0.0), axis=1, keepdims=True) for i in range(5)
    )
    c2 = (g2 - h12 * g1 / h11) / (h22 - h12 * h12 / h11)
    c1 = (g1 - h12 * c2) / h11

    def finish(z, _):
        for k in range(3):
            out[k, z] = out[k, z] + c1 * res[k, z] + c2 * ed[k, z]
        return 0

    lax.fori_loop(0, Z, finish, 0, unroll=2)

    for m in used:
        m.wait_send()

    @pl.when(core == 0)
    def _():
        for copy in gather[0]:
            copy.wait_send()

    @pl.when(core == 1)
    def _():
        for copy in gather[1] + scatter:
            copy.wait_send()


def solution(mesh):
    sizes = dict(mesh.shape)
    n_spots, n_chips = sizes["gx"] * sizes["gy"], sizes["gz"] // 2

    def local(residual, edge_diag, node_shift, coarse_shift):
        _, Z, X, Y = residual.shape
        ZC, XC, NB = Z // 2, X // 2, Z // 2
        assert X == 64 and Y == L and Z % 8 == 0

        def v(*shape):
            return pltpu.VMEM(shape, F32)

        scratch = [
            v(3, Z, X, L), v(3, Z, X, L), v(Z, X, L), v(ZC, XC, L // 2),
            v(3, Z + 2, X + 16, L), v(Z + 2, X + 16, L), v(ZC, X, L),
            v(ZC, XC, L), v(ZC, XC, L),
            v(ZC + 2, XC + 16, L), v(ZC + 2, XC + 16, L),
            v(ZC, XC, L), v(ZC, XC, L),
            v(3, Z + 1, X + 8, L), v(Z, 8, L), v(Z, 8, L),
            v(L, L), v(L, L), v(L, L), v(L, L), v(L, L), v(L, L), v(L, L),
            v(10, 8, L), v(XC, L), v(ZC, L), v(ZC, L), v(8, L), v(8, L),
            v(XC, L), v(ZC, L), v(ZC, L), v(8, L), v(8, L),
            v(2, 3, Z, L), v(2, 3, Z, L), v(2, Z, L), v(2, Z, L),
            v(2, ZC, L), v(2, ZC, L), v(ZC, L), v(ZC, L), v(3, Z, L), v(3, Z, L),
            v(6 * NB, L), v(2, 6 * NB, L), v(2 * NB, L), v(2, 2 * NB, L),
            v(8, L), v(2, 8, L), v(8, L), v(8, L), v(6 * NB, L), v(6 * NB, L),
            v(1, L), v(2 * n_spots, 1, L), v(n_chips, 1, L), pltpu.SemaphoreType.REGULAR((3,)),
            pltpu.SemaphoreType.DMA((12,)),
            pltpu.SemaphoreType.DMA((56,)), pltpu.SemaphoreType.DMA((56,)),
            pltpu.SemaphoreType.DMA((n_spots,)), pltpu.SemaphoreType.DMA((2 * n_spots,)),
            pltpu.SemaphoreType.DMA((2 * n_chips,)), pltpu.SemaphoreType.DMA((n_chips,)),
        ]
        return pl.pallas_call(
            functools.partial(kernel, sizes),
            out_shape=jax.ShapeDtypeStruct(residual.shape, F32),
            in_specs=[pl.BlockSpec(memory_space=pl.ANY)] * 4,
            out_specs=pl.BlockSpec(memory_space=pltpu.VMEM),
            scratch_shapes=scratch,
            compiler_params=pltpu.CompilerParams(
                collective_id=0, has_side_effects=True, vmem_limit_bytes=48 * 1024 * 1024
            ),
        )(*(
            pltpu.with_memory_space_constraint(x, pltpu.HBM)
            for x in (residual, edge_diag, node_shift, coarse_shift)
        ))

    fine, coarse = P(None, "gz", "gx", "gy"), P("gz", "gx", "gy")
    return jax.shard_map(
        local, mesh=mesh, in_specs=(fine, fine, coarse, coarse), out_specs=fine, check_vma=False
    )
```

```python
import functools

import jax
import jax.numpy as jnp
from jax import lax
from jax.experimental import pallas as pl
from jax.experimental.pallas import tpu as pltpu
from jax.sharding import PartitionSpec as P

MESH = pl.DeviceIdType.MESH
AXES = ("gx", "gy", "gz")
L = 128
F32 = jnp.float32


def iota(shape, dim):
    return lax.broadcasted_iota(jnp.int32, shape, dim)


class Message:
    def __init__(self, copy, sends, receives):
        self.copy, self.sends, self.receives = copy, sends, receives

    def start(self):
        pl.when(self.sends)(lambda: self.copy.start())

    def wait_recv(self):
        pl.when(self.receives)(lambda: self.copy.wait_recv())

    def wait_send(self):
        pl.when(self.sends)(lambda: self.copy.wait_send())


def kernel(
    sizes, res_h, ed_h, ns_h, cs_h, out,
    res, ed, ns, cs, sc, fg, tmp, cr, cd, v1, v2, wy1, wy2, ab, face_e, face_r,
    rt_g, rt_sc, rt_fg, rt_v1, rt_v2, rt_ab, rt_d,
    dv, v1b, x2s, x2r, y2s, y2r, cdz, cdxs, cdx, cdys, cdy,
    xs_sc, xr_sc, xs_fg, xr_fg, xs_v1, xr_v1, xs_v2, xr_v2, xs_ab, xr_ab,
    ys_sc, yr_sc, ys_fg, yr_fg, ys_v1, yr_v1, ys_v2, yr_v2, ys_ab, yr_ab,
    arow, ar1, ar2, present, in_sem, send_sem, recv_sem, ar_send, ar_recv, out_send, out_recv,
):
    _, Z, X, _ = res.shape
    ZC, XC = Z // 2, X // 2
    NB = Z // 2
    PC = L // XC
    NBC = ZC // PC
    me = {a: lax.axis_index(a) for a in AXES}
    core = lax.rem(me["gz"], 2)
    used = []

    def both(flags):
        return functools.reduce(jnp.logical_and, flags)

    def message(src, dst, *steps):
        i = len(used)
        steps = dict(zip(steps[::2], steps[1::2]))
        copy = pltpu.make_async_remote_copy(
            src_ref=src, dst_ref=dst, send_sem=send_sem.at[i], recv_sem=recv_sem.at[i],
            device_id={a: me[a] + d for a, d in steps.items()}, device_id_type=MESH,
        )
        low = {a: me[a] > 0 for a in steps}
        high = {a: me[a] < sizes[a] - 1 for a in steps}
        made = Message(
            copy,
            both([high[a] if d > 0 else low[a] for a, d in steps.items()]),
            both([low[a] if d > 0 else high[a] for a, d in steps.items()]),
        )
        used.append(made)
        return made

    def load(i, pick, into):
        return (
            pltpu.make_async_copy(pick(ed_h), into(ed, face_e), in_sem.at[2 * i]),
            pltpu.make_async_copy(pick(res_h), into(res, face_r), in_sem.at[2 * i + 1]),
        )

    loads = [
        load(0, lambda h: h.at[0, Z - 1], lambda v, f: v.at[0, Z - 1]),
        load(1, lambda h: h.at[1, :, pl.ds(X - 8, 8), :], lambda v, f: f),
        load(2, lambda h: h.at[2, pl.ds(0, Z // 2)], lambda v, f: v.at[2, pl.ds(0, Z // 2)]),
        load(5, lambda h: h.at[2, pl.ds(Z // 2, Z // 2)], lambda v, f: v.at[2, pl.ds(Z // 2, Z // 2)]),
        load(3, lambda h: h.at[1], lambda v, f: v.at[1]),
        load(4, lambda h: h.at[0, pl.ds(0, Z - 1)], lambda v, f: v.at[0, pl.ds(0, Z - 1)]),
    ]
    load_ns = pltpu.make_async_copy(ns_h, ns, in_sem.at[12])
    load_cs = pltpu.make_async_copy(cs_h, cs, in_sem.at[13])
    for pair in loads[:4]:
        for copy in pair:
            copy.start()

    def at(**steps):
        return {a: lax.rem(me[a] + d + sizes[a], sizes[a]) for a, d in steps.items()}

    near = [at(**{a: d}) for a in AXES for d in (1, -1)]
    barrier = pltpu.get_barrier_semaphore()

    zero_coarse = jnp.zeros((XC, L), F32)

    @pl.when(me["gz"] >= 0)
    def _():
        zero_plane = jnp.zeros((X, L), F32)
        for k in range(3):
            for z in (0, Z + 1):
                sc[k, z, 8 : 8 + X, :] = zero_plane
            ab[k, Z, 0:X, :] = zero_plane
        for z in (0, Z + 1):
            fg[z, 8 : 8 + X, :] = zero_plane
        for z in (0, ZC + 1):
            v1[z, 8 : 8 + XC, :] = zero_coarse
        v2[ZC + 1, 8 : 8 + XC, :] = zero_coarse
        for ref in (
            xr_sc, xr_fg, xr_v1, xr_v2, xr_ab, yr_sc, yr_fg, yr_v1, yr_v2, yr_ab,
            dv, v1b, x2r, y2r, cdz, cdx, cdy,
        ):
            ref[...] = jnp.zeros(ref.shape, F32)

    for other in near:
        pl.semaphore_signal(barrier, inc=1, device_id=other, device_id_type=MESH)

    lane = iota((X, L), 1)
    lane2 = iota((L, L), 1)
    lanec = iota((XC, L), 1)
    evenc = lanec % 2 == 0

    def put(packed, block, q):
        return jnp.where(lax.shift_right_logical(lane2, 1) == q, pltpu.roll(block, 2 * q + 1, 1), packed)

    def halo(rt, row, rows, q):
        return pltpu.roll(rt[pl.ds(row, rows), :], L - 1 - 2 * q, 1)

    def before(x, h, at):
        return jnp.where(at == 0, h, pltpu.roll(x, 1, 1))

    def after(x, h, at):
        return jnp.where(at == L - 1, h, pltpu.roll(x, L - 1, 1))

    def unpack(rt, low, high):
        n = low.shape[0]
        mixed = jnp.where(iota((n, L), 0) % 2 == 1, pltpu.roll(low, 1, 0), pltpu.roll(high, n - 1, 0))
        rt[...] = jnp.concatenate([mixed, jnp.zeros((L - n, L), F32)], axis=0).T

    def each(n, body, init, start=0):
        return lax.fori_loop(start, n, body, init, unroll=True)

    inner = pl.ds(8, X)
    third = 2 * NB
    sc_zu0 = message(sc.at[0, Z, inner, :], sc.at[0, 0, inner, :], "gz", 1)
    sc_xu1 = message(xs_sc.at[1, 1], xr_sc.at[0, 1], "gx", 1)
    sc_yu2 = message(ys_sc.at[pl.ds(2 * third, third)], yr_sc.at[0, pl.ds(2 * third, third)], "gy", 1)
    rest = [
        message(xs_sc.at[1, 0], xr_sc.at[0, 0], "gx", 1),
        message(xs_sc.at[1, 2], xr_sc.at[0, 2], "gx", 1),
        message(xs_sc.at[0], xr_sc.at[1], "gx", -1),
        message(ys_sc.at[pl.ds(0, 2 * third)], yr_sc.at[0, pl.ds(0, 2 * third)], "gy", 1),
        message(ys_sc, yr_sc.at[1], "gy", -1),
        message(sc.at[1:3, Z, inner, :], sc.at[1:3, 0, inner, :], "gz", 1),
        message(sc.at[:, 1, inner, :], sc.at[:, Z + 1, inner, :], "gz", -1),
    ]

    def arrived(i):
        for copy in loads[i]:
            copy.wait()

    def scale(k, z):
        r = 1.0 / ed[k, z]
        ed[k, z] = r
        s = res[k, z] * r
        sc[k, z + 1, 8 : 8 + X, :] = s
        xs_sc[0, k, pl.ds(z, 1), :] = s[0:1]
        if k != 1:
            xs_sc[1, k, pl.ds(z, 1), :] = s[X - 1 : X]
        return s

    def scale_all(k, packed, first):
        def body(b, packed):
            block = []
            for p in range(2):
                z = 2 * b + p
                block.append(scale(k, z))
            return put(packed, jnp.concatenate(block, axis=0), first + b)

        if k == 2:
            packed = each(NB // 2, body, packed)
            arrived(3)
            return each(NB, body, packed, NB // 2)
        return each(NB, body, packed)

    arrived(0)
    scale(0, Z - 1)
    arrived(1)
    xs_sc[1, 1] = face_r[:, 7, :] * (1.0 / face_e[:, 7, :])
    pl.semaphore_wait(barrier, len(near))
    for m in (sc_zu0, sc_xu1):
        m.start()

    known = [
        near,
        [at(**{a: d}) for a in AXES for d in (2, -2) if sizes[a] > 4 or (sizes[a] == 4 and d > 0)],
        [at(gz=d) for d in (4, -4) if sizes["gz"] > 8] + [{"gz": me["gz"] + 1 - 2 * core}],
    ]

    def tell(i):
        for other in known[i]:
            pl.semaphore_signal(present.at[i], inc=1, device_id=other, device_id_type=MESH)

    def told(i):
        if known[i]:
            pl.semaphore_wait(present.at[i], len(known[i]))

    arrived(2)
    for pair in loads[4:]:
        for copy in pair:
            copy.start()
    load_ns.start()
    load_cs.start()
    ys_sc[2 * third :] = scale_all(2, jnp.zeros((L, L), F32), 0).T[:third]
    sc_yu2.start()
    tell(0)
    arrived(4)
    packed = scale_all(1, jnp.zeros((L, L), F32), NB)
    arrived(5)

    def bulk(b, packed):
        block = [scale(0, 2 * b), scale(0, 2 * b + 1)]
        return put(packed, jnp.concatenate(block, axis=0), b)

    packed = each(NB - 1, bulk, packed)
    block = [scale(0, Z - 2), sc[0, Z, 8 : 8 + X, :]]
    packed = put(packed, jnp.concatenate(block, axis=0), NB - 1)
    ys_sc[0 : 2 * third] = packed.T[: 2 * third]
    for m in rest:
        m.start()

    load_ns.wait()
    load_cs.wait()

    def invert(z, _):
        ns[z] = 1.0 / (6.0 + ns[z])
        return 0

    lax.fori_loop(0, Z, invert, 0, unroll=2)
    twice = (iota((L // 2, L), 0) == iota((L // 2, L), 1) // 2).astype(F32)
    wide = jnp.dot(
        cs[...].reshape(ZC * XC, L // 2), twice,
        precision=lax.Precision.HIGHEST, preferred_element_type=F32,
    )
    cd[...] = (1.0 / (6.0 + wide)).reshape(ZC, XC, L)

    def pack_coarse(planes):
        packed = jnp.zeros((L, L), F32)
        for q in range(NBC):
            packed = put(packed, planes(PC * q, PC * (q + 1)).reshape(L, L), q)
        return packed

    cdxs[...] = cd[:, XC - 1, :]
    cdys[...] = pack_coarse(lambda a, b: cd[a:b]).T[:8]
    fixed = [
        message(cd.at[ZC - 1], cdz, "gz", 1),
        message(cdxs, cdx, "gx", 1),
        message(cdys, cdy, "gy", 1),
    ]
    for m in fixed:
        m.start()

    for m in (sc_yu2, sc_xu1, sc_zu0):
        m.wait_recv()
    told(0)
    sc[1, 1 : Z + 1, 7, :] = xr_sc[0, 1]
    low = yr_sc[0, 2 * third :]
    unpack(rt_g, low, jnp.zeros_like(low))

    def guess(b, packed):
        block = []
        for p in range(2):
            z = 2 * b + p
            s0, s0m = sc[0, z + 1, 8 : 8 + X, :], sc[0, z, 8 : 8 + X, :]
            s1, s1m = sc[1, z + 1, 8 : 8 + X, :], sc[1, z + 1, 7 : 7 + X, :]
            s2 = sc[2, z + 1, 8 : 8 + X, :]
            s2m = before(s2, halo(rt_g, p * X, X, b), lane)
            g = ((s0m - s0) + (s1m - s1) + (s2m - s2)) * ns[z]
            fg[z + 1, 8 : 8 + X, :] = g
            xs_fg[0, pl.ds(z, 1), :] = g[0:1]
            xs_fg[1, pl.ds(z, 1), :] = g[X - 1 : X]
            block.append(g)
        return put(packed, jnp.concatenate(block, axis=0), b)

    fg_z = [
        message(fg.at[Z, inner, :], fg.at[0, inner, :], "gz", 1),
        message(fg.at[1, inner, :], fg.at[Z + 1, inner, :], "gz", -1),
    ]
    fg_m = [
        message(ys_fg, yr_fg.at[0], "gy", 1),
        message(ys_fg, yr_fg.at[1], "gy", -1),
        message(xs_fg.at[1], xr_fg.at[0], "gx", 1),
        message(xs_fg.at[0], xr_fg.at[1], "gx", -1),
    ]
    packed = guess(NB - 1, guess(0, jnp.zeros((L, L), F32)))
    for m in fg_z:
        m.start()
    packed = each(NB - 1, guess, packed, 1)
    ys_fg[...] = packed.T[: 2 * NB]
    for m in fg_m:
        m.start()
    fg_m += fg_z
    tell(1)

    for m in fg_m:
        m.wait_recv()
    told(1)
    fg[1 : Z + 1, 7, :] = xr_fg[0]
    fg[1 : Z + 1, 8 + X, :] = xr_fg[1]
    unpack(rt_fg, yr_fg[0], yr_fg[1])

    def swap(x):
        return jnp.where(evenc, pltpu.roll(x, L - 1, 1), pltpu.roll(x, 1, 1))

    def restrict(b, _):
        total = None
        for p in range(2):
            z = 2 * b + p
            g = fg[z + 1, 8 : 8 + X, :]
            h = halo(rt_fg, p * X, X, b)
            n = fg[z, 8 : 8 + X, :] + fg[z + 2, 8 : 8 + X, :]
            n += fg[z + 1, 7 : 7 + X, :] + fg[z + 1, 9 : 9 + X, :]
            n += before(g, h, lane) + after(g, h, lane)
            ab[0, z, 0:X, :] = g + n * ns[z]
            total = n if p == 0 else total + n
        tmp[b] = total
        return 0

    def direction(b, _):
        u = tmp[b, pl.ds(0, XC, 2), :] + tmp[b, pl.ds(1, XC, 2), :]
        u = u + swap(u)
        cr[b] = u
        v = u * cd[b]
        v1[b + 1, 8 : 8 + XC, :] = v
        xs_v1[0, pl.ds(b, 1), :] = v[0:1]
        xs_v1[1, pl.ds(b, 1), :] = v[XC - 1 : XC]
        x2s[pl.ds(b, 1), :] = v[XC - 2 : XC - 1]
        return 0

    def coarse_faces(v, xs, xr, ys, yr):
        mid = pl.ds(8, XC)
        return [
            message(ys, yr.at[0], "gy", 1),
            message(ys, yr.at[1], "gy", -1),
            message(xs.at[1], xr.at[0], "gx", 1),
            message(xs.at[0], xr.at[1], "gx", -1),
            message(v.at[ZC, mid, :], v.at[0, mid, :], "gz", 1),
            message(v.at[1, mid, :], v.at[ZC + 1, mid, :], "gz", -1),
        ]

    def coarse_arrive(sent, v, xr, yr, rt):
        for m in sent:
            m.wait_recv()
        v[1 : ZC + 1, 7, :] = xr[0]
        v[1 : ZC + 1, 8 + XC, :] = xr[1]
        unpack(rt, yr[0], yr[1])

    def around(v, wy, rt, b):
        c = v[b + 1, 8 : 8 + XC, :]
        h = halo(rt, (b % PC) * XC, XC, b // PC)
        w = jnp.where(evenc, before(c, h, lanec), after(c, h, lanec))
        wy[b] = w
        n = v[b, 8 : 8 + XC, :] + v[b + 2, 8 : 8 + XC, :]
        n += v[b + 1, 7 : 7 + XC, :] + v[b + 1, 9 : 9 + XC, :]
        return c, n + (w + swap(w))

    v1_x = [
        message(xs_v1.at[1], dv.at[0], "gz", 1, "gx", 1),
        message(xs_v1.at[0], dv.at[1], "gz", 1, "gx", -1),
        message(xs_v1.at[1], dv.at[2], "gz", -1, "gx", 1),
        message(xs_v1.at[1], dv.at[3], "gx", 1, "gy", 1),
        message(xs_v1.at[1], dv.at[4], "gx", 1, "gy", -1),
        message(x2s, x2r, "gx", 1),
        message(v1.at[ZC - 1, pl.ds(8, XC), :], v1b, "gz", 1),
    ]
    v1_y = [
        message(ys_v1, dv.at[5], "gz", 1, "gy", 1),
        message(ys_v1, dv.at[6], "gz", 1, "gy", -1),
        message(ys_v1, dv.at[7], "gz", -1, "gy", 1),
        message(ys_v1, dv.at[8], "gx", 1, "gy", 1),
        message(ys_v1, dv.at[9], "gx", -1, "gy", 1),
        message(y2s, y2r, "gy", 1),
    ]
    v1_f = coarse_faces(v1, xs_v1, xr_v1, ys_v1, yr_v1)
    early = v1_f[4:] + v1_x[6:]
    for b in (0, ZC - 1, ZC - 2):
        restrict(b, 0)
    for b in (0, ZC - 1, ZC - 2):
        direction(b, 0)
    for m in early:
        m.start()
    each(ZC - 2, restrict, 0, 1)
    each(ZC - 2, direction, 0, 1)
    for m in v1_x[:6] + v1_f[2:4]:
        m.start()
    packed = pack_coarse(lambda a, b: v1[1 + a : 1 + b, 8 : 8 + XC, :])
    for q in range(NBC):
        block = v1[1 + PC * q : 1 + PC * (q + 1), 8 : 8 + XC, :].reshape(L, L)
        to = L // 4 + q
        packed = jnp.where(
            lax.shift_right_logical(lane2, 1) == to, pltpu.roll(block, 2 * to + 3, 1), packed
        )
    turned = packed.T
    ys_v1[...] = turned[:8]
    y2s[...] = turned[L // 2 : L // 2 + 8]
    for m in v1_y + v1_f[:2]:
        m.start()
    tell(2)
    coarse_arrive(v1_f, v1, xr_v1, yr_v1, rt_v1)

    def first(b, sums):
        g1, g2, h11, h12 = sums
        c, n = around(v1, wy1, rt_v1, b)
        r = cr[b]
        a = r - n
        w = a * cd[b]
        v2[b + 1, 8 : 8 + XC, :] = w
        xs_v2[pl.ds(b, 1), :] = w[0:1]
        return g1 + c * r, g2 + w * r, h11 + c * a, h12 + w * a

    sums = each(ZC, first, (zero_coarse,) * 4)
    for m in v1_x + v1_y + fixed:
        m.wait_recv()
    v1[0, 7:8, :] = dv[0, 7:8, :]
    v1[0, 8 + XC : 9 + XC, :] = dv[1, 7:8, :]
    unpack(rt_d, dv[5], dv[6])
    c = v1[0, 8 : 8 + XC, :]
    h = halo(rt_d, ((ZC - 1) % PC) * XC, XC, (ZC - 1) // PC)
    w = jnp.where(evenc, before(c, h, lanec), after(c, h, lanec))
    n = v1b[...] + v1[1, 8 : 8 + XC, :] + v1[0, 7 : 7 + XC, :] + v1[0, 9 : 9 + XC, :]
    below_z = c - cdz[...] * (n + (w + swap(w)))

    row, line = iota((8, L), 0), iota((8, L), 1)
    even = line % 2 == 0
    c = xr_v1[0]
    n = x2r[...] + xs_v1[0]
    n += jnp.where(row == 0, pltpu.roll(dv[0], 1, 0), pltpu.roll(c, 1, 0))
    n += jnp.where(row == 7, pltpu.roll(dv[2], 7, 0), pltpu.roll(c, 7, 0))
    low = jnp.where(line == 0, pltpu.roll(dv[3], 1, 1), pltpu.roll(c, 1, 1))
    high = jnp.where(line == L - 1, pltpu.roll(dv[4], L - 1, 1), pltpu.roll(c, L - 1, 1))
    w = jnp.where(even, low, high)
    n += w + jnp.where(even, pltpu.roll(w, L - 1, 1), pltpu.roll(w, 1, 1))
    below_x = c - cdx[...] * n

    c = yr_v1[0]
    n = y2r[...] + pltpu.roll(ys_v1[...], 7, 0)
    down = jnp.where(row >= 2, pltpu.roll(c, 2, 0), pltpu.roll(dv[5], 6, 0))
    up = jnp.where(row < 2, pltpu.roll(c, 6, 0), pltpu.roll(dv[7], 2, 0))
    n += pltpu.roll(jnp.where(line < L - XC, c, down), XC, 1)
    n += pltpu.roll(jnp.where(line >= XC, c, up), L - XC, 1)
    n += jnp.where(line % XC == 0, pltpu.roll(dv[8], L - XC + 1, 1), pltpu.roll(c, 1, 1))
    n += jnp.where(line % XC == XC - 1, pltpu.roll(dv[9], XC - 1, 1), pltpu.roll(c, L - 1, 1))
    below_y = c - cdy[...] * n

    unpack(rt_d, 2.0 * below_y, jnp.zeros((8, L), F32))
    nothing = jnp.zeros((XC, L), F32)
    v2[0, 8 : 8 + XC, :] = below_z
    v2[1 : ZC + 1, 7, :] = below_x

    def pairs(b, sums):
        c = v2[b + 1, 8 : 8 + XC, :]
        h = halo(rt_d, (b % PC) * XC, XC, b // PC)
        w = jnp.where(evenc, before(c, h, lanec), after(c, nothing, lanec))
        n = v2[b, 8 : 8 + XC, :] + v2[b + 1, 7 : 7 + XC, :]
        return sums + c * (2.0 * n + 2.0 * w)

    inside = each(ZC, pairs, zero_coarse)
    sums += (sums[3] - inside,)

    row = jnp.zeros((1, L), F32)
    for i, s in enumerate(sums):
        one = jnp.sum(jnp.sum(s, axis=0, keepdims=True), axis=1, keepdims=True)
        row = jnp.where(iota((1, L), 1) == i, one, row)
    arow[...] = row

    spots = [(dx, dy) for dx in range(sizes["gx"]) for dy in range(sizes["gy"])]
    n_spots, n_chips = len(spots), sizes["gz"] // 2

    def remote(src, dst, i, j, sends, receives, other):
        return pltpu.make_async_remote_copy(
            src_ref=src, dst_ref=dst, send_sem=sends.at[i], recv_sem=receives.at[j],
            device_id=other, device_id_type=MESH,
        )

    gather = [
        [
            remote(arow, ar1.at[n_spots * c + i], i, n_spots * c + i, ar_send, ar_recv, at(gx=dx, gy=dy, gz=1 - c))
            for i, (dx, dy) in enumerate(spots) if c == 0 or i > 0
        ]
        for c in range(2)
    ]
    scatter = [
        remote(ar2.at[0], ar2.at[d], 2 * d + c, d, out_send, out_recv, at(gz=2 * d - c))
        for d in range(n_chips) for c in range(2) if d or c
    ]
    told(2)

    @pl.when(core == 0)
    def _():
        for copy in gather[0]:
            copy.start()

    @pl.when(core == 1)
    def _():
        for copy in gather[1]:
            copy.start()
        ar1[n_spots] = arow[...]

    packed = pack_coarse(lambda a, b: v2[1 + a : 1 + b, 8 : 8 + XC, :])
    ys_v2[...] = packed.T[:8]
    v2_m = [
        message(ys_v2, yr_v2, "gy", -1),
        message(xs_v2, xr_v2, "gx", -1),
        message(v2.at[1, pl.ds(8, XC), :], v2.at[ZC + 1, pl.ds(8, XC), :], "gz", -1),
    ]
    for m in v2_m:
        m.start()

    def prolong(v, wy, j):
        def body(b, _):
            w = 3.0 * v[b + 1, 8 : 8 + XC, :] + wy[b]
            for px in range(2):
                wx = w + v[b + 1, 7 + 2 * px : 7 + 2 * px + XC, :]
                for pz in range(2):
                    z = 2 * b + pz
                    n = wx + v[b + 2 * pz, 8 : 8 + XC, :]
                    ab[j, z, pl.ds(px, XC, 2), :] = n * ns[z, pl.ds(px, XC, 2), :]
            return 0

        each(ZC, body, 0)

    prolong(v1, wy1, 1)
    def smooth(k):
        def body(b, _):
            for p in range(2):
                z = 2 * b + p
                s = sc[k, z + 1, 8 : 8 + X, :]
                h = halo(rt_sc, p * X, X, k * NB + b)
                n = sc[k, z, 8 : 8 + X, :] + sc[k, z + 2, 8 : 8 + X, :]
                n += sc[k, z + 1, 7 : 7 + X, :] + sc[k, z + 1, 9 : 9 + X, :]
                n += before(s, h, lane) + after(s, h, lane)
                out[k, z] = s + n * ed[k, z]
            return 0

        each(NB, body, 0)

    def fill_rows():
        for m in rest:
            m.wait_recv()
        for k in range(3):
            if k != 1:
                sc[k, 1 : Z + 1, 7, :] = xr_sc[0, k]
            sc[k, 1 : Z + 1, 8 + X, :] = xr_sc[1, k]
        unpack(rt_sc, yr_sc[0], yr_sc[1])

    fill_rows()
    smooth(0)

    @pl.when(core == 1)
    def _():
        for copy in gather[0] + gather[1]:
            copy.wait_recv()
        ar2[0] = jnp.sum(ar1[...], axis=0)
        for copy in scatter:
            copy.start()

    for m in v2_m:
        m.wait_recv()
    v2[1 : ZC + 1, 8 + XC, :] = xr_v2[...]
    unpack(rt_v2, below_y, yr_v2[...])

    def sides(b, _):
        c = v2[b + 1, 8 : 8 + XC, :]
        h = halo(rt_v2, (b % PC) * XC, XC, b // PC)
        wy2[b] = jnp.where(evenc, before(c, h, lanec), after(c, h, lanec))
        return 0

    each(ZC, sides, 0)
    prolong(v2, wy2, 2)

    def fill(j):
        def body(b, packed):
            block = []
            for p in range(2):
                z = 2 * b + p
                x = ab[j, z, 0:X, :]
                xs_ab[j, pl.ds(z, 1), :] = x[0:1]
                block.append(x)
            return put(packed, jnp.concatenate(block, axis=0), j * NB + b)

        return body

    packed = jnp.zeros((L, L), F32)
    for j in range(3):
        packed = each(NB, fill(j), packed)
    ys_ab[...] = packed.T[: 6 * NB]
    ab_m = [
        message(ab.at[:, 0, pl.ds(0, X), :], ab.at[:, Z, pl.ds(0, X), :], "gz", -1),
        message(xs_ab, xr_ab, "gx", -1),
        message(ys_ab, yr_ab, "gy", -1),
    ]
    for m in ab_m:
        m.start()

    smooth(1)
    smooth(2)
    for m in ab_m:
        m.wait_recv()
    ab[:, 0:Z, X, :] = xr_ab[...]
    rt_ab[...] = jnp.concatenate(
        [pltpu.roll(yr_ab[...], 6 * NB - 1, 0), jnp.zeros((L - 6 * NB, L), F32)], axis=0
    ).T

    def gradient(j, into, add):
        def body(b, _):
            for p in range(2):
                z = 2 * b + p
                f = ab[j, z, 0:X, :]
                h = halo(rt_ab, p * X, X, j * NB + b)
                d = (ab[j, z + 1, 0:X, :] - f, ab[j, z, 1 : X + 1, :] - f, after(f, h, lane) - f)
                for k in range(3):
                    into[k, z] = into[k, z] + d[k] if add else d[k]
            return 0

        each(NB, body, 0)

    gradient(0, out, True)
    gradient(1, res, False)
    gradient(2, ed, False)

    for d in range(1, n_chips):
        scatter[2 * d].wait_recv()

    @pl.when(core == 0)
    def _():
        scatter[0].wait_recv()

    total = jnp.sum(ar2[...], axis=0)
    g1, g2, h11, h12, h22 = (
        jnp.sum(jnp.where(iota((1, L), 1) == i, total, 0.0), axis=1, keepdims=True) for i in range(5)
    )
    c2 = (g2 - h12 * g1 / h11) / (h22 - h12 * h12 / h11)
    c1 = (g1 - h12 * c2) / h11

    def finish(z, _):
        for k in range(3):
            out[k, z] = out[k, z] + c1 * res[k, z] + c2 * ed[k, z]
        return 0

    lax.fori_loop(0, Z, finish, 0, unroll=4)

    for m in used:
        m.wait_send()

    @pl.when(core == 0)
    def _():
        for copy in gather[0]:
            copy.wait_send()

    @pl.when(core == 1)
    def _():
        for copy in gather[1] + scatter:
            copy.wait_send()


def solution(mesh):
    sizes = dict(mesh.shape)
    n_spots, n_chips = sizes["gx"] * sizes["gy"], sizes["gz"] // 2

    def local(residual, edge_diag, node_shift, coarse_shift):
        _, Z, X, Y = residual.shape
        ZC, XC, NB = Z // 2, X // 2, Z // 2
        assert X == 64 and Y == L and Z % 8 == 0

        def v(*shape):
            return pltpu.VMEM(shape, F32)

        scratch = [
            v(3, Z, X, L), v(3, Z, X, L), v(Z, X, L), v(ZC, XC, L // 2),
            v(3, Z + 2, X + 16, L), v(Z + 2, X + 16, L), v(ZC, X, L),
            v(ZC, XC, L), v(ZC, XC, L),
            v(ZC + 2, XC + 16, L), v(ZC + 2, XC + 16, L),
            v(ZC, XC, L), v(ZC, XC, L),
            v(3, Z + 1, X + 8, L), v(Z, 8, L), v(Z, 8, L),
            v(L, L), v(L, L), v(L, L), v(L, L), v(L, L), v(L, L), v(L, L),
            v(10, 8, L), v(XC, L), v(ZC, L), v(ZC, L), v(8, L), v(8, L),
            v(XC, L), v(ZC, L), v(ZC, L), v(8, L), v(8, L),
            v(2, 3, Z, L), v(2, 3, Z, L), v(2, Z, L), v(2, Z, L),
            v(2, ZC, L), v(2, ZC, L), v(ZC, L), v(ZC, L), v(3, Z, L), v(3, Z, L),
            v(6 * NB, L), v(2, 6 * NB, L), v(2 * NB, L), v(2, 2 * NB, L),
            v(8, L), v(2, 8, L), v(8, L), v(8, L), v(6 * NB, L), v(6 * NB, L),
            v(1, L), v(2 * n_spots, 1, L), v(n_chips, 1, L), pltpu.SemaphoreType.REGULAR((3,)),
            pltpu.SemaphoreType.DMA((14,)),
            pltpu.SemaphoreType.DMA((56,)), pltpu.SemaphoreType.DMA((56,)),
            pltpu.SemaphoreType.DMA((n_spots,)), pltpu.SemaphoreType.DMA((2 * n_spots,)),
            pltpu.SemaphoreType.DMA((2 * n_chips,)), pltpu.SemaphoreType.DMA((n_chips,)),
        ]
        return pl.pallas_call(
            functools.partial(kernel, sizes),
            out_shape=jax.ShapeDtypeStruct(residual.shape, F32),
            in_specs=[pl.BlockSpec(memory_space=pl.ANY)] * 4,
            out_specs=pl.BlockSpec(memory_space=pltpu.VMEM),
            scratch_shapes=scratch,
            compiler_params=pltpu.CompilerParams(
                collective_id=0, has_side_effects=True, vmem_limit_bytes=48 * 1024 * 1024,
            ),
        )(*(
            pltpu.with_memory_space_constraint(x, pltpu.HBM)
            for x in (residual, edge_diag, node_shift, coarse_shift)
        ))

    fine, coarse = P(None, "gz", "gx", "gy"), P("gz", "gx", "gy")
    return jax.shard_map(
        local, mesh=mesh, in_specs=(fine, fine, coarse, coarse), out_specs=fine, check_vma=False
    )
```
